8 devices in a mesh: replica: 1 (over z), model: 8 (over y, x, core).
Axes of the slice: x: 2, y: 2, z: 1, core: 2. Of those that a mesh axis runs over, the one named last changes fastest.
Arguments:
- x: bfloat16 [512, 2048], P('replica')
- w_query: bfloat16 [2048, 2048], P(None, 'model')
- w_key: bfloat16 [2048, 256], replicated
- w_value: bfloat16 [2048, 256], replicated
- w_out: bfloat16 [2048, 2048], P('model')
- k_cache: bfloat16 [512, 1, 2048, 256], P('replica')
- v_cache: bfloat16 [512, 1, 2048, 256], P('replica')
- lengths: int32 [512], P('replica')
Outputs:
- output 1: bfloat16 [512, 2048], P('replica')
- output 2: bfloat16 [512, 1, 256], P('replica')
- output 3: bfloat16 [512, 1, 256], P('replica')
All inputs are finite; a program needn't handle non-finite values.
Results may differ from the reference program's by a relative error of at most 0.00406014.
Values are sent between devices in bfloat16 or wider.
A program may use at most 4.25 GiB of HBM per device.

```python
import jax
import jax.numpy as jnp
from jax import lax

D_MODEL = 2048
NUM_HEADS = 8
KV_HEADS = 1
HEAD_DIM = 256
BATCH_SIZE = 512
CONTEXT_LEN = 2048


def draw_lengths(rng_key):
    key_perm, key_long, key_short = jax.random.split(rng_key, 3)
    perm_rank = jax.random.permutation(key_perm, BATCH_SIZE)
    long_count = max(1, BATCH_SIZE // 16)
    long_len = jax.random.randint(key_long, (BATCH_SIZE,), CONTEXT_LEN // 2, CONTEXT_LEN)
    short_len = jax.random.randint(key_short, (BATCH_SIZE,), 1, 33)
    seq_lens = jnp.where(perm_rank < 2 + long_count, long_len, short_len)
    seq_lens = jnp.where(perm_rank == 1, 1, seq_lens)
    seq_lens = jnp.where(perm_rank == 0, CONTEXT_LEN - 1, seq_lens)
    return seq_lens.astype(jnp.int32)


def setup_inputs(seed: int = 0, part: int = 0) -> dict:
    base_key = jax.random.key(seed)
    key_wq, key_wk, key_wv, key_wo = jax.random.split(base_key, 4)
    part_key = jax.random.fold_in(jax.random.key(seed + 1), part)
    key_x, key_kc, key_vc, key_mean, key_len = jax.random.split(part_key, 5)
    q_width = NUM_HEADS * HEAD_DIM
    kv_width = KV_HEADS * HEAD_DIM
    cache_shape = (BATCH_SIZE, KV_HEADS, CONTEXT_LEN, HEAD_DIM)
    x = jax.random.normal(key_x, (BATCH_SIZE, D_MODEL), jnp.float32).astype(jnp.bfloat16)
    w_query = (jax.random.normal(key_wq, (D_MODEL, q_width), jnp.float32) * D_MODEL ** -0.5).astype(jnp.bfloat16)
    w_key = (jax.random.normal(key_wk, (D_MODEL, kv_width), jnp.float32) * D_MODEL ** -0.5).astype(jnp.bfloat16)
    w_value = (jax.random.normal(key_wv, (D_MODEL, kv_width), jnp.float32) * D_MODEL ** -0.5).astype(jnp.bfloat16)
    w_out = (jax.random.normal(key_wo, (q_width, D_MODEL), jnp.float32) * q_width ** -0.5).astype(jnp.bfloat16)
    k_cache = (1.25 * jax.random.normal(key_kc, cache_shape, jnp.float32)).astype(jnp.bfloat16)
    v_mean = jax.random.normal(key_mean, (BATCH_SIZE, KV_HEADS, 1, HEAD_DIM), jnp.float32)
    v_cache = (jax.random.normal(key_vc, cache_shape, jnp.float32) + v_mean).astype(jnp.bfloat16)
    lengths = draw_lengths(key_len)
    return {"x": x, "w_query": w_query, "w_key": w_key, "w_value": w_value, "w_out": w_out, "k_cache": k_cache, "v_cache": v_cache, "lengths": lengths}


def reference(x, w_query, w_key, w_value, w_out, k_cache, v_cache, lengths):
    group_size = NUM_HEADS // KV_HEADS
    inv_sqrt = HEAD_DIM ** -0.5
    q_all = jnp.dot(x, w_query, preferred_element_type=jnp.float32).astype(jnp.bfloat16)
    k_new = jnp.dot(x, w_key, preferred_element_type=jnp.float32).astype(jnp.bfloat16).reshape(BATCH_SIZE, KV_HEADS, HEAD_DIM)
    v_new = jnp.dot(x, w_value, preferred_element_type=jnp.float32).astype(jnp.bfloat16).reshape(BATCH_SIZE, KV_HEADS, HEAD_DIM)
    q_heads = q_all.reshape(BATCH_SIZE, KV_HEADS, group_size, HEAD_DIM)
    positions = jnp.arange(CONTEXT_LEN)

    def one_sequence(item):
        q_seq, k_rows, v_rows, k_one, v_one, seq_len = item
        q_f32 = q_seq.astype(jnp.float32)
        scores = jnp.einsum("grd,gtd->grt", q_f32, k_rows.astype(jnp.float32)) * inv_sqrt
        score_new = jnp.einsum("grd,gd->gr", q_f32, k_one.astype(jnp.float32)) * inv_sqrt
        in_range = positions[None, None, :] < seq_len
        scores = jnp.where(in_range, scores, -jnp.inf)
        row_max = jnp.maximum(jnp.max(scores, axis=-1), score_new)
        weights = jnp.exp(scores - row_max[:, :, None])
        weight_new = jnp.exp(score_new - row_max)
        norm_sum = jnp.sum(weights, axis=-1) + weight_new
        out_sum = jnp.einsum("grt,gtd->grd", weights.astype(jnp.bfloat16).astype(jnp.float32), v_rows.astype(jnp.float32))
        out_sum = out_sum + weight_new.astype(jnp.bfloat16).astype(jnp.float32)[:, :, None] * v_one.astype(jnp.float32)[:, None, :]
        return (out_sum / norm_sum[:, :, None]).astype(jnp.bfloat16)

    attn_out = lax.map(one_sequence, (q_heads, k_cache, v_cache, k_new, v_new, lengths))
    o_flat = attn_out.reshape(BATCH_SIZE, NUM_HEADS * HEAD_DIM)
    y = (x.astype(jnp.float32) + jnp.dot(o_flat, w_out, preferred_element_type=jnp.float32)).astype(jnp.bfloat16)
    return (y, k_new, v_new)
```

```python
import functools

import jax
import jax.numpy as jnp
from jax import lax
from jax.experimental import pallas as pl
from jax.experimental.pallas import tpu as pltpu
from jax.sharding import PartitionSpec as P

BF = jnp.bfloat16
F32 = jnp.float32
HEADS = 8
HD = 256
LOCAL = 64
SHORT = 32
GROUP = 16
CHUNK = 256
MAXLEN = 2048
SLOTS = 12
SCALE = HD ** -0.5
DIMS_T = (((1,), (1,)), ((), ()))


def coords():
    me = lax.axis_index("model")
    return me, me // 4, (me // 2) % 2, me % 2


def peer(rel):
    _, y, x, k = coords()
    dy, dx, dk = rel // 4, (rel // 2) % 2, rel % 2
    return (((y + dy) % 2) * 2 + (x + dx) % 2) * 2 + (k + dk) % 2


def entry_barrier(rels):
    barrier = pltpu.get_barrier_semaphore()
    for rel in rels:
        pl.semaphore_signal(barrier, inc=1, device_id={"model": peer(rel)}, device_id_type=pl.DeviceIdType.MESH)
    pl.semaphore_wait(barrier, len(rels))


def remote(src, dst, send_sem, recv_sem, rel):
    return pltpu.make_async_remote_copy(
        src_ref=src, dst_ref=dst, send_sem=send_sem, recv_sem=recv_sem,
        device_id={"model": peer(rel)}, device_id_type=pl.DeviceIdType.MESH)


RELS = (6, 7, 2, 3, 4, 5, 1)


def project_kernel(x_hbm, wq_hbm, wk_hbm, wv_hbm, wo_hbm, q_out, kn_out, vn_out, wc_out,
                   x_v, wq_v, wk_v, wv_v, q_v, in_sem, own_sem, qs, qr, ws, wr):
    me, y, x, k = coords()
    loads = [pltpu.make_async_copy(src, dst, in_sem.at[i]) for i, (src, dst) in enumerate(
        ((wq_hbm, wq_v), (x_hbm, x_v), (wk_hbm, wk_v), (wv_hbm, wv_v)))]
    for load in loads:
        load.start()
    own_w = pltpu.make_async_copy(
        wo_hbm.at[:, pl.ds(pl.multiple_of(me * HD, HD), HD)], wc_out.at[pl.ds(pl.multiple_of(me * HD, HD), HD), :], own_sem)
    own_w.start()
    entry_barrier(RELS)
    loads[0].wait()
    loads[1].wait()
    copies = []
    for chip_rel in (6, 2, 4, 0):
        chip = peer(chip_rel) // 2
        rows = pl.ds(pl.multiple_of(chip * 2 * LOCAL, 2 * LOCAL), 2 * LOCAL)
        q_v[rows, :] = jnp.dot(x_v[rows, :], wq_v[...], preferred_element_type=F32).astype(BF)
        for rel in (chip_rel, chip_rel + 1):
            if rel == 0:
                continue
            there = peer(rel)
            copy = remote(q_v.at[pl.ds(pl.multiple_of(there * LOCAL, LOCAL), LOCAL), :], q_out.at[me],
                          qs.at[rel], qr.at[rel], rel)
            copy.start()
            copies.append(copy)
    mine = pl.ds(pl.multiple_of(me * LOCAL, LOCAL), LOCAL)
    q_out[me] = q_v[mine, :]
    for rel in RELS:
        there = peer(rel)
        copy = remote(wo_hbm.at[:, pl.ds(pl.multiple_of(there * HD, HD), HD)],
                      wc_out.at[pl.ds(pl.multiple_of(me * HD, HD), HD), :], ws.at[rel], wr.at[rel], rel)
        copy.start()
        copies.append(copy)
    loads[2].wait()
    loads[3].wait()
    for part in range(2):
        rows = pl.ds(part * 256, 256)
        kn_out[rows, :] = jnp.dot(x_v[rows, :], wk_v[...], preferred_element_type=F32).astype(BF)
        vn_out[rows, :] = jnp.dot(x_v[rows, :], wv_v[...], preferred_element_type=F32).astype(BF)
    own_w.wait()
    for copy in copies:
        copy.wait()


def project(x, wq, wk, wv, wo):
    rows, depth = x.shape
    hbm_spec = pl.BlockSpec(memory_space=pltpu.HBM)
    vmem_spec = pl.BlockSpec(memory_space=pltpu.VMEM)
    return pl.pallas_call(
        project_kernel,
        out_shape=(
            jax.ShapeDtypeStruct((HEADS, LOCAL, HD), BF),
            jax.ShapeDtypeStruct((rows, HD), BF),
            jax.ShapeDtypeStruct((rows, HD), BF),
            jax.ShapeDtypeStruct((HEADS * HD, HD), BF),
        ),
        in_specs=[hbm_spec] * 5,
        out_specs=(vmem_spec,) * 4,
        scratch_shapes=[
            pltpu.VMEM((rows, depth), BF),
            pltpu.VMEM((depth, HD), BF),
            pltpu.VMEM((depth, HD), BF),
            pltpu.VMEM((depth, HD), BF),
            pltpu.VMEM((rows, HD), BF),
            pltpu.SemaphoreType.DMA((4,)),
            pltpu.SemaphoreType.DMA,
            pltpu.SemaphoreType.DMA((8,)),
            pltpu.SemaphoreType.DMA((8,)),
            pltpu.SemaphoreType.DMA((8,)),
            pltpu.SemaphoreType.DMA((8,)),
        ],
        compiler_params=pltpu.CompilerParams(collective_id=0, has_side_effects=True, vmem_limit_bytes=40 * 2 ** 20),
        name="project",
    )(x, wq, wk, wv, wo)


def attend_kernel(len_ref, q_ref, kn_ref, vn_ref, k_hbm, v_hbm, o_ref, kn_out, vn_out,
                  ks, vs, kl, vl, qf, knf, vnf, acc, lens_v, lidx, short_sem, k_sem, v_sem, new_sem):
    me = lax.axis_index("model")
    base = me * LOCAL
    short_k = pltpu.make_async_copy(k_hbm.at[pl.ds(base, LOCAL), 0, pl.ds(0, SHORT), :], ks, short_sem.at[0])
    short_v = pltpu.make_async_copy(v_hbm.at[pl.ds(base, LOCAL), 0, pl.ds(0, SHORT), :], vs, short_sem.at[1])
    short_k.start()
    short_v.start()
    new_k = pltpu.make_async_copy(kn_ref, kn_out, new_sem.at[0])
    new_v = pltpu.make_async_copy(vn_ref, vn_out, new_sem.at[1])

    def chunk_copy(cache, dst, sem, seq, slot, c):
        rows = pl.ds(pl.multiple_of(c * CHUNK, CHUNK), CHUNK)
        return pltpu.make_async_copy(cache.at[base + seq, 0, rows, :], dst.at[slot, rows, :], sem.at[slot])

    k_copy = functools.partial(chunk_copy, k_hbm, kl, k_sem)
    v_copy = functools.partial(chunk_copy, v_hbm, vl, v_sem)

    def fetch(seq, slot):
        chunks = (len_ref[base + seq] + CHUNK - 1) // CHUNK

        @pl.loop(0, chunks)
        def _(c):
            k_copy(seq, slot, c).start()
            v_copy(seq, slot, c).start()

    def scan(i, count):
        length = len_ref[base + i]
        lens_v[pl.ds(i, 1), :] = jnp.full((1, 128), length, jnp.int32)
        is_long = length > SHORT

        @pl.when(is_long)
        def _():
            lidx[count] = i

            @pl.when(count < SLOTS)
            def _():
                fetch(i, count)

        return count + is_long.astype(jnp.int32)

    n_long = lax.fori_loop(0, LOCAL, scan, jnp.int32(0))
    new_k.start()
    new_v.start()

    own = pl.ds(pl.multiple_of(base, LOCAL), LOCAL)
    qf[...] = q_ref[...].astype(F32)
    knf[...] = kn_ref[own, :].astype(F32)
    vnf[...] = vn_ref[own, :].astype(F32)

    short_k.wait()
    short_v.wait()
    col = lax.broadcasted_iota(jnp.int32, (GROUP, GROUP * SHORT), 1)
    row = lax.broadcasted_iota(jnp.int32, (GROUP, GROUP * SHORT), 0)
    same = (col // SHORT) == row
    slot_pos = col % SHORT
    for g in range(LOCAL // GROUP):
        seqs = pl.ds(g * GROUP, GROUP)
        qb = q_ref[:, seqs, :].reshape(HEADS * GROUP, HD)
        kb = ks[seqs].reshape(GROUP * SHORT, HD)
        vb = vs[seqs].reshape(GROUP * SHORT, HD)
        s = lax.dot_general(qb, kb, DIMS_T, preferred_element_type=F32) * SCALE
        valid = same & (slot_pos < lens_v[seqs, 0:1])
        s = jnp.where(valid[None], s.reshape(HEADS, GROUP, GROUP * SHORT), -jnp.inf)
        s_new = jnp.sum(qf[:, seqs, :] * knf[seqs, :][None], axis=-1, keepdims=True) * SCALE
        m = jnp.maximum(jnp.max(s, axis=-1, keepdims=True), s_new)
        e = jnp.exp(s - m)
        e_new = jnp.exp(s_new - m)
        total = jnp.sum(e, axis=-1, keepdims=True) + e_new
        num = jnp.dot(e.astype(BF).reshape(HEADS * GROUP, GROUP * SHORT), vb, preferred_element_type=F32)
        num = num.reshape(HEADS, GROUP, HD) + e_new.astype(BF).astype(F32) * vnf[seqs, :][None]
        acc[:, seqs, :] = num / total

    @pl.loop(0, n_long)
    def _(i):
        seq = lidx[i]
        slot = i % SLOTS
        length = len_ref[base + seq]
        chunks = (length + CHUNK - 1) // CHUNK
        at = pl.ds(seq, 1)
        for n in range(1, MAXLEN // CHUNK + 1):
            @pl.when(chunks == n)
            def _():
                for c in range(n):
                    k_copy(seq, slot, c).wait()
                q8 = jnp.concatenate([qf[h, at, :] for h in range(HEADS)], axis=0)
                s = lax.dot_general(q8.astype(BF), kl[slot, pl.ds(0, n * CHUNK), :], DIMS_T, preferred_element_type=F32) * SCALE
                pos = lax.broadcasted_iota(jnp.int32, s.shape, 1)
                s = jnp.where(pos < length, s, -jnp.inf)
                s_new = jnp.sum(q8 * knf[at, :], axis=-1, keepdims=True) * SCALE
                m = jnp.maximum(jnp.max(s, axis=-1, keepdims=True), s_new)
                e = jnp.exp(s - m)
                e_new = jnp.exp(s_new - m)
                total = jnp.sum(e, axis=-1, keepdims=True) + e_new
                for c in range(n):
                    v_copy(seq, slot, c).wait()
                num = jnp.dot(e.astype(BF), vl[slot, pl.ds(0, n * CHUNK), :], preferred_element_type=F32)
                num = num + e_new.astype(BF).astype(F32) * vnf[at, :]
                out = num / total
                for h in range(HEADS):
                    acc[h, at, :] = out[h:h + 1, :]

        @pl.when(i + SLOTS < n_long)
        def _():
            fetch(lidx[i + SLOTS], slot)

    o_ref[...] = acc[...].astype(BF)
    new_k.wait()
    new_v.wait()


def attend(lengths, q, k_new, v_new, k_cache, v_cache):
    rows = k_new.shape[0]
    any_spec = pl.BlockSpec(memory_space=pl.ANY)
    vmem_spec = pl.BlockSpec(memory_space=pltpu.VMEM)
    return pl.pallas_call(
        attend_kernel,
        out_shape=(
            jax.ShapeDtypeStruct((HEADS, LOCAL, HD), BF),
            jax.ShapeDtypeStruct((rows, HD), BF),
            jax.ShapeDtypeStruct((rows, HD), BF),
        ),
        in_specs=[pl.BlockSpec(memory_space=pltpu.SMEM), vmem_spec, vmem_spec, vmem_spec, any_spec, any_spec],
        out_specs=(vmem_spec, any_spec, any_spec),
        scratch_shapes=[
            pltpu.VMEM((LOCAL, SHORT, HD), BF),
            pltpu.VMEM((LOCAL, SHORT, HD), BF),
            pltpu.VMEM((SLOTS, MAXLEN, HD), BF),
            pltpu.VMEM((SLOTS, MAXLEN, HD), BF),
            pltpu.VMEM((HEADS, LOCAL, HD), F32),
            pltpu.VMEM((LOCAL, HD), F32),
            pltpu.VMEM((LOCAL, HD), F32),
            pltpu.VMEM((HEADS, LOCAL, HD), F32),
            pltpu.VMEM((LOCAL, 128), jnp.int32),
            pltpu.SMEM((LOCAL,), jnp.int32),
            pltpu.SemaphoreType.DMA((2,)),
            pltpu.SemaphoreType.DMA((SLOTS,)),
            pltpu.SemaphoreType.DMA((SLOTS,)),
            pltpu.SemaphoreType.DMA((2,)),
        ],
        compiler_params=pltpu.CompilerParams(vmem_limit_bytes=48 * 2 ** 20),
        cost_estimate=pl.CostEstimate(flops=2 * 10 ** 9, bytes_accessed=10 ** 7, transcendentals=10 ** 6),
        name="attend",
    )(lengths, q, k_new, v_new, k_cache, v_cache)


HALF = HEADS // 2
X, Y, D, S = 2, 4, 6, 1


def output_kernel(o_ref, wc_ref, x_hbm, y_ref, og, xc, load_sem, os, orr, ys, yr):
    me, _, _, k = coords()
    cols = pl.ds(pl.multiple_of(me * HD, HD), HD)
    load_x = pltpu.make_async_copy(x_hbm.at[:, cols], xc, load_sem)
    load_x.start()
    entry_barrier((X, Y, S))
    started = []

    def o_copy(owner_rel, half, to, index):
        owner = peer(owner_rel)
        part = pl.ds(0, HEADS) if half is None else pl.ds(half * HALF, HALF)
        ref = og.at[owner, part]
        return remote(o_ref.at[part] if owner_rel == 0 else ref, ref, os.at[index], orr.at[index], to)

    def go(copy):
        copy.start()
        started.append(copy)

    def recv_o(owner_rel, half, to, index):
        o_copy(owner_rel, half, to, index).wait_recv()

    go(o_copy(0, 0, X, 0))
    go(o_copy(0, 1, Y, 1))
    go(o_copy(0, 1, X, 2))
    go(o_copy(0, 0, Y, 3))
    go(o_copy(0, None, S, 4))

    og[me] = o_ref[...]
    load_x.wait()

    def y_copy(col_rel, chip_rel, core, to, index):
        column = peer(col_rel)
        chip = peer(chip_rel) // 2
        first = chip * 2 + (0 if core is None else core)
        rows = pl.ds(pl.multiple_of(first * LOCAL, LOCAL), LOCAL if core is not None else 2 * LOCAL)
        ref = y_ref.at[rows, pl.ds(pl.multiple_of(column * HD, HD), HD)]
        return remote(ref, ref, ys.at[index], yr.at[index], to)

    def compute(step, chip_rel):
        chip = peer(chip_rel) // 2
        total = jnp.zeros((2 * LOCAL, HD), F32)
        for h in range(HEADS):
            lhs = og[pl.ds(chip * 2, 2), h].reshape(2 * LOCAL, HD)
            total = total + jnp.dot(lhs, wc_ref[pl.ds(h * HD, HD), :], preferred_element_type=F32)
        rows = pl.ds(pl.multiple_of(chip * 2 * LOCAL, 2 * LOCAL), 2 * LOCAL)
        y_ref[rows, cols] = (xc[rows, :].astype(F32) + total).astype(BF)
        b = step * 11
        go(y_copy(0, chip_rel, 0, X, b + 0))
        go(y_copy(0, chip_rel, 1, Y, b + 1))
        go(y_copy(0, chip_rel, 1, X, b + 2))
        go(y_copy(0, chip_rel, 0, Y, b + 3))
        go(y_copy(0, chip_rel, None, S, b + 4))

    recv_o(S, None, S, 4)
    compute(0, 0)
    recv_o(X, 0, X, 0)
    go(o_copy(X, 0, Y, 5))
    recv_o(Y, 1, Y, 1)
    go(o_copy(Y, 1, X, 6))
    recv_o(X, 1, X, 2)
    go(o_copy(X, None, S, 7))
    recv_o(Y, 0, Y, 3)
    go(o_copy(Y, None, S, 8))
    recv_o(X + S, None, S, 7)
    compute(1, X)
    recv_o(Y + S, None, S, 8)
    compute(2, Y)
    recv_o(D, 0, Y, 5)
    go(o_copy(D, 0, S, 9))
    recv_o(D, 1, X, 6)
    go(o_copy(D, 1, S, 10))
    recv_o(D + S, 0, S, 9)
    recv_o(D + S, 1, S, 10)
    compute(3, D)

    def xor(a, b):
        return ((a // 4 + b // 4) % 2) * 4 + ((a // 2 + b // 2) % 2) * 2 + (a + b) % 2

    order = (0, X, Y, D)
    for step, rel in enumerate(order):
        b = step * 11
        at_x, at_y, at_d = xor(rel, X), xor(rel, Y), xor(rel, D)
        y_copy(X, at_x, 0, X, b + 0).wait_recv()
        go(y_copy(X, at_x, 0, Y, b + 5))
        y_copy(Y, at_y, 1, Y, b + 1).wait_recv()
        go(y_copy(Y, at_y, 1, X, b + 6))
        y_copy(X, at_x, 1, X, b + 2).wait_recv()
        go(y_copy(X, at_x, None, S, b + 7))
        y_copy(Y, at_y, 0, Y, b + 3).wait_recv()
        go(y_copy(Y, at_y, None, S, b + 8))
    for step, rel in enumerate(order):
        b = step * 11
        at_d = xor(rel, D)
        y_copy(D, at_d, 0, Y, b + 5).wait_recv()
        go(y_copy(D, at_d, 0, S, b + 9))
        y_copy(D, at_d, 1, X, b + 6).wait_recv()
        go(y_copy(D, at_d, 1, S, b + 10))
    for step, rel in enumerate(order):
        b = step * 11
        at_x, at_y, at_d = xor(rel, X), xor(rel, Y), xor(rel, D)
        y_copy(S, rel, None, S, b + 4).wait_recv()
        y_copy(X + S, at_x, None, S, b + 7).wait_recv()
        y_copy(Y + S, at_y, None, S, b + 8).wait_recv()
        y_copy(D + S, at_d, 0, S, b + 9).wait_recv()
        y_copy(D + S, at_d, 1, S, b + 10).wait_recv()
    for copy in started:
        copy.wait_send()


def output(o, wc, x):
    rows, width = x.shape
    hbm_spec = pl.BlockSpec(memory_space=pltpu.HBM)
    vmem_spec = pl.BlockSpec(memory_space=pltpu.VMEM)
    return pl.pallas_call(
        output_kernel,
        out_shape=jax.ShapeDtypeStruct((rows, width), BF),
        in_specs=[vmem_spec, vmem_spec, hbm_spec],
        out_specs=vmem_spec,
        scratch_shapes=[
            pltpu.VMEM((8, HEADS, LOCAL, HD), BF),
            pltpu.VMEM((rows, HD), BF),
            pltpu.SemaphoreType.DMA,
            pltpu.SemaphoreType.DMA((11,)),
            pltpu.SemaphoreType.DMA((11,)),
            pltpu.SemaphoreType.DMA((44,)),
            pltpu.SemaphoreType.DMA((44,)),
        ],
        compiler_params=pltpu.CompilerParams(collective_id=1, has_side_effects=True, vmem_limit_bytes=40 * 2 ** 20),
        name="output",
    )(o, wc, x)


def solution(mesh):
    def local_step(x, w_query, w_key, w_value, w_out, k_cache, v_cache, lengths):
        q, k_new, v_new, w_cols = project(x, w_query, w_key, w_value, w_out)
        o, k_new, v_new = attend(lengths, q, k_new, v_new, k_cache, v_cache)
        y = output(o, w_cols, x)
        return y, k_new[:, None, :], v_new[:, None, :]

    rows_spec = P("replica")
    return jax.shard_map(
        local_step,
        mesh=mesh,
        in_specs=(P("replica", None), P(None, "model"), P(), P(), P("model", None), rows_spec, rows_spec, rows_spec),
        out_specs=(rows_spec, rows_spec, rows_spec),
        check_vma=False,
    )
```

```python
import functools

import jax
import jax.numpy as jnp
from jax import lax
from jax.experimental import pallas as pl
from jax.experimental.pallas import tpu as pltpu
from jax.sharding import PartitionSpec as P

BF = jnp.bfloat16
F32 = jnp.float32
HEADS = 8
PAIR = 2
HD = 256
LOCAL = 256
SHORT = 32
GROUP = 16
UNROLL = 4
CHUNK = 256
MAXLEN = 2048
SLOTS = 16
SCALE = HD ** -0.5
DIMS_T = (((1,), (1,)), ((), ()))
MIB = 2 ** 20
SIB, X, Y, D = 1, 2, 4, 6


def coords():
    me = lax.axis_index("model")
    return me, me // 4, (me // 2) % 2, me % 2


def peer(rel):
    _, y, x, k = coords()
    dy, dx, dk = rel // 4, (rel // 2) % 2, rel % 2
    return (((y + dy) % 2) * 2 + (x + dx) % 2) * 2 + (k + dk) % 2


def span(index, size):
    return pl.ds(pl.multiple_of(index * size, size), size)


def entry_barrier(rels):
    barrier = pltpu.get_barrier_semaphore()
    for rel in rels:
        pl.semaphore_signal(barrier, inc=1, device_id={"model": peer(rel)}, device_id_type=pl.DeviceIdType.MESH)
    pl.semaphore_wait(barrier, len(rels))


def remote(src, dst, send_sem, recv_sem, rel):
    return pltpu.make_async_remote_copy(
        src_ref=src, dst_ref=dst, send_sem=send_sem, recv_sem=recv_sem,
        device_id={"model": peer(rel)}, device_id_type=pl.DeviceIdType.MESH)


def project_kernel(x_hbm, wq_hbm, wk_hbm, wv_hbm, wo_hbm, k_hbm, v_hbm,
                   q_out, kn_out, vn_out, ks_out, vs_out, wx_out, wy_out, wd_out,
                   x_v, wq_v, wk_v, wv_v, q_v, in_sem, ss, rs):
    _, _, _, k = coords()
    other = peer(SIB) % 2
    mine, theirs = span(k, LOCAL), span(other, LOCAL)
    pairs = [
        (wq_hbm, wq_v),
        (x_hbm.at[theirs, :], x_v.at[theirs, :]),
        (x_hbm.at[mine, :], x_v.at[mine, :]),
        (wk_hbm, wk_v),
        (wv_hbm, wv_v),
    ]
    for rel, dst in ((D, wd_out), (X, wx_out), (Y, wy_out)):
        pairs.append((wo_hbm.at[:, span(peer(rel) // 2, 2 * HD)], dst))
    pairs.append((k_hbm.at[mine, 0, pl.ds(0, SHORT), :], ks_out))
    pairs.append((v_hbm.at[mine, 0, pl.ds(0, SHORT), :], vs_out))
    loads = [pltpu.make_async_copy(src, dst, in_sem.at[i]) for i, (src, dst) in enumerate(pairs)]
    for load in loads:
        load.start()
    entry_barrier((SIB,))
    loads[0].wait()
    loads[1].wait()
    q_v[...] = jnp.dot(x_v[theirs, :], wq_v[...], preferred_element_type=F32).astype(BF)
    copies = [remote(q_v, q_out.at[k], ss.at[0], rs.at[0], SIB)]
    copies[0].start()
    loads[2].wait()
    q_out[k] = jnp.dot(x_v[mine, :], wq_v[...], preferred_element_type=F32).astype(BF)
    for i, (w_v, out) in enumerate(((wk_v, kn_out), (wv_v, vn_out))):
        loads[3 + i].wait()
        out[mine, :] = jnp.dot(x_v[mine, :], w_v[...], preferred_element_type=F32).astype(BF)
        copy = remote(out.at[mine, :], out.at[mine, :], ss.at[1 + i], rs.at[1 + i], SIB)
        copy.start()
        copies.append(copy)
    for copy in copies:
        copy.wait_send()
    remote(q_v, q_out.at[other], ss.at[0], rs.at[0], SIB).wait_recv()
    for i, out in enumerate((kn_out, vn_out)):
        remote(out.at[theirs, :], out.at[theirs, :], ss.at[1 + i], rs.at[1 + i], SIB).wait_recv()
    for load in loads[5:]:
        load.wait()


def project(x, wq, wk, wv, wo, k_cache, v_cache):
    rows, depth = x.shape
    hbm_spec = pl.BlockSpec(memory_space=pltpu.HBM)
    vmem_spec = pl.BlockSpec(memory_space=pltpu.VMEM)
    piece = jax.ShapeDtypeStruct((HD, 2 * HD), BF)
    return pl.pallas_call(
        project_kernel,
        out_shape=(
            jax.ShapeDtypeStruct((PAIR, LOCAL, HD), BF),
            jax.ShapeDtypeStruct((rows, HD), BF),
            jax.ShapeDtypeStruct((rows, HD), BF),
            jax.ShapeDtypeStruct((LOCAL, SHORT, HD), BF),
            jax.ShapeDtypeStruct((LOCAL, SHORT, HD), BF),
            piece, piece, piece,
        ),
        in_specs=[hbm_spec] * 7,
        out_specs=(vmem_spec,) * 8,
        scratch_shapes=[
            pltpu.VMEM((rows, depth), BF),
            pltpu.VMEM((depth, HD), BF),
            pltpu.VMEM((depth, HD), BF),
            pltpu.VMEM((depth, HD), BF),
            pltpu.VMEM((LOCAL, HD), BF),
            pltpu.SemaphoreType.DMA((10,)),
            pltpu.SemaphoreType.DMA((3,)),
            pltpu.SemaphoreType.DMA((3,)),
        ],
        compiler_params=pltpu.CompilerParams(collective_id=0, has_side_effects=True, vmem_limit_bytes=A_LIMIT * MIB),
        name="project",
    )(x, wq, wk, wv, wo, k_cache, v_cache)


def softmax_parts(s, s_new):
    m = jnp.maximum(jnp.max(s, axis=-1, keepdims=True), s_new)
    e = jnp.exp(s - m)
    e_new = jnp.exp(s_new - m)
    total = jnp.sum(e, axis=-1, keepdims=True) + e_new
    return e.astype(BF), e_new.astype(BF).astype(F32), total


def attend_kernel(len_ref, q_ref, kn_ref, vn_ref, ks, vs, k_hbm, v_hbm, o_ref, kn_out, vn_out,
                  kl, vl, qf, knf, vnf, acc, lens_v, lidx, k_sem, v_sem, new_sem):
    base = (lax.axis_index("model") % 2) * LOCAL
    new_k = pltpu.make_async_copy(kn_ref, kn_out, new_sem.at[0])
    new_v = pltpu.make_async_copy(vn_ref, vn_out, new_sem.at[1])

    def part_copy(cache, dst, sem, seq, slot, first, rows):
        at = pl.ds(pl.multiple_of(first, CHUNK), rows)
        return pltpu.make_async_copy(cache.at[base + seq, 0, at, :], dst.at[slot, at, :], sem.at[slot])

    k_copy = functools.partial(part_copy, k_hbm, kl, k_sem)
    v_copy = functools.partial(part_copy, v_hbm, vl, v_sem)

    def fetch(seq, slot):
        chunks = (len_ref[base + seq] + CHUNK - 1) // CHUNK
        for copy in (k_copy, v_copy):
            first = jnp.int32(0)
            for size in (8, 4, 2, 1):
                take = chunks - first // CHUNK >= size

                @pl.when(take)
                def _():
                    copy(seq, slot, first, size * CHUNK).start()

                first = first + jnp.where(take, size * CHUNK, 0)

    def scan(block, count):
        for j in range(8):
            i = block * 8 + j
            length = len_ref[base + i]
            lens_v[pl.ds(i, 1), :] = jnp.full((1, 128), length, jnp.int32)
            lidx[count] = i
            count = count + jnp.where(length > SHORT, 1, 0)
        return count

    n_long = lax.fori_loop(0, LOCAL // 8, scan, jnp.int32(0))

    @pl.loop(0, jnp.minimum(n_long, SLOTS))
    def _(i):
        fetch(lidx[i], i)

    new_k.start()
    new_v.start()
    own = span(lax.axis_index("model") % 2, LOCAL)
    qf[...] = q_ref[...].astype(F32)
    knf[...] = kn_ref[own, :].astype(F32)
    vnf[...] = vn_ref[own, :].astype(F32)

    width = GROUP * SHORT
    col = lax.broadcasted_iota(jnp.int32, (GROUP, width), 1)
    same = (col // SHORT) == lax.broadcasted_iota(jnp.int32, (GROUP, width), 0)
    slot_pos = col % SHORT

    @pl.loop(0, LOCAL // GROUP // UNROLL)
    def _(block):
        for u in range(UNROLL):
            seqs = span(block * UNROLL + u, GROUP)
            qb = q_ref[:, seqs, :].reshape(PAIR * GROUP, HD)
            kb = ks[seqs].reshape(width, HD)
            vb = vs[seqs].reshape(width, HD)
            s = lax.dot_general(qb, kb, DIMS_T, preferred_element_type=F32) * SCALE
            valid = same & (slot_pos < lens_v[seqs, 0:1])
            s = jnp.where(valid[None], s.reshape(PAIR, GROUP, width), -jnp.inf)
            s_new = jnp.sum(qf[:, seqs, :] * knf[seqs, :][None], axis=-1, keepdims=True) * SCALE
            e, e_new, total = softmax_parts(s, s_new)
            num = jnp.dot(e.reshape(PAIR * GROUP, width), vb, preferred_element_type=F32)
            acc[:, seqs, :] = (num.reshape(PAIR, GROUP, HD) + e_new * vnf[seqs, :][None]) / total

    @pl.loop(0, n_long)
    def _(i):
        seq = lidx[i]
        slot = i % SLOTS
        length = len_ref[base + seq]
        chunks = (length + CHUNK - 1) // CHUNK
        at = pl.ds(seq, 1)
        for n in range(1, MAXLEN // CHUNK + 1):
            @pl.when(chunks == n)
            def _():
                rows = n * CHUNK
                k_copy(seq, slot, 0, rows).wait()
                q8 = jnp.concatenate([qf[h, at, :] for h in range(PAIR)], axis=0)
                s = lax.dot_general(q8.astype(BF), kl[slot, pl.ds(0, rows), :], DIMS_T, preferred_element_type=F32) * SCALE
                s = jnp.where(lax.broadcasted_iota(jnp.int32, s.shape, 1) < length, s, -jnp.inf)
                s_new = jnp.sum(q8 * knf[at, :], axis=-1, keepdims=True) * SCALE
                e, e_new, total = softmax_parts(s, s_new)
                v_copy(seq, slot, 0, rows).wait()
                num = jnp.dot(e, vl[slot, pl.ds(0, rows), :], preferred_element_type=F32)
                out = (num + e_new * vnf[at, :]) / total
                for h in range(PAIR):
                    acc[h, at, :] = out[h:h + 1, :]

        @pl.when(i + SLOTS < n_long)
        def _():
            fetch(lidx[i + SLOTS], slot)

    o_ref[...] = acc[...].astype(BF)
    new_k.wait()
    new_v.wait()


def attend(lengths, q, k_new, v_new, ks, vs, k_cache, v_cache):
    rows = k_new.shape[0]
    any_spec = pl.BlockSpec(memory_space=pl.ANY)
    vmem_spec = pl.BlockSpec(memory_space=pltpu.VMEM)
    return pl.pallas_call(
        attend_kernel,
        out_shape=(
            jax.ShapeDtypeStruct((PAIR, LOCAL, HD), BF),
            jax.ShapeDtypeStruct((rows, HD), BF),
            jax.ShapeDtypeStruct((rows, HD), BF),
        ),
        in_specs=[pl.BlockSpec(memory_space=pltpu.SMEM)] + [vmem_spec] * 5 + [any_spec] * 2,
        out_specs=(vmem_spec, any_spec, any_spec),
        scratch_shapes=[
            pltpu.VMEM((SLOTS, MAXLEN, HD), BF),
            pltpu.VMEM((SLOTS, MAXLEN, HD), BF),
            pltpu.VMEM((PAIR, LOCAL, HD), F32),
            pltpu.VMEM((LOCAL, HD), F32),
            pltpu.VMEM((LOCAL, HD), F32),
            pltpu.VMEM((PAIR, LOCAL, HD), F32),
            pltpu.VMEM((LOCAL, 128), jnp.int32),
            pltpu.SMEM((LOCAL + 8,), jnp.int32),
            pltpu.SemaphoreType.DMA((SLOTS,)),
            pltpu.SemaphoreType.DMA((SLOTS,)),
            pltpu.SemaphoreType.DMA((2,)),
        ],
        compiler_params=pltpu.CompilerParams(vmem_limit_bytes=B_LIMIT * MIB),
        cost_estimate=pl.CostEstimate(flops=4 * 10 ** 9, bytes_accessed=3 * 10 ** 7, transcendentals=10 ** 6),
        name="attend",
    )(lengths, q, k_new, v_new, ks, vs, k_cache, v_cache)


PIECES = 4
PIECE = LOCAL // PIECES
MSGS = 8


def output_kernel(o_ref, wo_hbm, wx_ref, wy_ref, wd_ref, x_hbm, y_ref, og, wc, xc, load_sem, wss, wrs, ss, rs):
    me, _, _, k = coords()
    other = peer(SIB) % 2
    load_x = pltpu.make_async_copy(x_hbm.at[:, :, span(me, HD)], xc, load_sem.at[0])
    load_x.start()
    w_loads = [pltpu.make_async_copy(wo_hbm.at[:, span(me, HD)], wc.at[me], load_sem.at[1])]
    w_copies = [remote(wo_hbm.at[:, span(peer(SIB), HD)], wc.at[me], wss.at[0], wrs.at[0], SIB)]
    w_recvs = [remote(wo_hbm.at[:, span(me, HD)], wc.at[peer(SIB)], wss.at[0], wrs.at[0], SIB)]
    for i, (rel, ref) in enumerate(((X, wx_ref), (Y, wy_ref), (D, wd_ref))):
        w_loads.append(pltpu.make_async_copy(ref.at[:, span(k, HD)], wc.at[peer(rel)], load_sem.at[2 + i]))
        w_copies.append(remote(ref.at[:, span(other, HD)], wc.at[peer(rel)], wss.at[1 + i], wrs.at[1 + i], SIB))
        w_recvs.append(remote(ref.at[:, span(other, HD)], wc.at[peer(rel + SIB)], wss.at[1 + i], wrs.at[1 + i], SIB))
    for load in w_loads:
        load.start()
    entry_barrier((X, Y, SIB))

    def item(kind, owner_rel, p, half):
        owner = peer(owner_rel)
        part = pl.ds(0, 2) if half is None else pl.ds(half, 1)
        rows = span(p, PIECE)
        if kind == 0:
            return og.at[owner, part, rows, :]
        return y_ref.at[part, rows, span(owner, HD)]

    def copy(kind, owner_rel, p, half, to, message):
        index = (kind * PIECES + p) * MSGS + message
        dst = item(kind, owner_rel, p, half)
        src = o_ref.at[:, span(p, PIECE), :] if kind == 0 and owner_rel == 0 else dst
        return remote(src, dst, ss.at[index], rs.at[index], to)

    def send_own(kind, p):
        copy(kind, 0, p, None, X, 0).start()
        copy(kind, 0, p, None, Y, 1).start()
        copy(kind, 0, p, None, SIB, 2).start()

    def first_hop(kind, p):
        copy(kind, X, p, None, X, 0).wait_recv()
        copy(kind, X, p, 0, Y, 3).start()
        copy(kind, X, p, None, SIB, 5).start()
        copy(kind, Y, p, None, Y, 1).wait_recv()
        copy(kind, Y, p, 1, X, 4).start()
        copy(kind, Y, p, None, SIB, 6).start()

    def second_hop(kind, p):
        copy(kind, D, p, 0, Y, 3).wait_recv()
        copy(kind, D, p, 1, X, 4).wait_recv()
        copy(kind, D, p, None, SIB, 7).start()

    def from_sibling(kind, p):
        copy(kind, SIB, p, None, SIB, 2).wait_recv()
        copy(kind, X + SIB, p, None, SIB, 5).wait_recv()
        copy(kind, Y + SIB, p, None, SIB, 6).wait_recv()
        copy(kind, D + SIB, p, None, SIB, 7).wait_recv()

    def sent(kind, p):
        copy(kind, 0, p, None, X, 0).wait_send()
        copy(kind, 0, p, None, Y, 1).wait_send()
        copy(kind, 0, p, None, SIB, 2).wait_send()
        copy(kind, X, p, 0, Y, 3).wait_send()
        copy(kind, Y, p, 1, X, 4).wait_send()
        copy(kind, X, p, None, SIB, 5).wait_send()
        copy(kind, Y, p, None, SIB, 6).wait_send()
        copy(kind, D, p, None, SIB, 7).wait_send()

    def finish(p):
        second_hop(0, p)
        from_sibling(0, p)
        rows = span(p, PIECE)
        total = jnp.zeros((2 * PIECE, HD), F32)
        for chip in range(4):
            for j in range(PAIR):
                lhs = og[pl.ds(2 * chip, 2), j, rows, :].reshape(2 * PIECE, HD)
                total = total + jnp.dot(lhs, wc[2 * chip + j], preferred_element_type=F32)
        y_ref[:, rows, span(me, HD)] = (xc[:, rows, :].astype(F32) + total.reshape(2, PIECE, HD)).astype(BF)
        send_own(1, p)

    send_own(0, 0)
    send_own(0, 1)
    for c in w_copies:
        c.start()
    og[me] = o_ref[...]
    first_hop(0, 0)
    load_x.wait()
    for load in w_loads:
        load.wait()
    for c in w_recvs:
        c.wait_recv()

    def middle(p, carry):
        @pl.when(p + 1 < PIECES)
        def _():
            send_own(0, p + 1)

        first_hop(0, p)
        finish(p - 1)
        return carry

    lax.fori_loop(1, PIECES, middle, 0)
    finish(PIECES - 1)
    first_hop(1, 0)

    def last(p, carry):
        first_hop(1, p)
        second_hop(1, p - 1)
        return carry

    lax.fori_loop(1, PIECES, last, 0)
    second_hop(1, PIECES - 1)

    def drain(p, carry):
        from_sibling(1, p)
        sent(0, p)
        sent(1, p)
        return carry

    lax.fori_loop(0, PIECES, drain, 0)
    for c in w_copies:
        c.wait_send()


def output(o, wo, pieces, x):
    hbm_spec = pl.BlockSpec(memory_space=pltpu.HBM)
    vmem_spec = pl.BlockSpec(memory_space=pltpu.VMEM)
    return pl.pallas_call(
        output_kernel,
        out_shape=jax.ShapeDtypeStruct(x.shape, BF),
        in_specs=[vmem_spec] + [hbm_spec] * 5,
        out_specs=vmem_spec,
        scratch_shapes=[
            pltpu.VMEM((8, PAIR, LOCAL, HD), BF),
            pltpu.VMEM((HEADS, HD, HD), BF),
            pltpu.VMEM((2, LOCAL, HD), BF),
            pltpu.SemaphoreType.DMA((5,)),
            pltpu.SemaphoreType.DMA((4,)),
            pltpu.SemaphoreType.DMA((4,)),
            pltpu.SemaphoreType.DMA((2 * PIECES * MSGS,)),
            pltpu.SemaphoreType.DMA((2 * PIECES * MSGS,)),
        ],
        compiler_params=pltpu.CompilerParams(collective_id=1, has_side_effects=True, vmem_limit_bytes=C_LIMIT * MIB),
        name="output",
    )(o, wo, *pieces, x)


A_LIMIT, B_LIMIT, C_LIMIT = 24, 38, 24


def solution(mesh):
    devices = mesh.shape["model"]

    def to_chip(rel):
        return [(d, d ^ rel) for d in range(devices)]

    def local_step(x, w_query, w_key, w_value, w_out, k_cache, v_cache, lengths):
        in_hbm = [pltpu.with_memory_space_constraint(a, pltpu.HBM) for a in (x, w_query, w_key, w_value, w_out)]
        q, k_new, v_new, ks, vs, wx, wy, wd = project(*in_hbm, k_cache, v_cache)
        pieces = [lax.ppermute(w, "model", to_chip(rel)) for w, rel in ((wx, X), (wy, Y), (wd, D))]
        o, k_new, v_new = attend(lengths, q, k_new, v_new, ks, vs, k_cache, v_cache)
        y = output(o, in_hbm[4], pieces, pltpu.with_memory_space_constraint(x.reshape(2, LOCAL, -1), pltpu.HBM))
        return y.reshape(x.shape), k_new[:, None, :], v_new[:, None, :]

    rows_spec = P("replica")
    return jax.shard_map(
        local_step,
        mesh=mesh,
        in_specs=(P("replica", None), P(None, "model"), P(), P(), P("model", None), rows_spec, rows_spec, rows_spec),
        out_specs=(rows_spec, rows_spec, rows_spec),
        check_vma=False,
    )
```

```python
import functools

import jax
import jax.numpy as jnp
from jax import lax
from jax.experimental import pallas as pl
from jax.experimental.pallas import tpu as pltpu
from jax.sharding import PartitionSpec as P

BF = jnp.bfloat16
F32 = jnp.float32
HEADS = 8
PAIR = 2
HD = 256
LOCAL = 256
SHORT = 32
GROUP = 16
UNROLL = 4
CHUNK = 256
MAXLEN = 2048
SLOTS = 16
SCALE = HD ** -0.5
DIMS_T = (((1,), (1,)), ((), ()))
MIB = 2 ** 20
SIB, X, Y, D = 1, 2, 4, 6


def coords():
    me = lax.axis_index("model")
    return me, me // 4, (me // 2) % 2, me % 2


def peer(rel):
    _, y, x, k = coords()
    dy, dx, dk = rel // 4, (rel // 2) % 2, rel % 2
    return (((y + dy) % 2) * 2 + (x + dx) % 2) * 2 + (k + dk) % 2


def span(index, size):
    return pl.ds(pl.multiple_of(index * size, size), size)


def entry_barrier(rels):
    barrier = pltpu.get_barrier_semaphore()
    for rel in rels:
        pl.semaphore_signal(barrier, inc=1, device_id={"model": peer(rel)}, device_id_type=pl.DeviceIdType.MESH)
    pl.semaphore_wait(barrier, len(rels))


def remote(src, dst, send_sem, recv_sem, rel):
    return pltpu.make_async_remote_copy(
        src_ref=src, dst_ref=dst, send_sem=send_sem, recv_sem=recv_sem,
        device_id={"model": peer(rel)}, device_id_type=pl.DeviceIdType.MESH)


def project_kernel(x_hbm, wq_hbm, wk_hbm, wv_hbm, wo_hbm, k_hbm, v_hbm,
                   q_out, kn_out, vn_out, ks_out, vs_out, wx_out, wy_out, wd_out,
                   x_v, wq_v, wk_v, wv_v, wo_v, q_v, in_sem, out_sem, ss, rs):
    _, _, _, k = coords()
    other = peer(SIB) % 2
    mine, theirs = span(k, LOCAL), span(other, LOCAL)
    pairs = (
        (wq_hbm, wq_v),
        (x_hbm.at[theirs, :], x_v.at[theirs, :]),
        (x_hbm.at[mine, :], x_v.at[mine, :]),
        (wo_hbm, wo_v),
        (wk_hbm, wk_v),
        (wv_hbm, wv_v),
        (k_hbm.at[mine, 0, pl.ds(0, SHORT), :], ks_out),
        (v_hbm.at[mine, 0, pl.ds(0, SHORT), :], vs_out),
    )
    loads = [pltpu.make_async_copy(src, dst, in_sem.at[i]) for i, (src, dst) in enumerate(pairs)]
    for load in loads[:6]:
        load.start()
    entry_barrier((SIB,))
    loads[0].wait()
    loads[1].wait()
    q_v[...] = jnp.dot(x_v[theirs, :], wq_v[...], preferred_element_type=F32).astype(BF)
    copies = [remote(q_v, q_out.at[k], ss.at[0], rs.at[0], SIB)]
    copies[0].start()
    loads[2].wait()
    loads[6].start()
    loads[7].start()
    q_out[k] = jnp.dot(x_v[mine, :], wq_v[...], preferred_element_type=F32).astype(BF)
    loads[3].wait()
    stores = []
    for i, (rel, out) in enumerate(((D, wd_out), (X, wx_out), (Y, wy_out))):
        stores.append(pltpu.make_async_copy(wo_v.at[:, span(peer(rel) // 2, 2 * HD)], out, out_sem.at[i]))
        stores[-1].start()
    for i, (w_v, out) in enumerate(((wk_v, kn_out), (wv_v, vn_out))):
        loads[4 + i].wait()
        out[mine, :] = jnp.dot(x_v[mine, :], w_v[...], preferred_element_type=F32).astype(BF)
        copy = remote(out.at[mine, :], out.at[mine, :], ss.at[1 + i], rs.at[1 + i], SIB)
        copy.start()
        copies.append(copy)
    for copy in copies:
        copy.wait_send()
    remote(q_v, q_out.at[other], ss.at[0], rs.at[0], SIB).wait_recv()
    for i, out in enumerate((kn_out, vn_out)):
        remote(out.at[theirs, :], out.at[theirs, :], ss.at[1 + i], rs.at[1 + i], SIB).wait_recv()
    for wait in loads[6:] + stores:
        wait.wait()


def project(x, wq, wk, wv, wo, k_cache, v_cache):
    rows, depth = x.shape
    hbm_spec = pl.BlockSpec(memory_space=pltpu.HBM)
    vmem_spec = pl.BlockSpec(memory_space=pltpu.VMEM)
    piece = jax.ShapeDtypeStruct((HD, 2 * HD), BF)
    return pl.pallas_call(
        project_kernel,
        out_shape=(
            jax.ShapeDtypeStruct((PAIR, LOCAL, HD), BF),
            jax.ShapeDtypeStruct((rows, HD), BF),
            jax.ShapeDtypeStruct((rows, HD), BF),
            jax.ShapeDtypeStruct((LOCAL, SHORT, HD), BF),
            jax.ShapeDtypeStruct((LOCAL, SHORT, HD), BF),
            piece, piece, piece,
        ),
        in_specs=[hbm_spec] * 7,
        out_specs=(vmem_spec,) * 5 + (hbm_spec,) * 3,
        scratch_shapes=[
            pltpu.VMEM((rows, depth), BF),
            pltpu.VMEM((depth, HD), BF),
            pltpu.VMEM((depth, HD), BF),
            pltpu.VMEM((depth, HD), BF),
            pltpu.VMEM(wo.shape, BF),
            pltpu.VMEM((LOCAL, HD), BF),
            pltpu.SemaphoreType.DMA((8,)),
            pltpu.SemaphoreType.DMA((3,)),
            pltpu.SemaphoreType.DMA((3,)),
            pltpu.SemaphoreType.DMA((3,)),
        ],
        compiler_params=pltpu.CompilerParams(collective_id=0, has_side_effects=True, vmem_limit_bytes=A_LIMIT * MIB),
        name="project",
    )(x, wq, wk, wv, wo, k_cache, v_cache)


def softmax_parts(s, s_new):
    m = jnp.maximum(jnp.max(s, axis=-1, keepdims=True), s_new)
    e = jnp.exp(s - m)
    e_new = jnp.exp(s_new - m)
    total = jnp.sum(e, axis=-1, keepdims=True) + e_new
    return e.astype(BF), e_new.astype(BF).astype(F32), total


def attend_kernel(len_ref, q_ref, kn_ref, vn_ref, ks, vs, k_hbm, v_hbm, o_ref, kn_out, vn_out,
                  kl, vl, qf, knf, vnf, acc, lens_v, lidx, k_sem, v_sem, new_sem):
    base = (lax.axis_index("model") % 2) * LOCAL
    new_k = pltpu.make_async_copy(kn_ref, kn_out, new_sem.at[0])
    new_v = pltpu.make_async_copy(vn_ref, vn_out, new_sem.at[1])

    def part_copy(cache, dst, sem, seq, slot, first, rows):
        at = pl.ds(pl.multiple_of(first, CHUNK), rows)
        return pltpu.make_async_copy(cache.at[base + seq, 0, at, :], dst.at[slot, at, :], sem.at[slot])

    k_copy = functools.partial(part_copy, k_hbm, kl, k_sem)
    v_copy = functools.partial(part_copy, v_hbm, vl, v_sem)

    def fetch(seq, slot):
        chunks = (len_ref[base + seq] + CHUNK - 1) // CHUNK
        for copy in (k_copy, v_copy):
            first = jnp.int32(0)
            for size in (8, 4, 2, 1):
                take = chunks - first // CHUNK >= size

                @pl.when(take)
                def _():
                    copy(seq, slot, first, size * CHUNK).start()

                first = first + jnp.where(take, size * CHUNK, 0)

    def scan(block, count):
        first = count
        for j in range(8):
            i = block * 8 + j
            length = len_ref[base + i]
            lens_v[pl.ds(i, 1), :] = jnp.full((1, 128), length, jnp.int32)
            lidx[count] = i
            count = count + jnp.where(length > SHORT, 1, 0)

        @pl.loop(jnp.minimum(first, SLOTS), jnp.minimum(count, SLOTS))
        def _(i):
            fetch(lidx[i], i)

        return count

    n_long = lax.fori_loop(0, LOCAL // 8, scan, jnp.int32(0))
    new_k.start()
    new_v.start()
    own = span(lax.axis_index("model") % 2, LOCAL)
    qf[...] = q_ref[...].astype(F32)
    knf[...] = kn_ref[own, :].astype(F32)
    vnf[...] = vn_ref[own, :].astype(F32)

    width = GROUP * SHORT
    col = lax.broadcasted_iota(jnp.int32, (GROUP, width), 1)
    same = (col // SHORT) == lax.broadcasted_iota(jnp.int32, (GROUP, width), 0)
    slot_pos = col % SHORT

    @pl.loop(0, LOCAL // GROUP // UNROLL)
    def _(block):
        for u in range(UNROLL):
            seqs = span(block * UNROLL + u, GROUP)
            qb = q_ref[:, seqs, :].reshape(PAIR * GROUP, HD)
            kb = ks[seqs].reshape(width, HD)
            vb = vs[seqs].reshape(width, HD)
            s = lax.dot_general(qb, kb, DIMS_T, preferred_element_type=F32) * SCALE
            valid = same & (slot_pos < lens_v[seqs, 0:1])
            s = jnp.where(valid[None], s.reshape(PAIR, GROUP, width), -jnp.inf)
            s_new = jnp.sum(qf[:, seqs, :] * knf[seqs, :][None], axis=-1, keepdims=True) * SCALE
            e, e_new, total = softmax_parts(s, s_new)
            num = jnp.dot(e.reshape(PAIR * GROUP, width), vb, preferred_element_type=F32)
            acc[:, seqs, :] = (num.reshape(PAIR, GROUP, HD) + e_new * vnf[seqs, :][None]) / total

    def chunks_of(i):
        return (len_ref[base + lidx[i]] + CHUNK - 1) // CHUNK

    def one_long(i, rows):
        seq = lidx[i]
        slot = i % SLOTS
        at = pl.ds(seq, 1)
        q8 = jnp.concatenate([qf[h, at, :] for h in range(PAIR)], axis=0)
        s = lax.dot_general(q8.astype(BF), kl[slot, pl.ds(0, rows), :], DIMS_T, preferred_element_type=F32) * SCALE
        s = jnp.where(lax.broadcasted_iota(jnp.int32, s.shape, 1) < len_ref[base + seq], s, -jnp.inf)
        s_new = jnp.sum(q8 * knf[at, :], axis=-1, keepdims=True) * SCALE
        e, e_new, total = softmax_parts(s, s_new)
        num = jnp.dot(e, vl[slot, pl.ds(0, rows), :], preferred_element_type=F32)
        return seq, (num + e_new * vnf[at, :]) / total

    def wait_and_clear(i, chunks, rows):
        slot = i % SLOTS
        for copy in (k_copy, v_copy):
            @pl.loop(0, chunks)
            def _(c):
                copy(0, slot, 0, CHUNK).wait()

        @pl.loop(chunks, rows // CHUNK)
        def _(c):
            vl[slot, span(c, CHUNK), :] = jnp.zeros((CHUNK, HD), BF)

    @pl.loop(0, (n_long + 1) // 2)
    def _(pair):
        a = pair * 2
        b = jnp.minimum(a + 1, n_long - 1)
        chunks_a, chunks_b = chunks_of(a), chunks_of(b)
        most = jnp.maximum(chunks_a, chunks_b)
        wait_and_clear(a, chunks_a, most * CHUNK)

        @pl.when(b > a)
        def _():
            wait_and_clear(b, chunks_b, most * CHUNK)

        for n in range(1, MAXLEN // CHUNK + 1):
            @pl.when(most == n)
            def _():
                results = [one_long(i, n * CHUNK) for i in (a, b)]
                for seq, out in results:
                    for h in range(PAIR):
                        acc[h, pl.ds(seq, 1), :] = out[h:h + 1, :]

        for i in (a, a + 1):
            @pl.when(i + SLOTS < n_long)
            def _():
                fetch(lidx[i + SLOTS], i % SLOTS)

    o_ref[...] = acc[...].astype(BF)
    new_k.wait()
    new_v.wait()


def attend(lengths, q, k_new, v_new, ks, vs, k_cache, v_cache):
    rows = k_new.shape[0]
    any_spec = pl.BlockSpec(memory_space=pl.ANY)
    vmem_spec = pl.BlockSpec(memory_space=pltpu.VMEM)
    return pl.pallas_call(
        attend_kernel,
        out_shape=(
            jax.ShapeDtypeStruct((PAIR, LOCAL, HD), BF),
            jax.ShapeDtypeStruct((rows, HD), BF),
            jax.ShapeDtypeStruct((rows, HD), BF),
        ),
        in_specs=[pl.BlockSpec(memory_space=pltpu.SMEM)] + [vmem_spec] * 5 + [any_spec] * 2,
        out_specs=(vmem_spec, any_spec, any_spec),
        scratch_shapes=[
            pltpu.VMEM((SLOTS, MAXLEN, HD), BF),
            pltpu.VMEM((SLOTS, MAXLEN, HD), BF),
            pltpu.VMEM((PAIR, LOCAL, HD), F32),
            pltpu.VMEM((LOCAL, HD), F32),
            pltpu.VMEM((LOCAL, HD), F32),
            pltpu.VMEM((PAIR, LOCAL, HD), F32),
            pltpu.VMEM((LOCAL, 128), jnp.int32),
            pltpu.SMEM((LOCAL + 8,), jnp.int32),
            pltpu.SemaphoreType.DMA((SLOTS,)),
            pltpu.SemaphoreType.DMA((SLOTS,)),
            pltpu.SemaphoreType.DMA((2,)),
        ],
        compiler_params=pltpu.CompilerParams(vmem_limit_bytes=B_LIMIT * MIB),
        cost_estimate=pl.CostEstimate(flops=4 * 10 ** 9, bytes_accessed=3 * 10 ** 7, transcendentals=10 ** 6),
        name="attend",
    )(lengths, q, k_new, v_new, ks, vs, k_cache, v_cache)


PIECES = 4
PIECE = LOCAL // PIECES
MSGS = 8


def output_kernel(o_ref, wo_hbm, wx_ref, wy_ref, wd_ref, x_hbm, y_ref, og, wc, xc, load_sem, wss, wrs, ss, rs):
    me, _, _, k = coords()
    other = peer(SIB) % 2
    load_x = pltpu.make_async_copy(x_hbm.at[:, :, span(me, HD)], xc, load_sem.at[0])
    load_x.start()
    w_loads = [pltpu.make_async_copy(wo_hbm.at[:, span(me, HD)], wc.at[me], load_sem.at[1])]
    w_copies = [remote(wo_hbm.at[:, span(peer(SIB), HD)], wc.at[me], wss.at[0], wrs.at[0], SIB)]
    w_recvs = [remote(wo_hbm.at[:, span(me, HD)], wc.at[peer(SIB)], wss.at[0], wrs.at[0], SIB)]
    for i, (rel, ref) in enumerate(((X, wx_ref), (Y, wy_ref), (D, wd_ref))):
        w_loads.append(pltpu.make_async_copy(ref.at[:, span(k, HD)], wc.at[peer(rel)], load_sem.at[2 + i]))
        w_copies.append(remote(ref.at[:, span(other, HD)], wc.at[peer(rel)], wss.at[1 + i], wrs.at[1 + i], SIB))
        w_recvs.append(remote(ref.at[:, span(other, HD)], wc.at[peer(rel + SIB)], wss.at[1 + i], wrs.at[1 + i], SIB))
    for load in w_loads:
        load.start()
    entry_barrier((X, Y, SIB))

    def item(kind, owner_rel, p, half):
        owner = peer(owner_rel)
        part = pl.ds(0, 2) if half is None else pl.ds(half, 1)
        rows = span(p, PIECE)
        if kind == 0:
            return og.at[owner, part, rows, :]
        return y_ref.at[part, rows, span(owner, HD)]

    def copy(kind, owner_rel, p, half, to, message):
        index = (kind * PIECES + p) * MSGS + message
        dst = item(kind, owner_rel, p, half)
        src = o_ref.at[:, span(p, PIECE), :] if kind == 0 and owner_rel == 0 else dst
        return remote(src, dst, ss.at[index], rs.at[index], to)

    def send_own(kind, p):
        copy(kind, 0, p, None, X, 0).start()
        copy(kind, 0, p, None, Y, 1).start()
        copy(kind, 0, p, None, SIB, 2).start()

    def first_hop(kind, p):
        copy(kind, X, p, None, X, 0).wait_recv()
        copy(kind, X, p, 0, Y, 3).start()
        copy(kind, X, p, None, SIB, 5).start()
        copy(kind, Y, p, None, Y, 1).wait_recv()
        copy(kind, Y, p, 1, X, 4).start()
        copy(kind, Y, p, None, SIB, 6).start()

    def second_hop(kind, p):
        copy(kind, D, p, 0, Y, 3).wait_recv()
        copy(kind, D, p, 1, X, 4).wait_recv()
        copy(kind, D, p, None, SIB, 7).start()

    def from_sibling(kind, p):
        copy(kind, SIB, p, None, SIB, 2).wait_recv()
        copy(kind, X + SIB, p, None, SIB, 5).wait_recv()
        copy(kind, Y + SIB, p, None, SIB, 6).wait_recv()
        copy(kind, D + SIB, p, None, SIB, 7).wait_recv()

    def sent(kind, p):
        copy(kind, 0, p, None, X, 0).wait_send()
        copy(kind, 0, p, None, Y, 1).wait_send()
        copy(kind, 0, p, None, SIB, 2).wait_send()
        copy(kind, X, p, 0, Y, 3).wait_send()
        copy(kind, Y, p, 1, X, 4).wait_send()
        copy(kind, X, p, None, SIB, 5).wait_send()
        copy(kind, Y, p, None, SIB, 6).wait_send()
        copy(kind, D, p, None, SIB, 7).wait_send()

    def finish(p):
        second_hop(0, p)
        from_sibling(0, p)
        rows = span(p, PIECE)
        total = jnp.zeros((2 * PIECE, HD), F32)
        for chip in range(4):
            for j in range(PAIR):
                lhs = og[pl.ds(2 * chip, 2), j, rows, :].reshape(2 * PIECE, HD)
                total = total + jnp.dot(lhs, wc[2 * chip + j], preferred_element_type=F32)
        y_ref[:, rows, span(me, HD)] = (xc[:, rows, :].astype(F32) + total.reshape(2, PIECE, HD)).astype(BF)
        send_own(1, p)

    for p in range(PIECES - 1):
        send_own(0, p)
    for c in w_copies:
        c.start()
    og[me] = o_ref[...]
    first_hop(0, 0)
    send_own(0, PIECES - 1)

    def forward(p, carry):
        first_hop(0, p)
        return carry

    lax.fori_loop(1, PIECES, forward, 0)
    load_x.wait()
    for load in w_loads:
        load.wait()
    for c in w_recvs:
        c.wait_recv()

    def middle(p, carry):
        finish(p)

        @pl.when(p > 0)
        def _():
            first_hop(1, p - 1)

        return carry

    lax.fori_loop(0, PIECES, middle, 0)
    second_hop(1, 0)
    first_hop(1, PIECES - 1)

    def last(p, carry):
        second_hop(1, p)
        return carry

    lax.fori_loop(1, PIECES, last, 0)

    def drain(p, carry):
        from_sibling(1, p)
        sent(0, p)
        sent(1, p)
        return carry

    lax.fori_loop(0, PIECES, drain, 0)
    for c in w_copies:
        c.wait_send()


def output(o, wo, pieces, x):
    hbm_spec = pl.BlockSpec(memory_space=pltpu.HBM)
    vmem_spec = pl.BlockSpec(memory_space=pltpu.VMEM)
    return pl.pallas_call(
        output_kernel,
        out_shape=jax.ShapeDtypeStruct(x.shape, BF),
        in_specs=[vmem_spec] + [hbm_spec] * 5,
        out_specs=vmem_spec,
        scratch_shapes=[
            pltpu.VMEM((8, PAIR, LOCAL, HD), BF),
            pltpu.VMEM((HEADS, HD, HD), BF),
            pltpu.VMEM((2, LOCAL, HD), BF),
            pltpu.SemaphoreType.DMA((5,)),
            pltpu.SemaphoreType.DMA((4,)),
            pltpu.SemaphoreType.DMA((4,)),
            pltpu.SemaphoreType.DMA((2 * PIECES * MSGS,)),
            pltpu.SemaphoreType.DMA((2 * PIECES * MSGS,)),
        ],
        compiler_params=pltpu.CompilerParams(collective_id=1, has_side_effects=True, vmem_limit_bytes=C_LIMIT * MIB),
        name="output",
    )(o, wo, *pieces, x)


A_LIMIT, B_LIMIT, C_LIMIT = 24, 38, 24


def solution(mesh):
    devices = mesh.shape["model"]

    def to_chip(rel):
        return [(d, d ^ rel) for d in range(devices)]

    def local_step(x, w_query, w_key, w_value, w_out, k_cache, v_cache, lengths):
        in_hbm = [pltpu.with_memory_space_constraint(a, pltpu.HBM) for a in (x, w_query, w_key, w_value, w_out)]
        q, k_new, v_new, ks, vs, wx, wy, wd = project(*in_hbm, k_cache, v_cache)
        pieces = [lax.ppermute(w, "model", to_chip(rel)) for w, rel in ((wx, X), (wy, Y), (wd, D))]
        o, k_new, v_new = attend(lengths, q, k_new, v_new, ks, vs, k_cache, v_cache)
        y = output(o, in_hbm[4], pieces, pltpu.with_memory_space_constraint(x.reshape(2, LOCAL, -1), pltpu.HBM))
        return y.reshape(x.shape), k_new[:, None, :], v_new[:, None, :]

    rows_spec = P("replica")
    return jax.shard_map(
        local_step,
        mesh=mesh,
        in_specs=(P("replica", None), P(None, "model"), P(), P(), P("model", None), rows_spec, rows_spec, rows_spec),
        out_specs=(rows_spec, rows_spec, rows_spec),
        check_vma=False,
    )
```

```python
import jax
import jax.numpy as jnp
from jax import lax
from jax.experimental import pallas as pl
from jax.experimental.pallas import tpu as pltpu
from jax.sharding import PartitionSpec as P

BF = jnp.bfloat16
F32 = jnp.float32
HEADS = 8
HD = 256
LOCAL = 64
SHORT = 32
GROUP = 16
CHUNK = 256
MAXLEN = 2048
SLOTS = 14
HALFW = 128
MIB = 2 ** 20
SCALE = HD ** -0.5
DIMS_T = (((1,), (1,)), ((), ()))


def coords():
    me = lax.axis_index("model")
    return me, me // 4, (me // 2) % 2, me % 2


def peer(rel):
    _, y, x, k = coords()
    dy, dx, dk = rel // 4, (rel // 2) % 2, rel % 2
    return (((y + dy) % 2) * 2 + (x + dx) % 2) * 2 + (k + dk) % 2


def span(index, size):
    return pl.ds(pl.multiple_of(index * size, size), size)


def entry_barrier(rels):
    barrier = pltpu.get_barrier_semaphore()
    for rel in rels:
        pl.semaphore_signal(barrier, inc=1, device_id={"model": peer(rel)}, device_id_type=pl.DeviceIdType.MESH)
    pl.semaphore_wait(barrier, len(rels))


def remote(src, dst, send_sem, recv_sem, rel):
    return pltpu.make_async_remote_copy(
        src_ref=src, dst_ref=dst, send_sem=send_sem, recv_sem=recv_sem,
        device_id={"model": peer(rel)}, device_id_type=pl.DeviceIdType.MESH)


RELS = (6, 7, 2, 3, 4, 5, 1)


def softmax_parts(s, s_new):
    m = jnp.maximum(jnp.max(s, axis=-1, keepdims=True), s_new)
    e = jnp.exp(s - m)
    e_new = jnp.exp(s_new - m)
    total = jnp.sum(e, axis=-1, keepdims=True) + e_new
    return e.astype(BF), e_new.astype(BF).astype(F32), total


def project_kernel(len_ref, x_hbm, wq_hbm, wk_hbm, wv_hbm, wo_hbm, k_hbm, v_hbm, q_out, kn_out, vn_out, wc_out, o_out,
                   x_v, wq_v, wk_v, wv_v, q_v, ks, vs, lens_v, in_sem, own_sem, qs, qr, ws, wr):
    me, y, x, k = coords()
    mine = span(me, LOCAL)
    loads = [pltpu.make_async_copy(src, dst, in_sem.at[i]) for i, (src, dst) in enumerate((
        (wq_hbm, wq_v),
        (x_hbm, x_v),
        (wk_hbm, wk_v),
        (wv_hbm, wv_v),
        (k_hbm.at[mine, 0, pl.ds(0, SHORT), :], ks),
        (v_hbm.at[mine, 0, pl.ds(0, SHORT), :], vs),
    ))]
    loads[0].start()
    loads[1].start()
    entry_barrier(RELS)
    loads[0].wait()
    loads[1].wait()
    q_copies, w_copies = [], []
    for chip_rel in (6, 2, 4, 0):
        rows = span(peer(chip_rel) // 2, 2 * LOCAL)
        q_v[rows, :] = jnp.dot(x_v[rows, :], wq_v[...], preferred_element_type=F32).astype(BF)
        for rel in (chip_rel, chip_rel + 1):
            if rel == 0:
                continue
            copy = remote(q_v.at[span(peer(rel), LOCAL), :], q_out.at[me], qs.at[rel], qr.at[rel], rel)
            copy.start()
            q_copies.append(copy)
    for rel in RELS:
        copy = remote(wo_hbm.at[:, span(peer(rel), HD)], wc_out.at[span(me, HD), :], ws.at[rel], wr.at[rel], rel)
        copy.start()
        w_copies.append(copy)
    own_w = pltpu.make_async_copy(wo_hbm.at[:, span(me, HD)], wc_out.at[span(me, HD), :], own_sem)
    own_w.start()
    for load in loads[2:]:
        load.start()
    q_out[me] = q_v[mine, :]

    def spread(i, carry):
        lens_v[pl.ds(i, 1), :] = jnp.full((1, 128), len_ref[me * LOCAL + i], jnp.int32)
        return carry

    lax.fori_loop(0, LOCAL, spread, 0)
    for load in loads[2:]:
        load.wait()
    for part in range(2):
        rows = pl.ds(part * 256, 256)
        kn_out[rows, :] = jnp.dot(x_v[rows, :], wk_v[...], preferred_element_type=F32).astype(BF)
        vn_out[rows, :] = jnp.dot(x_v[rows, :], wv_v[...], preferred_element_type=F32).astype(BF)
    for copy in q_copies:
        copy.wait()

    width = GROUP * SHORT
    col = lax.broadcasted_iota(jnp.int32, (GROUP, width), 1)
    same = (col // SHORT) == lax.broadcasted_iota(jnp.int32, (GROUP, width), 0)
    slot_pos = col % SHORT

    def group(g, carry):
        seqs = span(g, GROUP)
        new = pl.ds(pl.multiple_of(me * LOCAL + g * GROUP, GROUP), GROUP)
        qg = q_out[:, seqs, :]
        s = lax.dot_general(qg.reshape(HEADS * GROUP, HD), ks[seqs].reshape(width, HD), DIMS_T, preferred_element_type=F32) * SCALE
        valid = same & (slot_pos < lens_v[seqs, 0:1])
        s = jnp.where(valid[None], s.reshape(HEADS, GROUP, width), -jnp.inf)
        s_new = jnp.sum(qg.astype(F32) * kn_out[new, :].astype(F32)[None], axis=-1, keepdims=True) * SCALE
        e, e_new, total = softmax_parts(s, s_new)
        num = jnp.dot(e.reshape(HEADS * GROUP, width), vs[seqs].reshape(width, HD), preferred_element_type=F32)
        num = num.reshape(HEADS, GROUP, HD) + e_new * vn_out[new, :].astype(F32)[None]
        o_out[:, seqs, :] = (num / total).astype(BF)
        return carry

    lax.fori_loop(0, LOCAL // GROUP, group, 0)
    own_w.wait()
    for copy in w_copies:
        copy.wait()


def project(lengths, x, wq, wk, wv, wo, k_cache, v_cache):
    rows, depth = x.shape
    hbm_spec = pl.BlockSpec(memory_space=pltpu.HBM)
    vmem_spec = pl.BlockSpec(memory_space=pltpu.VMEM)
    return pl.pallas_call(
        project_kernel,
        out_shape=(
            jax.ShapeDtypeStruct((HEADS, LOCAL, HD), BF),
            jax.ShapeDtypeStruct((rows, HD), BF),
            jax.ShapeDtypeStruct((rows, HD), BF),
            jax.ShapeDtypeStruct((HEADS * HD, HD), BF),
            jax.ShapeDtypeStruct((HEADS, LOCAL, HD), BF),
        ),
        in_specs=[pl.BlockSpec(memory_space=pltpu.SMEM)] + [hbm_spec] * 7,
        out_specs=(vmem_spec,) * 5,
        scratch_shapes=[
            pltpu.VMEM((rows, depth), BF),
            pltpu.VMEM((depth, HD), BF),
            pltpu.VMEM((depth, HD), BF),
            pltpu.VMEM((depth, HD), BF),
            pltpu.VMEM((rows, HD), BF),
            pltpu.VMEM((LOCAL, SHORT, HD), BF),
            pltpu.VMEM((LOCAL, SHORT, HD), BF),
            pltpu.VMEM((LOCAL, 128), jnp.int32),
            pltpu.SemaphoreType.DMA((6,)),
            pltpu.SemaphoreType.DMA,
            pltpu.SemaphoreType.DMA((8,)),
            pltpu.SemaphoreType.DMA((8,)),
            pltpu.SemaphoreType.DMA((8,)),
            pltpu.SemaphoreType.DMA((8,)),
        ],
        compiler_params=pltpu.CompilerParams(collective_id=0, has_side_effects=True, vmem_limit_bytes=24 * MIB),
        name="project",
    )(lengths, x, wq, wk, wv, wo, k_cache, v_cache)


def attend_kernel(len_ref, q_ref, kn_ref, vn_ref, os_ref, k_hbm, v_hbm, o_ref, kn_out, vn_out,
                  kl, vl, qf, knf, vnf, acc, lidx, k_sem, v_sem, new_sem):
    me = lax.axis_index("model")
    base = me * LOCAL
    new_k = pltpu.make_async_copy(kn_ref, kn_out, new_sem.at[0])
    new_v = pltpu.make_async_copy(vn_ref, vn_out, new_sem.at[1])

    def chunks_of(i):
        return (len_ref[base + lidx[i]] + CHUNK - 1) // CHUNK

    def each_part(i, action):
        slot = i % SLOTS
        chunks = chunks_of(i)
        first = jnp.int32(0)
        for size in (8, 4, 2, 1):
            take = chunks - first >= size
            rows = pl.ds(pl.multiple_of(first * CHUNK, CHUNK), size * CHUNK)

            @pl.when(take)
            def _():
                for cache, dst, sem in ((k_hbm, kl, k_sem), (v_hbm, vl, v_sem)):
                    for half in range(2):
                        action(pltpu.make_async_copy(
                            cache.at[base + lidx[i], 0, rows, pl.ds(half * HALFW, HALFW)],
                            dst.at[slot, half, rows, :], sem.at[slot]))

            first = first + jnp.where(take, size, 0)

    def fetch(i):
        each_part(i, lambda copy: copy.start())

    def scan(i, count):
        lidx[count] = i
        is_long = len_ref[base + i] > SHORT

        @pl.when(is_long & (count < SLOTS))
        def _():
            fetch(count)

        return count + jnp.where(is_long, 1, 0)

    n_long = lax.fori_loop(0, LOCAL, scan, jnp.int32(0))
    new_k.start()
    new_v.start()
    own = span(me, LOCAL)
    qf[...] = q_ref[...].astype(F32)
    knf[...] = kn_ref[own, :].astype(F32)
    vnf[...] = vn_ref[own, :].astype(F32)
    acc[...] = os_ref[...].astype(F32)

    def rows_of(ref, slot, rows):
        return jnp.concatenate([ref[slot, half, pl.ds(0, rows), :] for half in range(2)], axis=-1)

    def one_long(i, rows):
        seq = lidx[i]
        slot = i % SLOTS
        at = pl.ds(seq, 1)
        q8 = jnp.concatenate([qf[h, at, :] for h in range(HEADS)], axis=0)
        s = lax.dot_general(q8.astype(BF), rows_of(kl, slot, rows), DIMS_T, preferred_element_type=F32) * SCALE
        s = jnp.where(lax.broadcasted_iota(jnp.int32, s.shape, 1) < len_ref[base + seq], s, -jnp.inf)
        s_new = jnp.sum(q8 * knf[at, :], axis=-1, keepdims=True) * SCALE
        e, e_new, total = softmax_parts(s, s_new)
        num = jnp.dot(e, rows_of(vl, slot, rows), preferred_element_type=F32)
        return seq, (num + e_new * vnf[at, :]) / total

    def wait_and_clear(i, most):
        each_part(i, lambda copy: copy.wait())

        @pl.loop(chunks_of(i), most)
        def _(c):
            vl[i % SLOTS, :, span(c, CHUNK), :] = jnp.zeros((2, CHUNK, HALFW), BF)

    @pl.loop(0, (n_long + 1) // 2)
    def _(pair):
        a = pair * 2
        b = jnp.minimum(a + 1, n_long - 1)
        most = jnp.maximum(chunks_of(a), chunks_of(b))
        wait_and_clear(a, most)

        @pl.when(b > a)
        def _():
            wait_and_clear(b, most)

        for n in range(1, MAXLEN // CHUNK + 1):
            @pl.when(most == n)
            def _():
                results = [one_long(i, n * CHUNK) for i in (a, b)]
                for seq, out in results:
                    for h in range(HEADS):
                        acc[h, pl.ds(seq, 1), :] = out[h:h + 1, :]

        for i in (a, a + 1):
            @pl.when(i + SLOTS < n_long)
            def _():
                fetch(i + SLOTS)

    o_ref[...] = acc[...].astype(BF)
    new_k.wait()
    new_v.wait()


def attend(lengths, q, k_new, v_new, o_short, k_cache, v_cache):
    rows = k_new.shape[0]
    any_spec = pl.BlockSpec(memory_space=pl.ANY)
    vmem_spec = pl.BlockSpec(memory_space=pltpu.VMEM)
    return pl.pallas_call(
        attend_kernel,
        out_shape=(
            jax.ShapeDtypeStruct((HEADS, LOCAL, HD), BF),
            jax.ShapeDtypeStruct((rows, HD), BF),
            jax.ShapeDtypeStruct((rows, HD), BF),
        ),
        in_specs=[pl.BlockSpec(memory_space=pltpu.SMEM)] + [vmem_spec] * 4 + [any_spec] * 2,
        out_specs=(vmem_spec, any_spec, any_spec),
        scratch_shapes=[
            pltpu.VMEM((SLOTS, 2, MAXLEN, HALFW), BF),
            pltpu.VMEM((SLOTS, 2, MAXLEN, HALFW), BF),
            pltpu.VMEM((HEADS, LOCAL, HD), F32),
            pltpu.VMEM((LOCAL, HD), F32),
            pltpu.VMEM((LOCAL, HD), F32),
            pltpu.VMEM((HEADS, LOCAL, HD), F32),
            pltpu.SMEM((LOCAL + 8,), jnp.int32),
            pltpu.SemaphoreType.DMA((SLOTS,)),
            pltpu.SemaphoreType.DMA((SLOTS,)),
            pltpu.SemaphoreType.DMA((2,)),
        ],
        compiler_params=pltpu.CompilerParams(vmem_limit_bytes=40 * MIB),
        cost_estimate=pl.CostEstimate(flops=4 * 10 ** 9, bytes_accessed=10 ** 7, transcendentals=10 ** 6),
        name="attend",
    )(lengths, q, k_new, v_new, o_short, k_cache, v_cache)


HALF = HEADS // 2
X, Y, D, S = 2, 4, 6, 1


def output_kernel(o_ref, wc_ref, x_hbm, y_ref, og, xc, load_sem, os, orr, ys, yr):
    me, _, _, k = coords()
    cols = pl.ds(pl.multiple_of(me * HD, HD), HD)
    load_x = pltpu.make_async_copy(x_hbm.at[:, cols], xc, load_sem)
    load_x.start()
    entry_barrier((X, Y, S))
    started = []

    def o_copy(owner_rel, half, to, index):
        owner = peer(owner_rel)
        part = pl.ds(0, HEADS) if half is None else pl.ds(half * HALF, HALF)
        ref = og.at[owner, part]
        return remote(o_ref.at[part] if owner_rel == 0 else ref, ref, os.at[index], orr.at[index], to)

    def go(copy):
        copy.start()
        started.append(copy)

    def recv_o(owner_rel, half, to, index):
        o_copy(owner_rel, half, to, index).wait_recv()

    go(o_copy(0, 0, X, 0))
    go(o_copy(0, 1, Y, 1))
    go(o_copy(0, 1, X, 2))
    go(o_copy(0, 0, Y, 3))
    go(o_copy(0, None, S, 4))

    og[me] = o_ref[...]
    load_x.wait()

    def y_copy(col_rel, chip_rel, core, to, index):
        column = peer(col_rel)
        chip = peer(chip_rel) // 2
        first = chip * 2 + (0 if core is None else core)
        rows = pl.ds(pl.multiple_of(first * LOCAL, LOCAL), LOCAL if core is not None else 2 * LOCAL)
        ref = y_ref.at[rows, pl.ds(pl.multiple_of(column * HD, HD), HD)]
        return remote(ref, ref, ys.at[index], yr.at[index], to)

    def compute(step, chip_rel):
        chip = peer(chip_rel) // 2
        total = jnp.zeros((2 * LOCAL, HD), F32)
        for h in range(HEADS):
            lhs = og[pl.ds(chip * 2, 2), h].reshape(2 * LOCAL, HD)
            total = total + jnp.dot(lhs, wc_ref[pl.ds(h * HD, HD), :], preferred_element_type=F32)
        rows = pl.ds(pl.multiple_of(chip * 2 * LOCAL, 2 * LOCAL), 2 * LOCAL)
        y_ref[rows, cols] = (xc[rows, :].astype(F32) + total).astype(BF)
        b = step * 11
        go(y_copy(0, chip_rel, 0, X, b + 0))
        go(y_copy(0, chip_rel, 1, Y, b + 1))
        go(y_copy(0, chip_rel, 1, X, b + 2))
        go(y_copy(0, chip_rel, 0, Y, b + 3))
        go(y_copy(0, chip_rel, None, S, b + 4))

    recv_o(S, None, S, 4)
    compute(0, 0)
    recv_o(X, 0, X, 0)
    go(o_copy(X, 0, Y, 5))
    recv_o(Y, 1, Y, 1)
    go(o_copy(Y, 1, X, 6))
    recv_o(X, 1, X, 2)
    go(o_copy(X, None, S, 7))
    recv_o(Y, 0, Y, 3)
    go(o_copy(Y, None, S, 8))
    recv_o(X + S, None, S, 7)
    compute(1, X)
    recv_o(Y + S, None, S, 8)
    compute(2, Y)
    recv_o(D, 0, Y, 5)
    go(o_copy(D, 0, S, 9))
    recv_o(D, 1, X, 6)
    go(o_copy(D, 1, S, 10))
    recv_o(D + S, 0, S, 9)
    recv_o(D + S, 1, S, 10)
    compute(3, D)

    def xor(a, b):
        return ((a // 4 + b // 4) % 2) * 4 + ((a // 2 + b // 2) % 2) * 2 + (a + b) % 2

    order = (0, X, Y, D)
    for step, rel in enumerate(order):
        b = step * 11
        at_x, at_y, at_d = xor(rel, X), xor(rel, Y), xor(rel, D)
        y_copy(X, at_x, 0, X, b + 0).wait_recv()
        go(y_copy(X, at_x, 0, Y, b + 5))
        y_copy(Y, at_y, 1, Y, b + 1).wait_recv()
        go(y_copy(Y, at_y, 1, X, b + 6))
        y_copy(X, at_x, 1, X, b + 2).wait_recv()
        go(y_copy(X, at_x, None, S, b + 7))
        y_copy(Y, at_y, 0, Y, b + 3).wait_recv()
        go(y_copy(Y, at_y, None, S, b + 8))
    for step, rel in enumerate(order):
        b = step * 11
        at_d = xor(rel, D)
        y_copy(D, at_d, 0, Y, b + 5).wait_recv()
        go(y_copy(D, at_d, 0, S, b + 9))
        y_copy(D, at_d, 1, X, b + 6).wait_recv()
        go(y_copy(D, at_d, 1, S, b + 10))
    for step, rel in enumerate(order):
        b = step * 11
        at_x, at_y, at_d = xor(rel, X), xor(rel, Y), xor(rel, D)
        y_copy(S, rel, None, S, b + 4).wait_recv()
        y_copy(X + S, at_x, None, S, b + 7).wait_recv()
        y_copy(Y + S, at_y, None, S, b + 8).wait_recv()
        y_copy(D + S, at_d, 0, S, b + 9).wait_recv()
        y_copy(D + S, at_d, 1, S, b + 10).wait_recv()
    for copy in started:
        copy.wait_send()


def output(o, wc, x):
    rows, width = x.shape
    hbm_spec = pl.BlockSpec(memory_space=pltpu.HBM)
    vmem_spec = pl.BlockSpec(memory_space=pltpu.VMEM)
    return pl.pallas_call(
        output_kernel,
        out_shape=jax.ShapeDtypeStruct((rows, width), BF),
        in_specs=[vmem_spec, vmem_spec, hbm_spec],
        out_specs=vmem_spec,
        scratch_shapes=[
            pltpu.VMEM((8, HEADS, LOCAL, HD), BF),
            pltpu.VMEM((rows, HD), BF),
            pltpu.SemaphoreType.DMA,
            pltpu.SemaphoreType.DMA((11,)),
            pltpu.SemaphoreType.DMA((11,)),
            pltpu.SemaphoreType.DMA((44,)),
            pltpu.SemaphoreType.DMA((44,)),
        ],
        compiler_params=pltpu.CompilerParams(collective_id=1, has_side_effects=True, vmem_limit_bytes=40 * 2 ** 20),
        name="output",
    )(o, wc, x)


def solution(mesh):
    def local_step(x, w_query, w_key, w_value, w_out, k_cache, v_cache, lengths):
        x, w_query, w_key, w_value, w_out = (
            pltpu.with_memory_space_constraint(a, pltpu.HBM) for a in (x, w_query, w_key, w_value, w_out))
        q, k_new, v_new, w_cols, o_short = project(lengths, x, w_query, w_key, w_value, w_out, k_cache, v_cache)
        o, k_new, v_new = attend(lengths, q, k_new, v_new, o_short, k_cache, v_cache)
        y = output(o, w_cols, x)
        return y, k_new[:, None, :], v_new[:, None, :]

    rows_spec = P("replica")
    return jax.shard_map(
        local_step,
        mesh=mesh,
        in_specs=(P("replica", None), P(None, "model"), P(), P(), P("model", None), rows_spec, rows_spec, rows_spec),
        out_specs=(rows_spec, rows_spec, rows_spec),
        check_vma=False,
    )
```

```python
import jax
import jax.numpy as jnp
from jax import lax
from jax.experimental import pallas as pl
from jax.experimental.pallas import tpu as pltpu
from jax.sharding import PartitionSpec as P

BF = jnp.bfloat16
F32 = jnp.float32
HEADS = 8
HD = 256
LOCAL = 64
SHORT = 32
GROUP = 16
CHUNK = 256
MAXLEN = 2048
SLOTS = 6
AHEAD = 4
HALFW = 128
MIB = 2 ** 20
SCALE = HD ** -0.5
DIMS_T = (((1,), (1,)), ((), ()))


def coords():
    me = lax.axis_index("model")
    return me, me // 4, (me // 2) % 2, me % 2


def peer(rel):
    _, y, x, k = coords()
    dy, dx, dk = rel // 4, (rel // 2) % 2, rel % 2
    return (((y + dy) % 2) * 2 + (x + dx) % 2) * 2 + (k + dk) % 2


def span(index, size):
    return pl.ds(pl.multiple_of(index * size, size), size)


def entry_barrier(rels):
    barrier = pltpu.get_barrier_semaphore()
    for rel in rels:
        pl.semaphore_signal(barrier, inc=1, device_id={"model": peer(rel)}, device_id_type=pl.DeviceIdType.MESH)
    pl.semaphore_wait(barrier, len(rels))


def remote(src, dst, send_sem, recv_sem, rel):
    return pltpu.make_async_remote_copy(
        src_ref=src, dst_ref=dst, send_sem=send_sem, recv_sem=recv_sem,
        device_id={"model": peer(rel)}, device_id_type=pl.DeviceIdType.MESH)


RELS = (6, 7, 2, 3, 4, 5, 1)


def softmax_parts(s, s_new):
    m = jnp.maximum(jnp.max(s, axis=-1, keepdims=True), s_new)
    e = jnp.exp(s - m)
    e_new = jnp.exp(s_new - m)
    total = jnp.sum(e, axis=-1, keepdims=True) + e_new
    return e.astype(BF), e_new.astype(BF).astype(F32), total


def project_kernel(len_hbm, x_hbm, wq_hbm, wk_hbm, wv_hbm, wo_hbm, k_hbm, v_hbm, q_out, kn_out, vn_out, wc_out, o_out, wx_out, wy_out,
                   x_v, wq_v, wk_v, wv_v, wo_v, q_v, ks, vs, lens_v, len_ref, in_sem, own_sem, qs, qr, ws, wr):
    me, y, x, k = coords()
    mine = span(me, LOCAL)
    loads = [pltpu.make_async_copy(src, dst, in_sem.at[i]) for i, (src, dst) in enumerate((
        (wq_hbm, wq_v),
        (x_hbm, x_v),
        (wk_hbm, wk_v),
        (wv_hbm, wv_v),
        (k_hbm.at[mine, 0, pl.ds(0, SHORT), :], ks),
        (v_hbm.at[mine, 0, pl.ds(0, SHORT), :], vs),
        (len_hbm, len_ref),
        (wo_hbm, wo_v),
    ))]
    loads[0].start()
    loads[1].start()
    loads[7].start()
    entry_barrier(RELS)
    loads[0].wait()
    loads[1].wait()
    q_copies, w_copies = [], []
    for chip_rel in (6, 2, 4, 0):
        rows = span(peer(chip_rel) // 2, 2 * LOCAL)
        q_v[rows, :] = jnp.dot(x_v[rows, :], wq_v[...], preferred_element_type=F32).astype(BF)
        for rel in (chip_rel, chip_rel + 1):
            if rel == 0:
                continue
            copy = remote(q_v.at[span(peer(rel), LOCAL), :], q_out.at[me], qs.at[rel], qr.at[rel], rel)
            copy.start()
            q_copies.append(copy)
    loads[7].wait()
    for rel in (6, 7, 1):
        copy = remote(wo_v.at[:, span(peer(rel), HD)], wc_out.at[span(me, HD), :], ws.at[rel], wr.at[rel], rel)
        copy.start()
        w_copies.append(copy)
    stores = [pltpu.make_async_copy(wo_v.at[:, span(peer(rel) // 2, 2 * HD)], out, own_sem.at[i])
              for i, (rel, out) in enumerate(((X, wx_out), (Y, wy_out)))]
    for store in stores:
        store.start()
    wc_out[span(me, HD), :] = wo_v[:, span(me, HD)]
    for load in loads[2:7]:
        load.start()
    q_out[me] = q_v[mine, :]

    def spread(i, carry):
        lens_v[pl.ds(i, 1), :] = jnp.full((1, 128), len_ref[me * LOCAL + i], jnp.int32)
        return carry

    loads[6].wait()
    lax.fori_loop(0, LOCAL, spread, 0)
    for load in loads[2:6]:
        load.wait()
    for part in range(2):
        rows = pl.ds(part * 256, 256)
        kn_out[rows, :] = jnp.dot(x_v[rows, :], wk_v[...], preferred_element_type=F32).astype(BF)
        vn_out[rows, :] = jnp.dot(x_v[rows, :], wv_v[...], preferred_element_type=F32).astype(BF)
    for copy in q_copies:
        copy.wait()

    width = GROUP * SHORT
    col = lax.broadcasted_iota(jnp.int32, (GROUP, width), 1)
    same = (col // SHORT) == lax.broadcasted_iota(jnp.int32, (GROUP, width), 0)
    slot_pos = col % SHORT

    def group(g, carry):
        seqs = span(g, GROUP)
        new = pl.ds(pl.multiple_of(me * LOCAL + g * GROUP, GROUP), GROUP)
        qg = q_out[:, seqs, :]
        s = lax.dot_general(qg.reshape(HEADS * GROUP, HD), ks[seqs].reshape(width, HD), DIMS_T, preferred_element_type=F32) * SCALE
        valid = same & (slot_pos < lens_v[seqs, 0:1])
        s = jnp.where(valid[None], s.reshape(HEADS, GROUP, width), -jnp.inf)
        s_new = jnp.sum(qg.astype(F32) * kn_out[new, :].astype(F32)[None], axis=-1, keepdims=True) * SCALE
        e, e_new, total = softmax_parts(s, s_new)
        num = jnp.dot(e.reshape(HEADS * GROUP, width), vs[seqs].reshape(width, HD), preferred_element_type=F32)
        num = num.reshape(HEADS, GROUP, HD) + e_new * vn_out[new, :].astype(F32)[None]
        o_out[:, seqs, :] = (num / total).astype(BF)
        return carry

    lax.fori_loop(0, LOCAL // GROUP, group, 0)
    for copy in w_copies + stores:
        copy.wait()


def project(lengths, x, wq, wk, wv, wo, k_cache, v_cache):
    rows, depth = x.shape
    hbm_spec = pl.BlockSpec(memory_space=pltpu.HBM)
    vmem_spec = pl.BlockSpec(memory_space=pltpu.VMEM)
    return pl.pallas_call(
        project_kernel,
        out_shape=(
            jax.ShapeDtypeStruct((HEADS, LOCAL, HD), BF),
            jax.ShapeDtypeStruct((rows, HD), BF),
            jax.ShapeDtypeStruct((rows, HD), BF),
            jax.ShapeDtypeStruct((HEADS * HD, HD), BF),
            jax.ShapeDtypeStruct((HEADS, LOCAL, HD), BF),
            jax.ShapeDtypeStruct((HD, 2 * HD), BF),
            jax.ShapeDtypeStruct((HD, 2 * HD), BF),
        ),
        in_specs=[hbm_spec] * 8,
        out_specs=(vmem_spec,) * 5 + (hbm_spec,) * 2,
        scratch_shapes=[
            pltpu.VMEM((rows, depth), BF),
            pltpu.VMEM((depth, HD), BF),
            pltpu.VMEM((depth, HD), BF),
            pltpu.VMEM((depth, HD), BF),
            pltpu.VMEM(wo.shape, BF),
            pltpu.VMEM((rows, HD), BF),
            pltpu.VMEM((LOCAL, SHORT, HD), BF),
            pltpu.VMEM((LOCAL, SHORT, HD), BF),
            pltpu.VMEM((LOCAL, 128), jnp.int32),
            pltpu.SMEM(lengths.shape, jnp.int32),
            pltpu.SemaphoreType.DMA((8,)),
            pltpu.SemaphoreType.DMA((2,)),
            pltpu.SemaphoreType.DMA((8,)),
            pltpu.SemaphoreType.DMA((8,)),
            pltpu.SemaphoreType.DMA((8,)),
            pltpu.SemaphoreType.DMA((8,)),
        ],
        compiler_params=pltpu.CompilerParams(collective_id=0, has_side_effects=True, vmem_limit_bytes=24 * MIB),
        name="project",
    )(lengths, x, wq, wk, wv, wo, k_cache, v_cache)


def attend_kernel(len_ref, q_ref, kn_ref, vn_ref, os_ref, k_hbm, v_hbm, o_ref, kn_out, vn_out,
                  kl, vl, qf, knf, vnf, acc, lidx, lchunks, k_sem, v_sem, new_sem):
    me = lax.axis_index("model")
    base = me * LOCAL
    new_k = pltpu.make_async_copy(kn_ref, kn_out, new_sem.at[0])
    new_v = pltpu.make_async_copy(vn_ref, vn_out, new_sem.at[1])

    def each_part(i, slot, action):
        seq = base + lidx[i]
        chunks = lchunks[i]
        first = 0
        for size in (8, 4, 2, 1):
            rows = pl.ds(pl.multiple_of(first * CHUNK, CHUNK), size * CHUNK)

            @pl.when(chunks & size != 0)
            def _():
                for cache, dst, sem in ((k_hbm, kl, k_sem), (v_hbm, vl, v_sem)):
                    for half in range(2):
                        action(pltpu.make_async_copy(
                            cache.at[seq, 0, rows, pl.ds(half * HALFW, HALFW)],
                            dst.at[slot, half, rows, :], sem.at[slot]))

            first = first + (chunks & size)

    def fetch(i, slot):
        each_part(i, slot, lambda copy: copy.start())

    def scan(i, count):
        length = len_ref[base + i]
        lidx[count] = i
        lchunks[count] = jnp.right_shift(length + (CHUNK - 1), CHUNK.bit_length() - 1)
        is_long = length > SHORT

        @pl.when(is_long & (count < AHEAD))
        def _():
            fetch(count, count)

        return count + jnp.where(is_long, 1, 0)

    n_long = lax.fori_loop(0, LOCAL, scan, jnp.int32(0))
    new_k.start()
    new_v.start()
    own = span(me, LOCAL)
    qf[...] = q_ref[...].astype(F32)
    knf[...] = kn_ref[own, :].astype(F32)
    vnf[...] = vn_ref[own, :].astype(F32)
    acc[...] = os_ref[...].astype(F32)

    def rows_of(ref, slot, rows):
        return jnp.concatenate([ref[slot, half, pl.ds(0, rows), :] for half in range(2)], axis=-1)

    def one_long(i, slot, rows):
        seq = lidx[i]
        at = pl.ds(seq, 1)
        q8 = jnp.concatenate([qf[h, at, :] for h in range(HEADS)], axis=0)
        s = lax.dot_general(q8.astype(BF), rows_of(kl, slot, rows), DIMS_T, preferred_element_type=F32) * SCALE
        s = jnp.where(lax.broadcasted_iota(jnp.int32, s.shape, 1) < len_ref[base + seq], s, -jnp.inf)
        s_new = jnp.sum(q8 * knf[at, :], axis=-1, keepdims=True) * SCALE
        e, e_new, total = softmax_parts(s, s_new)
        num = jnp.dot(e, rows_of(vl, slot, rows), preferred_element_type=F32)
        return seq, (num + e_new * vnf[at, :]) / total

    def wait_and_clear(i, slot, most):
        each_part(i, slot, lambda copy: copy.wait())

        @pl.loop(lchunks[i], most)
        def _(c):
            vl[slot, :, span(c, CHUNK), :] = jnp.zeros((2, CHUNK, HALFW), BF)

    def step(pair, slot):
        a = pair * 2
        alone = a + 1 >= n_long
        b = jnp.where(alone, a, a + 1)
        slot_b = jnp.where(alone, slot, slot + 1)
        most = jnp.maximum(lchunks[a], lchunks[b])
        wait_and_clear(a, slot, most)

        @pl.when(jnp.logical_not(alone))
        def _():
            wait_and_clear(b, slot + 1, most)

        later = jnp.where(slot >= SLOTS - AHEAD, slot + AHEAD - SLOTS, slot + AHEAD)
        for j in range(2):
            @pl.when(a + AHEAD + j < n_long)
            def _():
                fetch(a + AHEAD + j, later + j)

        for n in range(1, MAXLEN // CHUNK + 1):
            @pl.when(most == n)
            def _():
                results = [one_long(i, at, n * CHUNK) for i, at in ((a, slot), (b, slot_b))]
                for seq, out in results:
                    for h in range(HEADS):
                        acc[h, pl.ds(seq, 1), :] = out[h:h + 1, :]

        return jnp.where(slot + 2 >= SLOTS, 0, slot + 2)

    lax.fori_loop(0, jnp.right_shift(n_long + 1, 1), step, jnp.int32(0))
    o_ref[...] = acc[...].astype(BF)
    new_k.wait()
    new_v.wait()


def attend(lengths, q, k_new, v_new, o_short, k_cache, v_cache):
    rows = k_new.shape[0]
    any_spec = pl.BlockSpec(memory_space=pl.ANY)
    vmem_spec = pl.BlockSpec(memory_space=pltpu.VMEM)
    return pl.pallas_call(
        attend_kernel,
        out_shape=(
            jax.ShapeDtypeStruct((HEADS, LOCAL, HD), BF),
            jax.ShapeDtypeStruct((rows, HD), BF),
            jax.ShapeDtypeStruct((rows, HD), BF),
        ),
        in_specs=[pl.BlockSpec(memory_space=pltpu.SMEM)] + [vmem_spec] * 4 + [any_spec] * 2,
        out_specs=(vmem_spec, any_spec, any_spec),
        scratch_shapes=[
            pltpu.VMEM((SLOTS, 2, MAXLEN, HALFW), BF),
            pltpu.VMEM((SLOTS, 2, MAXLEN, HALFW), BF),
            pltpu.VMEM((HEADS, LOCAL, HD), F32),
            pltpu.VMEM((LOCAL, HD), F32),
            pltpu.VMEM((LOCAL, HD), F32),
            pltpu.VMEM((HEADS, LOCAL, HD), F32),
            pltpu.SMEM((LOCAL + 8,), jnp.int32),
            pltpu.SMEM((LOCAL + 8,), jnp.int32),
            pltpu.SemaphoreType.DMA((SLOTS,)),
            pltpu.SemaphoreType.DMA((SLOTS,)),
            pltpu.SemaphoreType.DMA((2,)),
        ],
        compiler_params=pltpu.CompilerParams(vmem_limit_bytes=24 * MIB),
        cost_estimate=pl.CostEstimate(flops=4 * 10 ** 9, bytes_accessed=10 ** 7, transcendentals=10 ** 6),
        name="attend",
    )(lengths, q, k_new, v_new, o_short, k_cache, v_cache)


HALF = HEADS // 2
X, Y, D, S = 2, 4, 6, 1


def output_kernel(o_ref, wc_ref, wx_hbm, wy_hbm, x_hbm, y_ref, og, xc, wp, load_sem, wss, wrs, os, orr, ys, yr):
    me, _, _, k = coords()
    other = peer(S) % 2
    w_loads, w_copies, w_recvs = [], [], []
    for i, (rel, ref) in enumerate(((X, wx_hbm), (Y, wy_hbm))):
        w_loads.append(pltpu.make_async_copy(ref.at[:, span(k, HD)], wp.at[2 * i + k], load_sem.at[1 + i]))
        w_copies.append(remote(ref.at[:, span(other, HD)], wp.at[2 * i + k], wss.at[i], wrs.at[i], S))
        w_recvs.append(remote(ref.at[:, span(other, HD)], wp.at[2 * i + other], wss.at[i], wrs.at[i], S))
    cols = pl.ds(pl.multiple_of(me * HD, HD), HD)
    load_x = pltpu.make_async_copy(x_hbm.at[:, cols], xc, load_sem.at[0])
    load_x.start()
    for load in w_loads:
        load.start()
    entry_barrier((X, Y, S))
    started = []

    def o_copy(owner_rel, half, to, index):
        owner = peer(owner_rel)
        part = pl.ds(0, HEADS) if half is None else pl.ds(half * HALF, HALF)
        ref = og.at[owner, part]
        return remote(o_ref.at[part] if owner_rel == 0 else ref, ref, os.at[index], orr.at[index], to)

    def go(copy):
        copy.start()
        started.append(copy)

    def recv_o(owner_rel, half, to, index):
        o_copy(owner_rel, half, to, index).wait_recv()

    go(o_copy(0, 0, X, 0))
    go(o_copy(0, 1, Y, 1))
    go(o_copy(0, 1, X, 2))
    go(o_copy(0, 0, Y, 3))
    go(o_copy(0, None, S, 4))
    for c in w_copies:
        go(c)

    og[me] = o_ref[...]
    load_x.wait()
    for load in w_loads:
        load.wait()
    for c in w_recvs:
        c.wait_recv()

    def y_copy(col_rel, chip_rel, core, to, index):
        column = peer(col_rel)
        chip = peer(chip_rel) // 2
        first = chip * 2 + (0 if core is None else core)
        rows = pl.ds(pl.multiple_of(first * LOCAL, LOCAL), LOCAL if core is not None else 2 * LOCAL)
        ref = y_ref.at[rows, pl.ds(pl.multiple_of(column * HD, HD), HD)]
        return remote(ref, ref, ys.at[index], yr.at[index], to)

    def compute(step, chip_rel):
        chip = peer(chip_rel) // 2
        total = jnp.zeros((2 * LOCAL, HD), F32)
        for i, head_rel in enumerate((0, D, X, Y)):
            for j in range(2):
                head = peer(head_rel) // 2 * 2 + j
                lhs = og[pl.ds(chip * 2, 2), head].reshape(2 * LOCAL, HD)
                rhs = wc_ref[span(head, HD), :] if i < 2 else wp[2 * (i - 2) + j]
                total = total + jnp.dot(lhs, rhs, preferred_element_type=F32)
        rows = pl.ds(pl.multiple_of(chip * 2 * LOCAL, 2 * LOCAL), 2 * LOCAL)
        y_ref[rows, cols] = (xc[rows, :].astype(F32) + total).astype(BF)
        b = step * 11
        go(y_copy(0, chip_rel, 0, X, b + 0))
        go(y_copy(0, chip_rel, 1, Y, b + 1))
        go(y_copy(0, chip_rel, 1, X, b + 2))
        go(y_copy(0, chip_rel, 0, Y, b + 3))
        go(y_copy(0, chip_rel, None, S, b + 4))

    recv_o(S, None, S, 4)
    compute(0, 0)
    recv_o(X, 0, X, 0)
    go(o_copy(X, 0, Y, 5))
    recv_o(Y, 1, Y, 1)
    go(o_copy(Y, 1, X, 6))
    recv_o(X, 1, X, 2)
    go(o_copy(X, None, S, 7))
    recv_o(Y, 0, Y, 3)
    go(o_copy(Y, None, S, 8))
    recv_o(X + S, None, S, 7)
    compute(1, X)
    recv_o(Y + S, None, S, 8)
    compute(2, Y)
    recv_o(D, 0, Y, 5)
    go(o_copy(D, 0, S, 9))
    recv_o(D, 1, X, 6)
    go(o_copy(D, 1, S, 10))
    recv_o(D + S, 0, S, 9)
    recv_o(D + S, 1, S, 10)
    compute(3, D)

    def xor(a, b):
        return ((a // 4 + b // 4) % 2) * 4 + ((a // 2 + b // 2) % 2) * 2 + (a + b) % 2

    order = (0, X, Y, D)
    for step, rel in enumerate(order):
        b = step * 11
        at_x, at_y, at_d = xor(rel, X), xor(rel, Y), xor(rel, D)
        y_copy(X, at_x, 0, X, b + 0).wait_recv()
        go(y_copy(X, at_x, 0, Y, b + 5))
        y_copy(Y, at_y, 1, Y, b + 1).wait_recv()
        go(y_copy(Y, at_y, 1, X, b + 6))
        y_copy(X, at_x, 1, X, b + 2).wait_recv()
        go(y_copy(X, at_x, None, S, b + 7))
        y_copy(Y, at_y, 0, Y, b + 3).wait_recv()
        go(y_copy(Y, at_y, None, S, b + 8))
    for step, rel in enumerate(order):
        b = step * 11
        at_d = xor(rel, D)
        y_copy(D, at_d, 0, Y, b + 5).wait_recv()
        go(y_copy(D, at_d, 0, S, b + 9))
        y_copy(D, at_d, 1, X, b + 6).wait_recv()
        go(y_copy(D, at_d, 1, S, b + 10))
    for step, rel in enumerate(order):
        b = step * 11
        at_x, at_y, at_d = xor(rel, X), xor(rel, Y), xor(rel, D)
        y_copy(S, rel, None, S, b + 4).wait_recv()
        y_copy(X + S, at_x, None, S, b + 7).wait_recv()
        y_copy(Y + S, at_y, None, S, b + 8).wait_recv()
        y_copy(D + S, at_d, 0, S, b + 9).wait_recv()
        y_copy(D + S, at_d, 1, S, b + 10).wait_recv()
    for copy in started:
        copy.wait_send()


def output(o, wc, wx, wy, x):
    rows, width = x.shape
    hbm_spec = pl.BlockSpec(memory_space=pltpu.HBM)
    vmem_spec = pl.BlockSpec(memory_space=pltpu.VMEM)
    return pl.pallas_call(
        output_kernel,
        out_shape=jax.ShapeDtypeStruct((rows, width), BF),
        in_specs=[vmem_spec, vmem_spec, hbm_spec, hbm_spec, hbm_spec],
        out_specs=vmem_spec,
        scratch_shapes=[
            pltpu.VMEM((8, HEADS, LOCAL, HD), BF),
            pltpu.VMEM((rows, HD), BF),
            pltpu.VMEM((4, HD, HD), BF),
            pltpu.SemaphoreType.DMA((3,)),
            pltpu.SemaphoreType.DMA((2,)),
            pltpu.SemaphoreType.DMA((2,)),
            pltpu.SemaphoreType.DMA((11,)),
            pltpu.SemaphoreType.DMA((11,)),
            pltpu.SemaphoreType.DMA((44,)),
            pltpu.SemaphoreType.DMA((44,)),
        ],
        compiler_params=pltpu.CompilerParams(collective_id=1, has_side_effects=True, vmem_limit_bytes=24 * MIB),
        name="output",
    )(o, wc, wx, wy, x)


def solution(mesh):
    def local_step(x, w_query, w_key, w_value, w_out, k_cache, v_cache, lengths):
        x, w_query, w_key, w_value, w_out = (
            pltpu.with_memory_space_constraint(a, pltpu.HBM) for a in (x, w_query, w_key, w_value, w_out))
        pinned = pltpu.with_memory_space_constraint(lengths, pltpu.HBM)
        q, k_new, v_new, w_cols, o_short, wx, wy = project(pinned, x, w_query, w_key, w_value, w_out, k_cache, v_cache)
        wx, wy = (lax.ppermute(w, "model", [(d, d ^ rel) for d in range(8)]) for w, rel in ((wx, X), (wy, Y)))
        o, k_new, v_new = attend(lengths, q, k_new, v_new, o_short, k_cache, v_cache)
        y = output(o, w_cols, wx, wy, x)
        return y, k_new[:, None, :], v_new[:, None, :]

    rows_spec = P("replica")
    return jax.shard_map(
        local_step,
        mesh=mesh,
        in_specs=(P("replica", None), P(None, "model"), P(), P(), P("model", None), rows_spec, rows_spec, rows_spec),
        out_specs=(rows_spec, rows_spec, rows_spec),
        check_vma=False,
    )
```

```python
import jax
import jax.numpy as jnp
from jax import lax
from jax.experimental import pallas as pl
from jax.experimental.pallas import tpu as pltpu
from jax.sharding import PartitionSpec as P

BF = jnp.bfloat16
F32 = jnp.float32
HEADS = 8
HD = 256
LOCAL = 64
SHORT = 32
GROUP = 16
CHUNK = 256
MAXLEN = 2048
SLOTS = 6
AHEAD = 4
HALFW = 128
MIB = 2 ** 20
SCALE = HD ** -0.5
DIMS_T = (((1,), (1,)), ((), ()))


def coords():
    me = lax.axis_index("model")
    return me, me // 4, (me // 2) % 2, me % 2


def peer(rel):
    _, y, x, k = coords()
    dy, dx, dk = rel // 4, (rel // 2) % 2, rel % 2
    return (((y + dy) % 2) * 2 + (x + dx) % 2) * 2 + (k + dk) % 2


def span(index, size):
    return pl.ds(pl.multiple_of(index * size, size), size)


def entry_barrier(rels):
    barrier = pltpu.get_barrier_semaphore()
    for rel in rels:
        pl.semaphore_signal(barrier, inc=1, device_id={"model": peer(rel)}, device_id_type=pl.DeviceIdType.MESH)
    pl.semaphore_wait(barrier, len(rels))


def remote(src, dst, send_sem, recv_sem, rel):
    return pltpu.make_async_remote_copy(
        src_ref=src, dst_ref=dst, send_sem=send_sem, recv_sem=recv_sem,
        device_id={"model": peer(rel)}, device_id_type=pl.DeviceIdType.MESH)


RELS = (6, 7, 2, 3, 4, 5, 1)


def softmax_parts(s, s_new):
    m = jnp.maximum(jnp.max(s, axis=-1, keepdims=True), s_new)
    e = jnp.exp(s - m)
    e_new = jnp.exp(s_new - m)
    total = jnp.sum(e, axis=-1, keepdims=True) + e_new
    return e.astype(BF), e_new.astype(BF).astype(F32), total


def project_kernel(len_hbm, x_hbm, wq_hbm, wk_hbm, wv_hbm, wo_hbm, k_hbm, v_hbm, q_out, kn_out, vn_out, wd_out, o_out, wx_out, wy_out,
                   x_v, wq_v, wk_v, wv_v, wo_v, q_v, ks, vs, lens_v, len_ref, in_sem, own_sem, qs, qr, ws, wr):
    me, y, x, k = coords()
    mine = span(me, LOCAL)
    loads = [pltpu.make_async_copy(src, dst, in_sem.at[i]) for i, (src, dst) in enumerate((
        (wq_hbm, wq_v),
        (wo_hbm, wo_v),
        (wk_hbm, wk_v),
        (wv_hbm, wv_v),
        (k_hbm.at[mine, 0, pl.ds(0, SHORT), :], ks),
        (v_hbm.at[mine, 0, pl.ds(0, SHORT), :], vs),
        (len_hbm, len_ref),
    ))]
    loads[0].start()
    blocks = []
    for i, chip_rel in enumerate((6, 2, 4, 0)):
        rows = span(peer(chip_rel) // 2, 2 * LOCAL)
        blocks.append(pltpu.make_async_copy(x_hbm.at[rows, :], x_v.at[rows, :], in_sem.at[7 + i]))
        blocks[-1].start()
    loads[1].start()
    entry_barrier(RELS)
    loads[0].wait()
    q_copies, w_copies = [], []
    for i, chip_rel in enumerate((6, 2, 4, 0)):
        rows = span(peer(chip_rel) // 2, 2 * LOCAL)
        blocks[i].wait()
        q_v[rows, :] = jnp.dot(x_v[rows, :], wq_v[...], preferred_element_type=F32).astype(BF)
        for rel in (chip_rel, chip_rel + 1):
            if rel == 0:
                continue
            copy = remote(q_v.at[span(peer(rel), LOCAL), :], q_out.at[me], qs.at[rel], qr.at[rel], rel)
            copy.start()
            q_copies.append(copy)
    loads[1].wait()
    w_copies.append(remote(wo_v.at[:, span(peer(6) // 2, 2 * HD)], wd_out, ws.at[0], wr.at[0], 6))
    w_copies[0].start()
    stores = [pltpu.make_async_copy(wo_v.at[:, span(peer(rel) // 2, 2 * HD)], out, own_sem.at[i])
              for i, (rel, out) in enumerate(((X, wx_out), (Y, wy_out)))]
    for store in stores:
        store.start()
    for load in loads[2:7]:
        load.start()
    q_out[me] = q_v[mine, :]

    def spread(i, carry):
        lens_v[pl.ds(i, 1), :] = jnp.full((1, 128), len_ref[me * LOCAL + i], jnp.int32)
        return carry

    loads[6].wait()
    lax.fori_loop(0, LOCAL, spread, 0)
    for load in loads[2:6]:
        load.wait()
    for part in range(2):
        rows = pl.ds(part * 256, 256)
        kn_out[rows, :] = jnp.dot(x_v[rows, :], wk_v[...], preferred_element_type=F32).astype(BF)
        vn_out[rows, :] = jnp.dot(x_v[rows, :], wv_v[...], preferred_element_type=F32).astype(BF)
    for copy in q_copies:
        copy.wait()

    width = GROUP * SHORT
    col = lax.broadcasted_iota(jnp.int32, (GROUP, width), 1)
    same = (col // SHORT) == lax.broadcasted_iota(jnp.int32, (GROUP, width), 0)
    slot_pos = col % SHORT

    def group(g, carry):
        seqs = span(g, GROUP)
        new = pl.ds(pl.multiple_of(me * LOCAL + g * GROUP, GROUP), GROUP)
        qg = q_out[:, seqs, :]
        s = lax.dot_general(qg.reshape(HEADS * GROUP, HD), ks[seqs].reshape(width, HD), DIMS_T, preferred_element_type=F32) * SCALE
        valid = same & (slot_pos < lens_v[seqs, 0:1])
        s = jnp.where(valid[None], s.reshape(HEADS, GROUP, width), -jnp.inf)
        s_new = jnp.sum(qg.astype(F32) * kn_out[new, :].astype(F32)[None], axis=-1, keepdims=True) * SCALE
        e, e_new, total = softmax_parts(s, s_new)
        num = jnp.dot(e.reshape(HEADS * GROUP, width), vs[seqs].reshape(width, HD), preferred_element_type=F32)
        num = num.reshape(HEADS, GROUP, HD) + e_new * vn_out[new, :].astype(F32)[None]
        o_out[:, seqs, :] = (num / total).astype(BF)
        return carry

    lax.fori_loop(0, LOCAL // GROUP, group, 0)
    for copy in w_copies + stores:
        copy.wait()


def project(lengths, x, wq, wk, wv, wo, k_cache, v_cache):
    rows, depth = x.shape
    hbm_spec = pl.BlockSpec(memory_space=pltpu.HBM)
    vmem_spec = pl.BlockSpec(memory_space=pltpu.VMEM)
    return pl.pallas_call(
        project_kernel,
        out_shape=(
            jax.ShapeDtypeStruct((HEADS, LOCAL, HD), BF),
            jax.ShapeDtypeStruct((rows, HD), BF),
            jax.ShapeDtypeStruct((rows, HD), BF),
            jax.ShapeDtypeStruct((HD, 2 * HD), BF),
            jax.ShapeDtypeStruct((HEADS, LOCAL, HD), BF),
            jax.ShapeDtypeStruct((HD, 2 * HD), BF),
            jax.ShapeDtypeStruct((HD, 2 * HD), BF),
        ),
        in_specs=[hbm_spec] * 8,
        out_specs=(vmem_spec,) * 5 + (hbm_spec,) * 2,
        scratch_shapes=[
            pltpu.VMEM((rows, depth), BF),
            pltpu.VMEM((depth, HD), BF),
            pltpu.VMEM((depth, HD), BF),
            pltpu.VMEM((depth, HD), BF),
            pltpu.VMEM(wo.shape, BF),
            pltpu.VMEM((rows, HD), BF),
            pltpu.VMEM((LOCAL, SHORT, HD), BF),
            pltpu.VMEM((LOCAL, SHORT, HD), BF),
            pltpu.VMEM((LOCAL, 128), jnp.int32),
            pltpu.SMEM(lengths.shape, jnp.int32),
            pltpu.SemaphoreType.DMA((11,)),
            pltpu.SemaphoreType.DMA((2,)),
            pltpu.SemaphoreType.DMA((8,)),
            pltpu.SemaphoreType.DMA((8,)),
            pltpu.SemaphoreType.DMA((1,)),
            pltpu.SemaphoreType.DMA((1,)),
        ],
        compiler_params=pltpu.CompilerParams(collective_id=0, has_side_effects=True, vmem_limit_bytes=24 * MIB),
        name="project",
    )(lengths, x, wq, wk, wv, wo, k_cache, v_cache)


def attend_kernel(len_ref, q_ref, kn_ref, vn_ref, os_ref, k_hbm, v_hbm, o_ref, kn_out, vn_out,
                  kl, vl, qf, knf, vnf, acc, lidx, lchunks, k_sem, v_sem, new_sem):
    me = lax.axis_index("model")
    base = me * LOCAL
    new_k = pltpu.make_async_copy(kn_ref, kn_out, new_sem.at[0])
    new_v = pltpu.make_async_copy(vn_ref, vn_out, new_sem.at[1])

    def each_part(i, slot, action):
        seq = base + lidx[i]
        chunks = lchunks[i]
        first = 0
        for size in (8, 4, 2, 1):
            rows = pl.ds(pl.multiple_of(first * CHUNK, CHUNK), size * CHUNK)

            @pl.when(chunks & size != 0)
            def _():
                for cache, dst, sem in ((k_hbm, kl, k_sem), (v_hbm, vl, v_sem)):
                    for half in range(2):
                        action(pltpu.make_async_copy(
                            cache.at[seq, 0, rows, pl.ds(half * HALFW, HALFW)],
                            dst.at[slot, half, rows, :], sem.at[slot]))

            first = first + (chunks & size)

    def fetch(i, slot, priority=1):
        each_part(i, slot, lambda copy: copy.start(priority=priority))

    def scan(i, count):
        length = len_ref[base + i]
        lidx[count] = i
        lchunks[count] = jnp.right_shift(length + (CHUNK - 1), CHUNK.bit_length() - 1)
        is_long = length > SHORT

        @pl.when(is_long & (count < 2))
        def _():
            fetch(count, count, 0)

        @pl.when(is_long & (count >= 2) & (count < AHEAD))
        def _():
            fetch(count, count)

        return count + jnp.where(is_long, 1, 0)

    n_long = lax.fori_loop(0, LOCAL, scan, jnp.int32(0))
    new_k.start()
    new_v.start()
    own = span(me, LOCAL)
    qf[...] = q_ref[...].astype(F32)
    knf[...] = kn_ref[own, :].astype(F32)
    vnf[...] = vn_ref[own, :].astype(F32)
    acc[...] = os_ref[...].astype(F32)

    def rows_of(ref, slot, rows):
        return jnp.concatenate([ref[slot, half, pl.ds(0, rows), :] for half in range(2)], axis=-1)

    def one_long(i, slot, rows):
        seq = lidx[i]
        at = pl.ds(seq, 1)
        q8 = jnp.concatenate([qf[h, at, :] for h in range(HEADS)], axis=0)
        s = lax.dot_general(q8.astype(BF), rows_of(kl, slot, rows), DIMS_T, preferred_element_type=F32) * SCALE
        s = jnp.where(lax.broadcasted_iota(jnp.int32, s.shape, 1) < len_ref[base + seq], s, -jnp.inf)
        s_new = jnp.sum(q8 * knf[at, :], axis=-1, keepdims=True) * SCALE
        e, e_new, total = softmax_parts(s, s_new)
        num = jnp.dot(e, rows_of(vl, slot, rows), preferred_element_type=F32)
        return seq, (num + e_new * vnf[at, :]) / total

    def wait_and_clear(i, slot, most):
        each_part(i, slot, lambda copy: copy.wait())

        @pl.loop(lchunks[i], most)
        def _(c):
            vl[slot, :, span(c, CHUNK), :] = jnp.zeros((2, CHUNK, HALFW), BF)

    def step(pair, slot):
        a = pair * 2
        alone = a + 1 >= n_long
        b = jnp.where(alone, a, a + 1)
        slot_b = jnp.where(alone, slot, slot + 1)
        most = jnp.maximum(lchunks[a], lchunks[b])
        wait_and_clear(a, slot, most)

        @pl.when(jnp.logical_not(alone))
        def _():
            wait_and_clear(b, slot + 1, most)

        later = jnp.where(slot >= SLOTS - AHEAD, slot + AHEAD - SLOTS, slot + AHEAD)
        for j in range(2):
            @pl.when(a + AHEAD + j < n_long)
            def _():
                fetch(a + AHEAD + j, later + j)

        for n in range(1, MAXLEN // CHUNK + 1):
            @pl.when(most == n)
            def _():
                results = [one_long(i, at, n * CHUNK) for i, at in ((a, slot), (b, slot_b))]
                for seq, out in results:
                    for h in range(HEADS):
                        acc[h, pl.ds(seq, 1), :] = out[h:h + 1, :]

        return jnp.where(slot + 2 >= SLOTS, 0, slot + 2)

    lax.fori_loop(0, jnp.right_shift(n_long + 1, 1), step, jnp.int32(0))
    o_ref[...] = acc[...].astype(BF)
    new_k.wait()
    new_v.wait()


def attend(lengths, q, k_new, v_new, o_short, k_cache, v_cache):
    rows = k_new.shape[0]
    any_spec = pl.BlockSpec(memory_space=pl.ANY)
    vmem_spec = pl.BlockSpec(memory_space=pltpu.VMEM)
    return pl.pallas_call(
        attend_kernel,
        out_shape=(
            jax.ShapeDtypeStruct((HEADS, LOCAL, HD), BF),
            jax.ShapeDtypeStruct((rows, HD), BF),
            jax.ShapeDtypeStruct((rows, HD), BF),
        ),
        in_specs=[pl.BlockSpec(memory_space=pltpu.SMEM)] + [vmem_spec] * 4 + [any_spec] * 2,
        out_specs=(vmem_spec, any_spec, any_spec),
        scratch_shapes=[
            pltpu.VMEM((SLOTS, 2, MAXLEN, HALFW), BF),
            pltpu.VMEM((SLOTS, 2, MAXLEN, HALFW), BF),
            pltpu.VMEM((HEADS, LOCAL, HD), F32),
            pltpu.VMEM((LOCAL, HD), F32),
            pltpu.VMEM((LOCAL, HD), F32),
            pltpu.VMEM((HEADS, LOCAL, HD), F32),
            pltpu.SMEM((LOCAL + 8,), jnp.int32),
            pltpu.SMEM((LOCAL + 8,), jnp.int32),
            pltpu.SemaphoreType.DMA((SLOTS,)),
            pltpu.SemaphoreType.DMA((SLOTS,)),
            pltpu.SemaphoreType.DMA((2,)),
        ],
        compiler_params=pltpu.CompilerParams(vmem_limit_bytes=24 * MIB),
        cost_estimate=pl.CostEstimate(flops=4 * 10 ** 9, bytes_accessed=10 ** 7, transcendentals=10 ** 6),
        name="attend",
    )(lengths, q, k_new, v_new, o_short, k_cache, v_cache)


HALF = HEADS // 2
X, Y, D, S = 2, 4, 6, 1
MSGS = 11


def output_kernel(o_ref, wo_hbm, wx_ref, wy_ref, wd_ref, x_hbm, y_ref, og, wc, xc, load_sem, wss, wrs, os, orr, ys, yr):
    me, _, _, _ = coords()
    chip = me // 2
    load_x = pltpu.make_async_copy(x_hbm.at[:, span(chip, 2 * HD)], xc, load_sem.at[0])
    load_x.start()
    w_loads, w_copies, w_recvs = [], [], []
    for i, (rel, ref) in enumerate(((0, wo_hbm.at[:, span(chip, 2 * HD)]), (D, wd_ref), (X, wx_ref), (Y, wy_ref))):
        w_loads.append(pltpu.make_async_copy(ref, wc.at[peer(rel)], load_sem.at[1 + i]))
        w_loads[-1].start()
        w_copies.append(remote(ref, wc.at[peer(rel)], wss.at[i], wrs.at[i], S))
        w_recvs.append(remote(ref, wc.at[peer(rel + S)], wss.at[i], wrs.at[i], S))
    entry_barrier((X, Y, S))
    started = []

    def go(copy):
        copy.start()
        started.append(copy)

    def o_copy(owner_rel, half, to, index):
        part = pl.ds(half * HALF, HALF)
        dst = og.at[peer(owner_rel) // 2, part]
        return remote(o_ref.at[part] if owner_rel == 0 else dst, dst, os.at[index], orr.at[index], to)

    def y_copy(col_rel, row_rel, half, to, index):
        if half is None:
            rows = span(peer(row_rel), LOCAL)
        else:
            rows = span(peer(row_rel) * 2 + half, LOCAL // 2)
        ref = y_ref.at[rows, span(peer(col_rel) // 2, 2 * HD)]
        return remote(ref, ref, ys.at[index], yr.at[index], to)

    def compute(step, rel):
        total = jnp.zeros((LOCAL, 2 * HD), F32)
        for h in range(HEADS):
            total = total + jnp.dot(og[peer(rel) // 2, h], wc[h], preferred_element_type=F32)
        rows = span(peer(rel), LOCAL)
        y_ref[rows, span(chip, 2 * HD)] = (xc[rows, :].astype(F32) + total).astype(BF)
        b = step * MSGS
        go(y_copy(0, rel, 0, X, b + 0))
        go(y_copy(0, rel, 1, Y, b + 1))
        go(y_copy(0, rel, 1, X, b + 2))
        go(y_copy(0, rel, 0, Y, b + 3))
        go(y_copy(0, rel, None, S, b + 4))

    go(o_copy(0, 0, X, 0))
    go(o_copy(0, 1, Y, 1))
    go(o_copy(0, 1, X, 2))
    go(o_copy(0, 0, Y, 3))
    for c in w_copies:
        go(c)
    og[chip] = o_ref[...]
    load_x.wait()
    for load in w_loads:
        load.wait()
    for c in w_recvs:
        c.wait_recv()
    compute(0, 0)
    o_copy(X, 0, X, 0).wait_recv()
    go(o_copy(X, 0, Y, 4))
    o_copy(Y, 1, Y, 1).wait_recv()
    go(o_copy(Y, 1, X, 5))
    o_copy(X, 1, X, 2).wait_recv()
    compute(1, X)
    o_copy(Y, 0, Y, 3).wait_recv()
    compute(2, Y)
    o_copy(D, 0, Y, 4).wait_recv()
    o_copy(D, 1, X, 5).wait_recv()
    compute(3, D)

    def xor(a, b):
        return ((a // 4 + b // 4) % 2) * 4 + ((a // 2 + b // 2) % 2) * 2 + (a + b) % 2

    order = (0, X, Y, D)
    for step, rel in enumerate(order):
        b = step * MSGS
        at_x, at_y = xor(rel, X), xor(rel, Y)
        y_copy(X, at_x, 0, X, b + 0).wait_recv()
        go(y_copy(X, at_x, 0, Y, b + 5))
        y_copy(Y, at_y, 1, Y, b + 1).wait_recv()
        go(y_copy(Y, at_y, 1, X, b + 6))
        y_copy(X, at_x, 1, X, b + 2).wait_recv()
        go(y_copy(X, at_x, None, S, b + 7))
        y_copy(Y, at_y, 0, Y, b + 3).wait_recv()
        go(y_copy(Y, at_y, None, S, b + 8))
    for step, rel in enumerate(order):
        b = step * MSGS
        at_d = xor(rel, D)
        y_copy(D, at_d, 0, Y, b + 5).wait_recv()
        go(y_copy(D, at_d, 0, S, b + 9))
        y_copy(D, at_d, 1, X, b + 6).wait_recv()
        go(y_copy(D, at_d, 1, S, b + 10))
    for step, rel in enumerate(order):
        b = step * MSGS
        y_copy(S, rel + S, None, S, b + 4).wait_recv()
        y_copy(X + S, xor(rel, X) + S, None, S, b + 7).wait_recv()
        y_copy(Y + S, xor(rel, Y) + S, None, S, b + 8).wait_recv()
        y_copy(D + S, xor(rel, D) + S, 0, S, b + 9).wait_recv()
        y_copy(D + S, xor(rel, D) + S, 1, S, b + 10).wait_recv()
    for copy in started:
        copy.wait_send()


def output(o, wo, wx, wy, wd, x):
    rows, width = x.shape
    hbm_spec = pl.BlockSpec(memory_space=pltpu.HBM)
    vmem_spec = pl.BlockSpec(memory_space=pltpu.VMEM)
    return pl.pallas_call(
        output_kernel,
        out_shape=jax.ShapeDtypeStruct((rows, width), BF),
        in_specs=[vmem_spec] + [hbm_spec] * 3 + [vmem_spec, hbm_spec],
        out_specs=vmem_spec,
        scratch_shapes=[
            pltpu.VMEM((4, HEADS, LOCAL, HD), BF),
            pltpu.VMEM((HEADS, HD, 2 * HD), BF),
            pltpu.VMEM((rows, 2 * HD), BF),
            pltpu.SemaphoreType.DMA((5,)),
            pltpu.SemaphoreType.DMA((4,)),
            pltpu.SemaphoreType.DMA((4,)),
            pltpu.SemaphoreType.DMA((6,)),
            pltpu.SemaphoreType.DMA((6,)),
            pltpu.SemaphoreType.DMA((4 * MSGS,)),
            pltpu.SemaphoreType.DMA((4 * MSGS,)),
        ],
        compiler_params=pltpu.CompilerParams(collective_id=1, has_side_effects=True, vmem_limit_bytes=24 * MIB),
        name="output",
    )(o, wo, wx, wy, wd, x)


def solution(mesh):
    def local_step(x, w_query, w_key, w_value, w_out, k_cache, v_cache, lengths):
        x, w_query, w_key, w_value, w_out = (
            pltpu.with_memory_space_constraint(a, pltpu.HBM) for a in (x, w_query, w_key, w_value, w_out))
        pinned = pltpu.with_memory_space_constraint(lengths, pltpu.HBM)
        q, k_new, v_new, wd, o_short, wx, wy = project(pinned, x, w_query, w_key, w_value, w_out, k_cache, v_cache)
        wx, wy = (lax.ppermute(w, "model", [(d, d ^ rel) for d in range(8)]) for w, rel in ((wx, X), (wy, Y)))
        o, k_new, v_new = attend(lengths, q, k_new, v_new, o_short, k_cache, v_cache)
        y = output(o, w_out, wx, wy, wd, x)
        return y, k_new[:, None, :], v_new[:, None, :]

    rows_spec = P("replica")
    return jax.shard_map(
        local_step,
        mesh=mesh,
        in_specs=(P("replica", None), P(None, "model"), P(), P(), P("model", None), rows_spec, rows_spec, rows_spec),
        out_specs=(rows_spec, rows_spec, rows_spec),
        check_vma=False,
    )
```

```python
import jax
import jax.numpy as jnp
from jax import lax
from jax.experimental import pallas as pl
from jax.experimental.pallas import tpu as pltpu
from jax.sharding import PartitionSpec as P

BF = jnp.bfloat16
F32 = jnp.float32
HEADS = 8
HD = 256
LOCAL = 64
SHORT = 32
GROUP = 16
CHUNK = 256
MAXLEN = 2048
SLOTS = 6
AHEAD = 4
HALFW = 128
MIB = 2 ** 20
SCALE = HD ** -0.5
DIMS_T = (((1,), (1,)), ((), ()))


def coords():
    me = lax.axis_index("model")
    return me, me // 4, (me // 2) % 2, me % 2


def peer(rel):
    _, y, x, k = coords()
    dy, dx, dk = rel // 4, (rel // 2) % 2, rel % 2
    return (((y + dy) % 2) * 2 + (x + dx) % 2) * 2 + (k + dk) % 2


def span(index, size):
    return pl.ds(pl.multiple_of(index * size, size), size)


def entry_barrier(rels):
    barrier = pltpu.get_barrier_semaphore()
    for rel in rels:
        pl.semaphore_signal(barrier, inc=1, device_id={"model": peer(rel)}, device_id_type=pl.DeviceIdType.MESH)
    pl.semaphore_wait(barrier, len(rels))


def remote(src, dst, send_sem, recv_sem, rel):
    return pltpu.make_async_remote_copy(
        src_ref=src, dst_ref=dst, send_sem=send_sem, recv_sem=recv_sem,
        device_id={"model": peer(rel)}, device_id_type=pl.DeviceIdType.MESH)


RELS = (6, 7, 2, 3, 4, 5, 1)


def softmax_parts(s, s_new):
    m = jnp.maximum(jnp.max(s, axis=-1, keepdims=True), s_new)
    e = jnp.exp(s - m)
    e_new = jnp.exp(s_new - m)
    total = jnp.sum(e, axis=-1, keepdims=True) + e_new
    return e.astype(BF), e_new.astype(BF).astype(F32), total


def project_kernel(len_hbm, x_hbm, wq_hbm, wk_hbm, wv_hbm, wo_hbm, k_hbm, v_hbm, q_out, kn_out, vn_out, wx_out, wy_out, o_out, wd_out,
                   x_v, wq_v, wk_v, wv_v, wo_v, q_v, ks, vs, lens_v, len_ref, in_sem, own_sem, qs, qr, ws, wr):
    me, y, x, k = coords()
    mine = span(me, LOCAL)
    loads = [pltpu.make_async_copy(src, dst, in_sem.at[i]) for i, (src, dst) in enumerate((
        (wq_hbm, wq_v),
        (wo_hbm, wo_v),
        (wk_hbm, wk_v),
        (wv_hbm, wv_v),
        (k_hbm.at[mine, 0, pl.ds(0, SHORT), :], ks),
        (v_hbm.at[mine, 0, pl.ds(0, SHORT), :], vs),
        (len_hbm, len_ref),
    ))]
    loads[0].start()
    blocks = []
    for i, chip_rel in enumerate((6, 2, 4, 0)):
        rows = span(peer(chip_rel) // 2, 2 * LOCAL)
        blocks.append(pltpu.make_async_copy(x_hbm.at[rows, :], x_v.at[rows, :], in_sem.at[7 + i]))
        blocks[-1].start()
    loads[1].start()
    entry_barrier(RELS)
    loads[0].wait()
    q_copies, w_copies = [], []
    for i, chip_rel in enumerate((6, 2, 4, 0)):
        rows = span(peer(chip_rel) // 2, 2 * LOCAL)
        blocks[i].wait()
        q_v[rows, :] = jnp.dot(x_v[rows, :], wq_v[...], preferred_element_type=F32).astype(BF)
        for rel in (chip_rel, chip_rel + 1):
            if rel == 0:
                continue
            copy = remote(q_v.at[span(peer(rel), LOCAL), :], q_out.at[me], qs.at[rel], qr.at[rel], rel)
            copy.start()
            q_copies.append(copy)
    loads[1].wait()
    for i, (rel, out) in enumerate(((X, wx_out), (Y, wy_out))):
        w_copies.append(remote(wo_v.at[:, span(peer(rel) // 2, 2 * HD)], out, ws.at[i], wr.at[i], rel))
        w_copies[i].start()
    store = pltpu.make_async_copy(wo_v.at[:, span(peer(D) // 2, 2 * HD)], wd_out, own_sem)
    store.start()
    for load in loads[2:7]:
        load.start()
    q_out[me] = q_v[mine, :]

    def spread(i, carry):
        lens_v[pl.ds(i, 1), :] = jnp.full((1, 128), len_ref[me * LOCAL + i], jnp.int32)
        return carry

    loads[6].wait()
    lax.fori_loop(0, LOCAL, spread, 0)
    for load in loads[2:6]:
        load.wait()
    for part in range(2):
        rows = pl.ds(part * 256, 256)
        kn_out[rows, :] = jnp.dot(x_v[rows, :], wk_v[...], preferred_element_type=F32).astype(BF)
        vn_out[rows, :] = jnp.dot(x_v[rows, :], wv_v[...], preferred_element_type=F32).astype(BF)
    for copy in q_copies:
        copy.wait()

    width = GROUP * SHORT
    col = lax.broadcasted_iota(jnp.int32, (GROUP, width), 1)
    same = (col // SHORT) == lax.broadcasted_iota(jnp.int32, (GROUP, width), 0)
    slot_pos = col % SHORT

    def group(g, carry):
        seqs = span(g, GROUP)
        new = pl.ds(pl.multiple_of(me * LOCAL + g * GROUP, GROUP), GROUP)
        qg = q_out[:, seqs, :]
        s = lax.dot_general(qg.reshape(HEADS * GROUP, HD), ks[seqs].reshape(width, HD), DIMS_T, preferred_element_type=F32) * SCALE
        valid = same & (slot_pos < lens_v[seqs, 0:1])
        s = jnp.where(valid[None], s.reshape(HEADS, GROUP, width), -jnp.inf)
        s_new = jnp.sum(qg.astype(F32) * kn_out[new, :].astype(F32)[None], axis=-1, keepdims=True) * SCALE
        e, e_new, total = softmax_parts(s, s_new)
        num = jnp.dot(e.reshape(HEADS * GROUP, width), vs[seqs].reshape(width, HD), preferred_element_type=F32)
        num = num.reshape(HEADS, GROUP, HD) + e_new * vn_out[new, :].astype(F32)[None]
        o_out[:, seqs, :] = (num / total).astype(BF)
        return carry

    lax.fori_loop(0, LOCAL // GROUP, group, 0)
    for copy in w_copies + [store]:
        copy.wait()


def project(lengths, x, wq, wk, wv, wo, k_cache, v_cache):
    rows, depth = x.shape
    hbm_spec = pl.BlockSpec(memory_space=pltpu.HBM)
    vmem_spec = pl.BlockSpec(memory_space=pltpu.VMEM)
    return pl.pallas_call(
        project_kernel,
        out_shape=(
            jax.ShapeDtypeStruct((HEADS, LOCAL, HD), BF),
            jax.ShapeDtypeStruct((rows, HD), BF),
            jax.ShapeDtypeStruct((rows, HD), BF),
            jax.ShapeDtypeStruct((HD, 2 * HD), BF),
            jax.ShapeDtypeStruct((HD, 2 * HD), BF),
            jax.ShapeDtypeStruct((HEADS, LOCAL, HD), BF),
            jax.ShapeDtypeStruct((HD, 2 * HD), BF),
        ),
        in_specs=[hbm_spec] * 8,
        out_specs=(vmem_spec,) * 6 + (hbm_spec,),
        scratch_shapes=[
            pltpu.VMEM((rows, depth), BF),
            pltpu.VMEM((depth, HD), BF),
            pltpu.VMEM((depth, HD), BF),
            pltpu.VMEM((depth, HD), BF),
            pltpu.VMEM(wo.shape, BF),
            pltpu.VMEM((rows, HD), BF),
            pltpu.VMEM((LOCAL, SHORT, HD), BF),
            pltpu.VMEM((LOCAL, SHORT, HD), BF),
            pltpu.VMEM((LOCAL, 128), jnp.int32),
            pltpu.SMEM(lengths.shape, jnp.int32),
            pltpu.SemaphoreType.DMA((11,)),
            pltpu.SemaphoreType.DMA,
            pltpu.SemaphoreType.DMA((8,)),
            pltpu.SemaphoreType.DMA((8,)),
            pltpu.SemaphoreType.DMA((2,)),
            pltpu.SemaphoreType.DMA((2,)),
        ],
        compiler_params=pltpu.CompilerParams(collective_id=0, has_side_effects=True, vmem_limit_bytes=24 * MIB),
        name="project",
    )(lengths, x, wq, wk, wv, wo, k_cache, v_cache)


def attend_kernel(len_ref, q_ref, kn_ref, vn_ref, os_ref, k_hbm, v_hbm, o_ref, kn_out, vn_out,
                  kl, vl, qf, knf, vnf, acc, lidx, lchunks, k_sem, v_sem, new_sem):
    me = lax.axis_index("model")
    base = me * LOCAL
    new_k = pltpu.make_async_copy(kn_ref, kn_out, new_sem.at[0])
    new_v = pltpu.make_async_copy(vn_ref, vn_out, new_sem.at[1])

    def each_part(i, slot, action):
        seq = base + lidx[i]
        chunks = lchunks[i]
        first = 0
        for size in (8, 4, 2, 1):
            rows = pl.ds(pl.multiple_of(first * CHUNK, CHUNK), size * CHUNK)

            @pl.when(chunks & size != 0)
            def _():
                for cache, dst, sem in ((k_hbm, kl, k_sem), (v_hbm, vl, v_sem)):
                    for half in range(2):
                        action(pltpu.make_async_copy(
                            cache.at[seq, 0, rows, pl.ds(half * HALFW, HALFW)],
                            dst.at[slot, half, rows, :], sem.at[slot]))

            first = first + (chunks & size)

    def fetch(i, slot, priority=1):
        each_part(i, slot, lambda copy: copy.start(priority=priority))

    def scan(i, count):
        length = len_ref[base + i]
        lidx[count] = i
        lchunks[count] = jnp.right_shift(length + (CHUNK - 1), CHUNK.bit_length() - 1)
        is_long = length > SHORT

        @pl.when(is_long & (count < 2))
        def _():
            fetch(count, count, 0)

        @pl.when(is_long & (count >= 2) & (count < AHEAD))
        def _():
            fetch(count, count)

        return count + jnp.where(is_long, 1, 0)

    n_long = lax.fori_loop(0, LOCAL, scan, jnp.int32(0))
    new_k.start()
    new_v.start()
    own = span(me, LOCAL)
    qf[...] = q_ref[...].astype(F32)
    knf[...] = kn_ref[own, :].astype(F32)
    vnf[...] = vn_ref[own, :].astype(F32)
    acc[...] = os_ref[...].astype(F32)

    def rows_of(ref, slot, rows):
        return jnp.concatenate([ref[slot, half, pl.ds(0, rows), :] for half in range(2)], axis=-1)

    def one_long(i, slot, rows):
        seq = lidx[i]
        at = pl.ds(seq, 1)
        q8 = jnp.concatenate([qf[h, at, :] for h in range(HEADS)], axis=0)
        s = lax.dot_general(q8.astype(BF), rows_of(kl, slot, rows), DIMS_T, preferred_element_type=F32) * SCALE
        s = jnp.where(lax.broadcasted_iota(jnp.int32, s.shape, 1) < len_ref[base + seq], s, -jnp.inf)
        s_new = jnp.sum(q8 * knf[at, :], axis=-1, keepdims=True) * SCALE
        e, e_new, total = softmax_parts(s, s_new)
        num = jnp.dot(e, rows_of(vl, slot, rows), preferred_element_type=F32)
        return seq, (num + e_new * vnf[at, :]) / total

    def wait_and_clear(i, slot, most):
        each_part(i, slot, lambda copy: copy.wait())

        @pl.loop(lchunks[i], most)
        def _(c):
            vl[slot, :, span(c, CHUNK), :] = jnp.zeros((2, CHUNK, HALFW), BF)

    def step(pair, slot):
        a = pair * 2
        alone = a + 1 >= n_long
        b = jnp.where(alone, a, a + 1)
        slot_b = jnp.where(alone, slot, slot + 1)
        most = jnp.maximum(lchunks[a], lchunks[b])
        wait_and_clear(a, slot, most)

        @pl.when(jnp.logical_not(alone))
        def _():
            wait_and_clear(b, slot + 1, most)

        later = jnp.where(slot >= SLOTS - AHEAD, slot + AHEAD - SLOTS, slot + AHEAD)
        for j in range(2):
            @pl.when(a + AHEAD + j < n_long)
            def _():
                fetch(a + AHEAD + j, later + j)

        for n in range(1, MAXLEN // CHUNK + 1):
            @pl.when(most == n)
            def _():
                results = [one_long(i, at, n * CHUNK) for i, at in ((a, slot), (b, slot_b))]
                for seq, out in results:
                    for h in range(HEADS):
                        acc[h, pl.ds(seq, 1), :] = out[h:h + 1, :]

        return jnp.where(slot + 2 >= SLOTS, 0, slot + 2)

    lax.fori_loop(0, jnp.right_shift(n_long + 1, 1), step, jnp.int32(0))
    o_ref[...] = acc[...].astype(BF)
    new_k.wait()
    new_v.wait()


def attend(lengths, q, k_new, v_new, o_short, k_cache, v_cache):
    rows = k_new.shape[0]
    any_spec = pl.BlockSpec(memory_space=pl.ANY)
    vmem_spec = pl.BlockSpec(memory_space=pltpu.VMEM)
    return pl.pallas_call(
        attend_kernel,
        out_shape=(
            jax.ShapeDtypeStruct((HEADS, LOCAL, HD), BF),
            jax.ShapeDtypeStruct((rows, HD), BF),
            jax.ShapeDtypeStruct((rows, HD), BF),
        ),
        in_specs=[pl.BlockSpec(memory_space=pltpu.SMEM)] + [vmem_spec] * 4 + [any_spec] * 2,
        out_specs=(vmem_spec, any_spec, any_spec),
        scratch_shapes=[
            pltpu.VMEM((SLOTS, 2, MAXLEN, HALFW), BF),
            pltpu.VMEM((SLOTS, 2, MAXLEN, HALFW), BF),
            pltpu.VMEM((HEADS, LOCAL, HD), F32),
            pltpu.VMEM((LOCAL, HD), F32),
            pltpu.VMEM((LOCAL, HD), F32),
            pltpu.VMEM((HEADS, LOCAL, HD), F32),
            pltpu.SMEM((LOCAL + 8,), jnp.int32),
            pltpu.SMEM((LOCAL + 8,), jnp.int32),
            pltpu.SemaphoreType.DMA((SLOTS,)),
            pltpu.SemaphoreType.DMA((SLOTS,)),
            pltpu.SemaphoreType.DMA((2,)),
        ],
        compiler_params=pltpu.CompilerParams(vmem_limit_bytes=24 * MIB),
        cost_estimate=pl.CostEstimate(flops=4 * 10 ** 9, bytes_accessed=10 ** 7, transcendentals=10 ** 6),
        name="attend",
    )(lengths, q, k_new, v_new, o_short, k_cache, v_cache)


HALF = HEADS // 2
X, Y, D, S = 2, 4, 6, 1
MSGS = 11


def output_kernel(o_ref, wo_hbm, wx_ref, wy_ref, wd_ref, x_hbm, y_ref, og, wc, xc, load_sem, wss, wrs, os, orr, ys, yr):
    me, _, _, _ = coords()
    chip = me // 2
    load_x = pltpu.make_async_copy(x_hbm.at[:, span(chip, 2 * HD)], xc, load_sem.at[0])
    load_x.start()
    w_loads, w_copies, w_recvs = [], [], []
    for i, (rel, ref) in enumerate(((0, wo_hbm.at[:, span(chip, 2 * HD)]), (D, wd_ref), (X, wx_ref), (Y, wy_ref))):
        w_loads.append(pltpu.make_async_copy(ref, wc.at[peer(rel)], load_sem.at[1 + i]))
        w_loads[-1].start()
        w_copies.append(remote(ref, wc.at[peer(rel)], wss.at[i], wrs.at[i], S))
        w_recvs.append(remote(ref, wc.at[peer(rel + S)], wss.at[i], wrs.at[i], S))
    entry_barrier((X, Y, S))
    started = []

    def go(copy):
        copy.start()
        started.append(copy)

    def o_copy(owner_rel, half, to, index):
        part = pl.ds(half * HALF, HALF)
        dst = og.at[peer(owner_rel) // 2, part]
        return remote(o_ref.at[part] if owner_rel == 0 else dst, dst, os.at[index], orr.at[index], to)

    def y_copy(col_rel, row_rel, half, to, index):
        if half is None:
            rows = span(peer(row_rel), LOCAL)
        else:
            rows = span(peer(row_rel) * 2 + half, LOCAL // 2)
        ref = y_ref.at[rows, span(peer(col_rel) // 2, 2 * HD)]
        return remote(ref, ref, ys.at[index], yr.at[index], to)

    def compute(step, rel):
        total = jnp.zeros((LOCAL, 2 * HD), F32)
        for h in range(HEADS):
            total = total + jnp.dot(og[peer(rel) // 2, h], wc[h], preferred_element_type=F32)
        rows = span(peer(rel), LOCAL)
        y_ref[rows, span(chip, 2 * HD)] = (xc[rows, :].astype(F32) + total).astype(BF)
        b = step * MSGS
        go(y_copy(0, rel, 0, X, b + 0))
        go(y_copy(0, rel, 1, Y, b + 1))
        go(y_copy(0, rel, 1, X, b + 2))
        go(y_copy(0, rel, 0, Y, b + 3))
        go(y_copy(0, rel, None, S, b + 4))

    go(o_copy(0, 0, X, 0))
    go(o_copy(0, 1, Y, 1))
    go(o_copy(0, 1, X, 2))
    go(o_copy(0, 0, Y, 3))
    for c in w_copies:
        go(c)
    og[chip] = o_ref[...]
    load_x.wait()
    for load in w_loads:
        load.wait()
    for c in w_recvs:
        c.wait_recv()
    compute(0, 0)
    o_copy(X, 0, X, 0).wait_recv()
    go(o_copy(X, 0, Y, 4))
    o_copy(Y, 1, Y, 1).wait_recv()
    go(o_copy(Y, 1, X, 5))
    o_copy(X, 1, X, 2).wait_recv()
    compute(1, X)
    o_copy(Y, 0, Y, 3).wait_recv()
    compute(2, Y)
    o_copy(D, 0, Y, 4).wait_recv()
    o_copy(D, 1, X, 5).wait_recv()
    compute(3, D)

    def xor(a, b):
        return ((a // 4 + b // 4) % 2) * 4 + ((a // 2 + b // 2) % 2) * 2 + (a + b) % 2

    order = (0, X, Y, D)
    for step, rel in enumerate(order):
        b = step * MSGS
        at_x, at_y = xor(rel, X), xor(rel, Y)
        y_copy(X, at_x, 0, X, b + 0).wait_recv()
        go(y_copy(X, at_x, 0, Y, b + 5))
        y_copy(Y, at_y, 1, Y, b + 1).wait_recv()
        go(y_copy(Y, at_y, 1, X, b + 6))
        y_copy(X, at_x, 1, X, b + 2).wait_recv()
        go(y_copy(X, at_x, None, S, b + 7))
        y_copy(Y, at_y, 0, Y, b + 3).wait_recv()
        go(y_copy(Y, at_y, None, S, b + 8))
    for step, rel in enumerate(order):
        b = step * MSGS
        at_d = xor(rel, D)
        y_copy(D, at_d, 0, Y, b + 5).wait_recv()
        go(y_copy(D, at_d, 0, S, b + 9))
        y_copy(D, at_d, 1, X, b + 6).wait_recv()
        go(y_copy(D, at_d, 1, S, b + 10))
    for step, rel in enumerate(order):
        b = step * MSGS
        y_copy(S, rel + S, None, S, b + 4).wait_recv()
        y_copy(X + S, xor(rel, X) + S, None, S, b + 7).wait_recv()
        y_copy(Y + S, xor(rel, Y) + S, None, S, b + 8).wait_recv()
        y_copy(D + S, xor(rel, D) + S, 0, S, b + 9).wait_recv()
        y_copy(D + S, xor(rel, D) + S, 1, S, b + 10).wait_recv()
    for copy in started:
        copy.wait_send()


def output(o, wo, wx, wy, wd, x):
    rows, width = x.shape
    hbm_spec = pl.BlockSpec(memory_space=pltpu.HBM)
    vmem_spec = pl.BlockSpec(memory_space=pltpu.VMEM)
    return pl.pallas_call(
        output_kernel,
        out_shape=jax.ShapeDtypeStruct((rows, width), BF),
        in_specs=[vmem_spec, hbm_spec, vmem_spec, vmem_spec, hbm_spec, hbm_spec],
        out_specs=vmem_spec,
        scratch_shapes=[
            pltpu.VMEM((4, HEADS, LOCAL, HD), BF),
            pltpu.VMEM((HEADS, HD, 2 * HD), BF),
            pltpu.VMEM((rows, 2 * HD), BF),
            pltpu.SemaphoreType.DMA((5,)),
            pltpu.SemaphoreType.DMA((4,)),
            pltpu.SemaphoreType.DMA((4,)),
            pltpu.SemaphoreType.DMA((6,)),
            pltpu.SemaphoreType.DMA((6,)),
            pltpu.SemaphoreType.DMA((4 * MSGS,)),
            pltpu.SemaphoreType.DMA((4 * MSGS,)),
        ],
        compiler_params=pltpu.CompilerParams(collective_id=1, has_side_effects=True, vmem_limit_bytes=24 * MIB),
        name="output",
    )(o, wo, wx, wy, wd, x)


def solution(mesh):
    def local_step(x, w_query, w_key, w_value, w_out, k_cache, v_cache, lengths):
        x, w_query, w_key, w_value, w_out = (
            pltpu.with_memory_space_constraint(a, pltpu.HBM) for a in (x, w_query, w_key, w_value, w_out))
        pinned = pltpu.with_memory_space_constraint(lengths, pltpu.HBM)
        q, k_new, v_new, wx, wy, o_short, wd = project(pinned, x, w_query, w_key, w_value, w_out, k_cache, v_cache)
        wd = lax.ppermute(wd, "model", [(d, d ^ D) for d in range(8)])
        o, k_new, v_new = attend(lengths, q, k_new, v_new, o_short, k_cache, v_cache)
        y = output(o, w_out, wx, wy, wd, x)
        return y, k_new[:, None, :], v_new[:, None, :]

    rows_spec = P("replica")
    return jax.shard_map(
        local_step,
        mesh=mesh,
        in_specs=(P("replica", None), P(None, "model"), P(), P(), P("model", None), rows_spec, rows_spec, rows_spec),
        out_specs=(rows_spec, rows_spec, rows_spec),
        check_vma=False,
    )
```

```python
import jax
import jax.numpy as jnp
from jax import lax
from jax.experimental import pallas as pl
from jax.experimental.pallas import tpu as pltpu
from jax.sharding import PartitionSpec as P

BF = jnp.bfloat16
F32 = jnp.float32
HEADS = 8
HD = 256
LOCAL = 64
SHORT = 32
GROUP = 16
CHUNK = 256
MAXLEN = 2048
SLOTS = 8
AHEAD = 4
HALFW = 128
MIB = 2 ** 20
SCALE = HD ** -0.5
DIMS_T = (((1,), (1,)), ((), ()))


def coords():
    me = lax.axis_index("model")
    return me, me // 4, (me // 2) % 2, me % 2


def peer(rel):
    _, y, x, k = coords()
    dy, dx, dk = rel // 4, (rel // 2) % 2, rel % 2
    return (((y + dy) % 2) * 2 + (x + dx) % 2) * 2 + (k + dk) % 2


def span(index, size):
    return pl.ds(pl.multiple_of(index * size, size), size)


def entry_barrier(rels):
    barrier = pltpu.get_barrier_semaphore()
    for rel in rels:
        pl.semaphore_signal(barrier, inc=1, device_id={"model": peer(rel)}, device_id_type=pl.DeviceIdType.MESH)
    pl.semaphore_wait(barrier, len(rels))


def remote(src, dst, send_sem, recv_sem, rel):
    return pltpu.make_async_remote_copy(
        src_ref=src, dst_ref=dst, send_sem=send_sem, recv_sem=recv_sem,
        device_id={"model": peer(rel)}, device_id_type=pl.DeviceIdType.MESH)


RELS = (6, 7, 2, 3, 4, 5, 1)


def softmax_parts(s, s_new):
    m = jnp.maximum(jnp.max(s, axis=-1, keepdims=True), s_new)
    e = jnp.exp(s - m)
    e_new = jnp.exp(s_new - m)
    total = jnp.sum(e, axis=-1, keepdims=True) + e_new
    return e.astype(BF), e_new.astype(BF).astype(F32), total


def project_kernel(len_hbm, x_hbm, wq_hbm, wk_hbm, wv_hbm, wo_hbm, k_hbm, v_hbm, q_out, kn_out, vn_out, wx_out, wy_out, o_out, wd_out,
                   x_v, wq_v, wk_v, wv_v, wo_v, q_v, ks, vs, lens_v, len_ref, in_sem, own_sem, qs, qr, ws, wr):
    me, y, x, k = coords()
    mine = span(me, LOCAL)
    loads = [pltpu.make_async_copy(src, dst, in_sem.at[i]) for i, (src, dst) in enumerate((
        (wq_hbm, wq_v),
        (wo_hbm, wo_v),
        (wk_hbm, wk_v),
        (wv_hbm, wv_v),
        (k_hbm.at[mine, 0, pl.ds(0, SHORT), :], ks),
        (v_hbm.at[mine, 0, pl.ds(0, SHORT), :], vs),
        (len_hbm, len_ref),
    ))]
    loads[0].start()
    blocks = []
    for i, chip_rel in enumerate((6, 2, 4, 0)):
        rows = span(peer(chip_rel) // 2, 2 * LOCAL)
        blocks.append(pltpu.make_async_copy(x_hbm.at[rows, :], x_v.at[rows, :], in_sem.at[7 + i]))
        blocks[-1].start()
    loads[1].start()
    entry_barrier(RELS)
    loads[0].wait()
    q_copies, w_copies = [], []
    for i, chip_rel in enumerate((6, 2, 4, 0)):
        rows = span(peer(chip_rel) // 2, 2 * LOCAL)
        blocks[i].wait()
        q_v[rows, :] = jnp.dot(x_v[rows, :], wq_v[...], preferred_element_type=F32).astype(BF)
        for rel in (chip_rel, chip_rel + 1):
            if rel == 0:
                continue
            copy = remote(q_v.at[span(peer(rel), LOCAL), :], q_out.at[me], qs.at[rel], qr.at[rel], rel)
            copy.start()
            q_copies.append(copy)
    loads[1].wait()
    for i, (rel, out) in enumerate(((X, wx_out), (Y, wy_out))):
        w_copies.append(remote(wo_v.at[:, span(peer(rel) // 2, 2 * HD)], out, ws.at[i], wr.at[i], rel))
        w_copies[i].start()
    store = pltpu.make_async_copy(wo_v.at[:, span(peer(D) // 2, 2 * HD)], wd_out, own_sem)
    store.start()
    for load in loads[2:7]:
        load.start()
    q_out[me] = q_v[mine, :]

    def spread(i, carry):
        lens_v[pl.ds(i, 1), :] = jnp.full((1, 128), len_ref[me * LOCAL + i], jnp.int32)
        return carry

    loads[6].wait()
    lax.fori_loop(0, LOCAL, spread, 0)
    for load in loads[2:6]:
        load.wait()
    for part in range(2):
        rows = pl.ds(part * 256, 256)
        kn_out[rows, :] = jnp.dot(x_v[rows, :], wk_v[...], preferred_element_type=F32).astype(BF)
        vn_out[rows, :] = jnp.dot(x_v[rows, :], wv_v[...], preferred_element_type=F32).astype(BF)
    for copy in q_copies:
        copy.wait()

    width = GROUP * SHORT
    col = lax.broadcasted_iota(jnp.int32, (GROUP, width), 1)
    same = (col // SHORT) == lax.broadcasted_iota(jnp.int32, (GROUP, width), 0)
    slot_pos = col % SHORT

    def group(g, carry):
        seqs = span(g, GROUP)
        new = pl.ds(pl.multiple_of(me * LOCAL + g * GROUP, GROUP), GROUP)
        qg = q_out[:, seqs, :]
        s = lax.dot_general(qg.reshape(HEADS * GROUP, HD), ks[seqs].reshape(width, HD), DIMS_T, preferred_element_type=F32) * SCALE
        valid = same & (slot_pos < lens_v[seqs, 0:1])
        s = jnp.where(valid[None], s.reshape(HEADS, GROUP, width), -jnp.inf)
        s_new = jnp.sum(qg.astype(F32) * kn_out[new, :].astype(F32)[None], axis=-1, keepdims=True) * SCALE
        e, e_new, total = softmax_parts(s, s_new)
        num = jnp.dot(e.reshape(HEADS * GROUP, width), vs[seqs].reshape(width, HD), preferred_element_type=F32)
        num = num.reshape(HEADS, GROUP, HD) + e_new * vn_out[new, :].astype(F32)[None]
        o_out[:, seqs, :] = (num / total).astype(BF)
        return carry

    lax.fori_loop(0, LOCAL // GROUP, group, 0)
    for copy in w_copies + [store]:
        copy.wait()


def project(lengths, x, wq, wk, wv, wo, k_cache, v_cache):
    rows, depth = x.shape
    hbm_spec = pl.BlockSpec(memory_space=pltpu.HBM)
    vmem_spec = pl.BlockSpec(memory_space=pltpu.VMEM)
    return pl.pallas_call(
        project_kernel,
        out_shape=(
            jax.ShapeDtypeStruct((HEADS, LOCAL, HD), BF),
            jax.ShapeDtypeStruct((rows, HD), BF),
            jax.ShapeDtypeStruct((rows, HD), BF),
            jax.ShapeDtypeStruct((HD, 2 * HD), BF),
            jax.ShapeDtypeStruct((HD, 2 * HD), BF),
            jax.ShapeDtypeStruct((HEADS, LOCAL, HD), BF),
            jax.ShapeDtypeStruct((HD, 2 * HD), BF),
        ),
        in_specs=[hbm_spec] * 8,
        out_specs=(vmem_spec,) * 6 + (hbm_spec,),
        scratch_shapes=[
            pltpu.VMEM((rows, depth), BF),
            pltpu.VMEM((depth, HD), BF),
            pltpu.VMEM((depth, HD), BF),
            pltpu.VMEM((depth, HD), BF),
            pltpu.VMEM(wo.shape, BF),
            pltpu.VMEM((rows, HD), BF),
            pltpu.VMEM((LOCAL, SHORT, HD), BF),
            pltpu.VMEM((LOCAL, SHORT, HD), BF),
            pltpu.VMEM((LOCAL, 128), jnp.int32),
            pltpu.SMEM(lengths.shape, jnp.int32),
            pltpu.SemaphoreType.DMA((11,)),
            pltpu.SemaphoreType.DMA,
            pltpu.SemaphoreType.DMA((8,)),
            pltpu.SemaphoreType.DMA((8,)),
            pltpu.SemaphoreType.DMA((2,)),
            pltpu.SemaphoreType.DMA((2,)),
        ],
        compiler_params=pltpu.CompilerParams(collective_id=0, has_side_effects=True, vmem_limit_bytes=24 * MIB),
        name="project",
    )(lengths, x, wq, wk, wv, wo, k_cache, v_cache)


def attend_kernel(len_ref, q_ref, kn_ref, vn_ref, os_ref, k_hbm, v_hbm, o_ref, kn_out, vn_out,
                  kl, vl, qf, knf, vnf, acc, es, st, lidx, lchunks, k_sem, v_sem, new_sem):
    me = lax.axis_index("model")
    base = me * LOCAL
    new_k = pltpu.make_async_copy(kn_ref, kn_out, new_sem.at[0])
    new_v = pltpu.make_async_copy(vn_ref, vn_out, new_sem.at[1])

    def each_part(i, slot, cache, dst, sem, action):
        seq = base + lidx[i]
        chunks = lchunks[i]
        first = 0
        for size in (8, 4, 2, 1):
            rows = pl.ds(pl.multiple_of(first * CHUNK, CHUNK), size * CHUNK)

            @pl.when(chunks & size != 0)
            def _():
                for half in range(2):
                    action(pltpu.make_async_copy(
                        cache.at[seq, 0, rows, pl.ds(half * HALFW, HALFW)],
                        dst.at[slot, half, rows, :], sem.at[slot]))

            first = first + (chunks & size)

    def start(copy):
        copy.start()

    def wait(copy):
        copy.wait()

    keys, values = (k_hbm, kl, k_sem), (v_hbm, vl, v_sem)

    def scan(i, count):
        length = len_ref[base + i]
        lidx[count] = i
        lchunks[count] = jnp.right_shift(length + (CHUNK - 1), CHUNK.bit_length() - 1)
        is_long = length > SHORT

        @pl.when(is_long & (count < AHEAD))
        def _():
            each_part(count, count, *keys, start)

        return count + jnp.where(is_long, 1, 0)

    n_long = lax.fori_loop(0, LOCAL, scan, jnp.int32(0))

    @pl.loop(0, SLOTS * 2)
    def _(i):
        vl[jnp.right_shift(i, 1), i & 1] = jnp.zeros((MAXLEN, HALFW), BF)

    @pl.loop(0, jnp.minimum(n_long, AHEAD))
    def _(i):
        each_part(i, i, *values, start)

    new_k.start()
    new_v.start()
    own = span(me, LOCAL)
    qf[...] = q_ref[...].astype(F32)
    knf[...] = kn_ref[own, :].astype(F32)
    vnf[...] = vn_ref[own, :].astype(F32)
    acc[...] = os_ref[...].astype(F32)

    def rows_of(ref, slot, rows):
        return jnp.concatenate([ref[slot, half, pl.ds(0, rows), :] for half in range(2)], axis=-1)

    def score(i, slot, n):
        rows = n * CHUNK
        at = pl.ds(lidx[i], 1)
        q8 = jnp.concatenate([qf[h, at, :] for h in range(HEADS)], axis=0)
        s = lax.dot_general(q8.astype(BF), rows_of(kl, slot, rows), DIMS_T, preferred_element_type=F32) * SCALE
        s = jnp.where(lax.broadcasted_iota(jnp.int32, s.shape, 1) < len_ref[base + lidx[i]], s, -jnp.inf)
        s_new = jnp.sum(q8 * knf[at, :], axis=-1, keepdims=True) * SCALE
        return softmax_parts(s, s_new)

    def weigh(i, slot, j, n):
        num = jnp.dot(es[j, :, pl.ds(0, n * CHUNK)], rows_of(vl, slot, n * CHUNK), preferred_element_type=F32)
        return (num + st[j, 0, :, 0:1] * vnf[pl.ds(lidx[i], 1), :]) / st[j, 1, :, 0:1]

    def work(now, before, n):
        outs = [weigh(i, slot, j, n) for j, (i, slot) in enumerate(before)]
        parts = [score(i, slot, n) for i, slot in now]
        for (i, _), out in zip(before, outs):
            for h in range(HEADS):
                acc[h, pl.ds(lidx[i], 1), :] = out[h:h + 1, :]
        for j, (e, e_new, total) in enumerate(parts):
            es[j, :, pl.ds(0, n * CHUNK)] = e
            if n * CHUNK < MAXLEN:
                es[j, :, pl.ds(n * CHUNK, MAXLEN - n * CHUNK)] = jnp.zeros((HEADS, MAXLEN - n * CHUNK), BF)
            st[j, 0] = jnp.broadcast_to(e_new, (HEADS, 128))
            st[j, 1] = jnp.broadcast_to(total, (HEADS, 128))

    pairs = jnp.right_shift(n_long + 1, 1)

    def members(p):
        a = p * 2
        slot = a & (SLOTS - 1)
        alone = a + 1 >= n_long
        return a, slot, jnp.where(alone, a, a + 1), jnp.where(alone, slot, slot + 1), alone

    @pl.loop(0, jnp.where(n_long > 0, pairs + 1, 0))
    def _(p):
        a, slot_a, b, slot_b, alone = members(jnp.minimum(p, pairs - 1))
        c, slot_c, d, slot_d, alone_before = members(jnp.maximum(p - 1, 0))
        has_now, has_before = p < pairs, p > 0

        @pl.when(has_now)
        def _():
            each_part(a, slot_a, *keys, wait)

        @pl.when(has_now & jnp.logical_not(alone))
        def _():
            each_part(b, slot_b, *keys, wait)

        @pl.when(has_before)
        def _():
            each_part(c, slot_c, *values, wait)

        @pl.when(has_before & jnp.logical_not(alone_before))
        def _():
            each_part(d, slot_d, *values, wait)

        for j in range(2):
            i = p * 2 + AHEAD + j

            @pl.when(i < n_long)
            def _():
                each_part(i, i & (SLOTS - 1), *keys, start)
                each_part(i, i & (SLOTS - 1), *values, start)

        now, before = ((a, slot_a), (b, slot_b)), ((c, slot_c), (d, slot_d))
        most_now = jnp.maximum(lchunks[a], lchunks[b])
        most_before = jnp.maximum(lchunks[c], lchunks[d])
        for cond, most, args in (
            (has_now & has_before, jnp.maximum(most_now, most_before), (now, before)),
            (p == 0, most_now, (now, ())),
            (p == pairs, most_before, ((), before)),
        ):
            @pl.when(cond)
            def _():
                for n in range(1, MAXLEN // CHUNK + 1):
                    @pl.when(most == n)
                    def _():
                        work(*args, n)

    o_ref[...] = acc[...].astype(BF)
    new_k.wait()
    new_v.wait()


def attend(lengths, q, k_new, v_new, o_short, k_cache, v_cache):
    rows = k_new.shape[0]
    any_spec = pl.BlockSpec(memory_space=pl.ANY)
    vmem_spec = pl.BlockSpec(memory_space=pltpu.VMEM)
    return pl.pallas_call(
        attend_kernel,
        out_shape=(
            jax.ShapeDtypeStruct((HEADS, LOCAL, HD), BF),
            jax.ShapeDtypeStruct((rows, HD), BF),
            jax.ShapeDtypeStruct((rows, HD), BF),
        ),
        in_specs=[pl.BlockSpec(memory_space=pltpu.SMEM)] + [vmem_spec] * 4 + [any_spec] * 2,
        out_specs=(vmem_spec, any_spec, any_spec),
        scratch_shapes=[
            pltpu.VMEM((SLOTS, 2, MAXLEN, HALFW), BF),
            pltpu.VMEM((SLOTS, 2, MAXLEN, HALFW), BF),
            pltpu.VMEM((HEADS, LOCAL, HD), F32),
            pltpu.VMEM((LOCAL, HD), F32),
            pltpu.VMEM((LOCAL, HD), F32),
            pltpu.VMEM((HEADS, LOCAL, HD), F32),
            pltpu.VMEM((2, HEADS, MAXLEN), BF),
            pltpu.VMEM((2, 2, HEADS, 128), F32),
            pltpu.SMEM((LOCAL + 8,), jnp.int32),
            pltpu.SMEM((LOCAL + 8,), jnp.int32),
            pltpu.SemaphoreType.DMA((SLOTS,)),
            pltpu.SemaphoreType.DMA((SLOTS,)),
            pltpu.SemaphoreType.DMA((2,)),
        ],
        compiler_params=pltpu.CompilerParams(vmem_limit_bytes=24 * MIB),
        cost_estimate=pl.CostEstimate(flops=4 * 10 ** 9, bytes_accessed=10 ** 7, transcendentals=10 ** 6),
        name="attend",
    )(lengths, q, k_new, v_new, o_short, k_cache, v_cache)


HALF = HEADS // 2
X, Y, D, S = 2, 4, 6, 1
MSGS = 11


def output_kernel(o_ref, wo_hbm, wx_ref, wy_ref, wd_ref, x_hbm, y_ref, og, wc, xc, load_sem, wss, wrs, os, orr, ys, yr):
    me, _, _, _ = coords()
    chip = me // 2
    load_x = pltpu.make_async_copy(x_hbm.at[:, span(chip, 2 * HD)], xc, load_sem.at[0])
    load_x.start()
    w_loads, w_copies, w_recvs = [], [], []
    for i, (rel, ref) in enumerate(((0, wo_hbm.at[:, span(chip, 2 * HD)]), (D, wd_ref), (X, wx_ref), (Y, wy_ref))):
        w_loads.append(pltpu.make_async_copy(ref, wc.at[peer(rel)], load_sem.at[1 + i]))
        w_loads[-1].start()
        w_copies.append(remote(ref, wc.at[peer(rel)], wss.at[i], wrs.at[i], S))
        w_recvs.append(remote(ref, wc.at[peer(rel + S)], wss.at[i], wrs.at[i], S))
    entry_barrier((X, Y, S))
    started = []

    def go(copy):
        copy.start()
        started.append(copy)

    def o_copy(owner_rel, half, to, index):
        part = pl.ds(half * HALF, HALF)
        dst = og.at[peer(owner_rel) // 2, part]
        return remote(o_ref.at[part] if owner_rel == 0 else dst, dst, os.at[index], orr.at[index], to)

    def y_copy(col_rel, row_rel, half, to, index):
        if half is None:
            rows = span(peer(row_rel), LOCAL)
        else:
            rows = span(peer(row_rel) * 2 + half, LOCAL // 2)
        ref = y_ref.at[rows, span(peer(col_rel) // 2, 2 * HD)]
        return remote(ref, ref, ys.at[index], yr.at[index], to)

    def compute(step, rel):
        total = jnp.zeros((LOCAL, 2 * HD), F32)
        for h in range(HEADS):
            total = total + jnp.dot(og[peer(rel) // 2, h], wc[h], preferred_element_type=F32)
        rows = span(peer(rel), LOCAL)
        y_ref[rows, span(chip, 2 * HD)] = (xc[rows, :].astype(F32) + total).astype(BF)
        b = step * MSGS
        go(y_copy(0, rel, 0, X, b + 0))
        go(y_copy(0, rel, 1, Y, b + 1))
        go(y_copy(0, rel, 1, X, b + 2))
        go(y_copy(0, rel, 0, Y, b + 3))
        go(y_copy(0, rel, None, S, b + 4))

    go(o_copy(0, 0, X, 0))
    go(o_copy(0, 1, Y, 1))
    go(o_copy(0, 1, X, 2))
    go(o_copy(0, 0, Y, 3))
    for c in w_copies:
        go(c)
    og[chip] = o_ref[...]
    load_x.wait()
    for load in w_loads:
        load.wait()
    for c in w_recvs:
        c.wait_recv()
    compute(0, 0)
    o_copy(X, 0, X, 0).wait_recv()
    go(o_copy(X, 0, Y, 4))
    o_copy(Y, 1, Y, 1).wait_recv()
    go(o_copy(Y, 1, X, 5))
    o_copy(X, 1, X, 2).wait_recv()
    compute(1, X)
    o_copy(Y, 0, Y, 3).wait_recv()
    compute(2, Y)
    o_copy(D, 0, Y, 4).wait_recv()
    o_copy(D, 1, X, 5).wait_recv()
    compute(3, D)

    def xor(a, b):
        return ((a // 4 + b // 4) % 2) * 4 + ((a // 2 + b // 2) % 2) * 2 + (a + b) % 2

    order = (0, X, Y, D)
    for step, rel in enumerate(order):
        b = step * MSGS
        at_x, at_y = xor(rel, X), xor(rel, Y)
        y_copy(X, at_x, 0, X, b + 0).wait_recv()
        go(y_copy(X, at_x, 0, Y, b + 5))
        y_copy(Y, at_y, 1, Y, b + 1).wait_recv()
        go(y_copy(Y, at_y, 1, X, b + 6))
        y_copy(X, at_x, 1, X, b + 2).wait_recv()
        go(y_copy(X, at_x, None, S, b + 7))
        y_copy(Y, at_y, 0, Y, b + 3).wait_recv()
        go(y_copy(Y, at_y, None, S, b + 8))
    for step, rel in enumerate(order):
        b = step * MSGS
        at_d = xor(rel, D)
        y_copy(D, at_d, 0, Y, b + 5).wait_recv()
        go(y_copy(D, at_d, 0, S, b + 9))
        y_copy(D, at_d, 1, X, b + 6).wait_recv()
        go(y_copy(D, at_d, 1, S, b + 10))
    for step, rel in enumerate(order):
        b = step * MSGS
        y_copy(S, rel + S, None, S, b + 4).wait_recv()
        y_copy(X + S, xor(rel, X) + S, None, S, b + 7).wait_recv()
        y_copy(Y + S, xor(rel, Y) + S, None, S, b + 8).wait_recv()
        y_copy(D + S, xor(rel, D) + S, 0, S, b + 9).wait_recv()
        y_copy(D + S, xor(rel, D) + S, 1, S, b + 10).wait_recv()
    for copy in started:
        copy.wait_send()


def output(o, wo, wx, wy, wd, x):
    rows, width = x.shape
    hbm_spec = pl.BlockSpec(memory_space=pltpu.HBM)
    vmem_spec = pl.BlockSpec(memory_space=pltpu.VMEM)
    return pl.pallas_call(
        output_kernel,
        out_shape=jax.ShapeDtypeStruct((rows, width), BF),
        in_specs=[vmem_spec, hbm_spec, vmem_spec, vmem_spec, hbm_spec, hbm_spec],
        out_specs=vmem_spec,
        scratch_shapes=[
            pltpu.VMEM((4, HEADS, LOCAL, HD), BF),
            pltpu.VMEM((HEADS, HD, 2 * HD), BF),
            pltpu.VMEM((rows, 2 * HD), BF),
            pltpu.SemaphoreType.DMA((5,)),
            pltpu.SemaphoreType.DMA((4,)),
            pltpu.SemaphoreType.DMA((4,)),
            pltpu.SemaphoreType.DMA((6,)),
            pltpu.SemaphoreType.DMA((6,)),
            pltpu.SemaphoreType.DMA((4 * MSGS,)),
            pltpu.SemaphoreType.DMA((4 * MSGS,)),
        ],
        compiler_params=pltpu.CompilerParams(collective_id=1, has_side_effects=True, vmem_limit_bytes=24 * MIB),
        name="output",
    )(o, wo, wx, wy, wd, x)


def solution(mesh):
    def local_step(x, w_query, w_key, w_value, w_out, k_cache, v_cache, lengths):
        x, w_query, w_key, w_value, w_out = (
            pltpu.with_memory_space_constraint(a, pltpu.HBM) for a in (x, w_query, w_key, w_value, w_out))
        pinned = pltpu.with_memory_space_constraint(lengths, pltpu.HBM)
        q, k_new, v_new, wx, wy, o_short, wd = project(pinned, x, w_query, w_key, w_value, w_out, k_cache, v_cache)
        wd = lax.ppermute(wd, "model", [(d, d ^ D) for d in range(8)])
        o, k_new, v_new = attend(lengths, q, k_new, v_new, o_short, k_cache, v_cache)
        y = output(o, w_out, wx, wy, wd, x)
        return y, k_new[:, None, :], v_new[:, None, :]

    rows_spec = P("replica")
    return jax.shard_map(
        local_step,
        mesh=mesh,
        in_specs=(P("replica", None), P(None, "model"), P(), P(), P("model", None), rows_spec, rows_spec, rows_spec),
        out_specs=(rows_spec, rows_spec, rows_spec),
        check_vma=False,
    )
```

```python
import jax
import jax.numpy as jnp
from jax import lax
from jax.experimental import pallas as pl
from jax.experimental.pallas import tpu as pltpu
from jax.sharding import PartitionSpec as P

BF = jnp.bfloat16
F32 = jnp.float32
HEADS = 8
HD = 256
LOCAL = 64
SHORT = 32
GROUP = 16
CHUNK = 256
MAXLEN = 2048
SLOTS = 6
AHEAD = 4
HALFW = 128
MIB = 2 ** 20
SCALE = HD ** -0.5
DIMS_T = (((1,), (1,)), ((), ()))


def coords():
    me = lax.axis_index("model")
    return me, me // 4, (me // 2) % 2, me % 2


def peer(rel):
    _, y, x, k = coords()
    dy, dx, dk = rel // 4, (rel // 2) % 2, rel % 2
    return (((y + dy) % 2) * 2 + (x + dx) % 2) * 2 + (k + dk) % 2


def span(index, size):
    return pl.ds(pl.multiple_of(index * size, size), size)


def entry_barrier(rels):
    barrier = pltpu.get_barrier_semaphore()
    for rel in rels:
        pl.semaphore_signal(barrier, inc=1, device_id={"model": peer(rel)}, device_id_type=pl.DeviceIdType.MESH)
    pl.semaphore_wait(barrier, len(rels))


def remote(src, dst, send_sem, recv_sem, rel):
    return pltpu.make_async_remote_copy(
        src_ref=src, dst_ref=dst, send_sem=send_sem, recv_sem=recv_sem,
        device_id={"model": peer(rel)}, device_id_type=pl.DeviceIdType.MESH)


RELS = (6, 7, 2, 3, 4, 5, 1)


def softmax_parts(s, s_new):
    m = jnp.maximum(jnp.max(s, axis=-1, keepdims=True), s_new)
    e = jnp.exp(s - m)
    e_new = jnp.exp(s_new - m)
    total = jnp.sum(e, axis=-1, keepdims=True) + e_new
    return e.astype(BF), e_new.astype(BF).astype(F32), total


def project_kernel(len_hbm, x_hbm, wq_hbm, wk_hbm, wv_hbm, wo_hbm, k_hbm, v_hbm, q_out, kn_out, vn_out, wx_out, wy_out, o_out, wd_out,
                   x_v, wq_v, wk_v, wv_v, wo_v, q_v, ks, vs, lens_v, len_ref, in_sem, own_sem, qs, qr, ws, wr):
    me, y, x, k = coords()
    mine = span(me, LOCAL)
    loads = [pltpu.make_async_copy(src, dst, in_sem.at[i]) for i, (src, dst) in enumerate((
        (wq_hbm, wq_v),
        (wo_hbm, wo_v),
        (wk_hbm, wk_v),
        (wv_hbm, wv_v),
        (k_hbm.at[mine, 0, pl.ds(0, SHORT), :], ks),
        (v_hbm.at[mine, 0, pl.ds(0, SHORT), :], vs),
        (len_hbm, len_ref),
    ))]
    loads[0].start()
    blocks = []
    for i, chip_rel in enumerate((6, 2, 4, 0)):
        rows = span(peer(chip_rel) // 2, 2 * LOCAL)
        blocks.append(pltpu.make_async_copy(x_hbm.at[rows, :], x_v.at[rows, :], in_sem.at[7 + i]))
        blocks[-1].start()
    loads[1].start()
    entry_barrier(RELS)
    loads[0].wait()
    q_copies, w_copies = [], []
    for i, chip_rel in enumerate((6, 2, 4, 0)):
        rows = span(peer(chip_rel) // 2, 2 * LOCAL)
        blocks[i].wait()
        q_v[rows, :] = jnp.dot(x_v[rows, :], wq_v[...], preferred_element_type=F32).astype(BF)
        for rel in (chip_rel, chip_rel + 1):
            if rel == 0:
                continue
            copy = remote(q_v.at[span(peer(rel), LOCAL), :], q_out.at[me], qs.at[rel], qr.at[rel], rel)
            copy.start()
            q_copies.append(copy)
    loads[1].wait()
    for i, (rel, out) in enumerate(((X, wx_out), (Y, wy_out))):
        w_copies.append(remote(wo_v.at[:, span(peer(rel) // 2, 2 * HD)], out, ws.at[i], wr.at[i], rel))
        w_copies[i].start()
    store = pltpu.make_async_copy(wo_v.at[:, span(peer(D) // 2, 2 * HD)], wd_out, own_sem)
    store.start()
    for load in loads[2:7]:
        load.start()
    q_out[me] = q_v[mine, :]

    def spread(i, carry):
        lens_v[pl.ds(i, 1), :] = jnp.full((1, 128), len_ref[me * LOCAL + i], jnp.int32)
        return carry

    loads[6].wait()
    lax.fori_loop(0, LOCAL, spread, 0)
    for load in loads[2:6]:
        load.wait()
    for part in range(2):
        rows = pl.ds(part * 256, 256)
        kn_out[rows, :] = jnp.dot(x_v[rows, :], wk_v[...], preferred_element_type=F32).astype(BF)
        vn_out[rows, :] = jnp.dot(x_v[rows, :], wv_v[...], preferred_element_type=F32).astype(BF)
    for copy in q_copies:
        copy.wait()

    width = GROUP * SHORT
    col = lax.broadcasted_iota(jnp.int32, (GROUP, width), 1)
    same = (col // SHORT) == lax.broadcasted_iota(jnp.int32, (GROUP, width), 0)
    slot_pos = col % SHORT

    def group(g, carry):
        seqs = span(g, GROUP)
        new = pl.ds(pl.multiple_of(me * LOCAL + g * GROUP, GROUP), GROUP)
        qg = q_out[:, seqs, :]
        s = lax.dot_general(qg.reshape(HEADS * GROUP, HD), ks[seqs].reshape(width, HD), DIMS_T, preferred_element_type=F32) * SCALE
        valid = same & (slot_pos < lens_v[seqs, 0:1])
        s = jnp.where(valid[None], s.reshape(HEADS, GROUP, width), -jnp.inf)
        s_new = jnp.sum(qg.astype(F32) * kn_out[new, :].astype(F32)[None], axis=-1, keepdims=True) * SCALE
        e, e_new, total = softmax_parts(s, s_new)
        num = jnp.dot(e.reshape(HEADS * GROUP, width), vs[seqs].reshape(width, HD), preferred_element_type=F32)
        num = num.reshape(HEADS, GROUP, HD) + e_new * vn_out[new, :].astype(F32)[None]
        o_out[:, seqs, :] = (num / total).astype(BF)
        return carry

    lax.fori_loop(0, LOCAL // GROUP, group, 0)
    for copy in w_copies + [store]:
        copy.wait()


def project(lengths, x, wq, wk, wv, wo, k_cache, v_cache):
    rows, depth = x.shape
    hbm_spec = pl.BlockSpec(memory_space=pltpu.HBM)
    vmem_spec = pl.BlockSpec(memory_space=pltpu.VMEM)
    return pl.pallas_call(
        project_kernel,
        out_shape=(
            jax.ShapeDtypeStruct((HEADS, LOCAL, HD), BF),
            jax.ShapeDtypeStruct((rows, HD), BF),
            jax.ShapeDtypeStruct((rows, HD), BF),
            jax.ShapeDtypeStruct((HD, 2 * HD), BF),
            jax.ShapeDtypeStruct((HD, 2 * HD), BF),
            jax.ShapeDtypeStruct((HEADS, LOCAL, HD), BF),
            jax.ShapeDtypeStruct((HD, 2 * HD), BF),
        ),
        in_specs=[hbm_spec] * 8,
        out_specs=(vmem_spec,) * 6 + (hbm_spec,),
        scratch_shapes=[
            pltpu.VMEM((rows, depth), BF),
            pltpu.VMEM((depth, HD), BF),
            pltpu.VMEM((depth, HD), BF),
            pltpu.VMEM((depth, HD), BF),
            pltpu.VMEM(wo.shape, BF),
            pltpu.VMEM((rows, HD), BF),
            pltpu.VMEM((LOCAL, SHORT, HD), BF),
            pltpu.VMEM((LOCAL, SHORT, HD), BF),
            pltpu.VMEM((LOCAL, 128), jnp.int32),
            pltpu.SMEM(lengths.shape, jnp.int32),
            pltpu.SemaphoreType.DMA((11,)),
            pltpu.SemaphoreType.DMA,
            pltpu.SemaphoreType.DMA((8,)),
            pltpu.SemaphoreType.DMA((8,)),
            pltpu.SemaphoreType.DMA((2,)),
            pltpu.SemaphoreType.DMA((2,)),
        ],
        compiler_params=pltpu.CompilerParams(collective_id=0, has_side_effects=True, vmem_limit_bytes=24 * MIB),
        name="project",
    )(lengths, x, wq, wk, wv, wo, k_cache, v_cache)


def attend_kernel(len_ref, q_ref, kn_ref, vn_ref, os_ref, k_hbm, v_hbm, o_ref, kn_out, vn_out,
                  kl, vl, qf, knf, vnf, acc, lidx, lchunks, k_sem, v_sem, new_sem):
    me = lax.axis_index("model")
    base = me * LOCAL
    new_k = pltpu.make_async_copy(kn_ref, kn_out, new_sem.at[0])
    new_v = pltpu.make_async_copy(vn_ref, vn_out, new_sem.at[1])

    def each_part(i, slot, action):
        seq = base + lidx[i]
        chunks = lchunks[i]
        first = 0
        for size in (8, 4, 2, 1):
            rows = pl.ds(pl.multiple_of(first * CHUNK, CHUNK), size * CHUNK)

            @pl.when(chunks & size != 0)
            def _():
                for queue, (cache, dst, sem) in enumerate(((k_hbm, kl, k_sem), (v_hbm, vl, v_sem))):
                    for half in range(2):
                        action(pltpu.make_async_copy(
                            cache.at[seq, 0, rows, pl.ds(half * HALFW, HALFW)],
                            dst.at[slot, half, rows, :], sem.at[slot]), queue)

            first = first + (chunks & size)

    def fetch(i, slot):
        each_part(i, slot, lambda copy, queue: copy.start(priority=queue))

    def scan(i, count):
        length = len_ref[base + i]
        lidx[count] = i
        lchunks[count] = jnp.right_shift(length + (CHUNK - 1), CHUNK.bit_length() - 1)
        is_long = length > SHORT

        @pl.when(is_long & (count < AHEAD))
        def _():
            fetch(count, count)

        return count + jnp.where(is_long, 1, 0)

    n_long = lax.fori_loop(0, LOCAL, scan, jnp.int32(0))
    new_k.start()
    new_v.start()
    own = span(me, LOCAL)
    qf[...] = q_ref[...].astype(F32)
    knf[...] = kn_ref[own, :].astype(F32)
    vnf[...] = vn_ref[own, :].astype(F32)
    acc[...] = os_ref[...].astype(F32)

    def rows_of(ref, slot, rows):
        return jnp.concatenate([ref[slot, half, pl.ds(0, rows), :] for half in range(2)], axis=-1)

    def one_long(i, slot, rows):
        seq = lidx[i]
        at = pl.ds(seq, 1)
        q8 = jnp.concatenate([qf[h, at, :] for h in range(HEADS)], axis=0)
        s = lax.dot_general(q8.astype(BF), rows_of(kl, slot, rows), DIMS_T, preferred_element_type=F32) * SCALE
        s = jnp.where(lax.broadcasted_iota(jnp.int32, s.shape, 1) < len_ref[base + seq], s, -jnp.inf)
        s_new = jnp.sum(q8 * knf[at, :], axis=-1, keepdims=True) * SCALE
        e, e_new, total = softmax_parts(s, s_new)
        num = jnp.dot(e, rows_of(vl, slot, rows), preferred_element_type=F32)
        return seq, (num + e_new * vnf[at, :]) / total

    def wait_and_clear(i, slot, most):
        each_part(i, slot, lambda copy, _: copy.wait())

        @pl.loop(lchunks[i], most)
        def _(c):
            vl[slot, :, span(c, CHUNK), :] = jnp.zeros((2, CHUNK, HALFW), BF)

    def step(pair, slot):
        a = pair * 2
        alone = a + 1 >= n_long
        b = jnp.where(alone, a, a + 1)
        slot_b = jnp.where(alone, slot, slot + 1)
        most = jnp.maximum(lchunks[a], lchunks[b])
        wait_and_clear(a, slot, most)

        @pl.when(jnp.logical_not(alone))
        def _():
            wait_and_clear(b, slot + 1, most)

        later = jnp.where(slot >= SLOTS - AHEAD, slot + AHEAD - SLOTS, slot + AHEAD)
        for j in range(2):
            @pl.when(a + AHEAD + j < n_long)
            def _():
                fetch(a + AHEAD + j, later + j)

        for n in range(1, MAXLEN // CHUNK + 1):
            @pl.when(most == n)
            def _():
                results = [one_long(i, at, n * CHUNK) for i, at in ((a, slot), (b, slot_b))]
                for seq, out in results:
                    for h in range(HEADS):
                        acc[h, pl.ds(seq, 1), :] = out[h:h + 1, :]

        return jnp.where(slot + 2 >= SLOTS, 0, slot + 2)

    lax.fori_loop(0, jnp.right_shift(n_long + 1, 1), step, jnp.int32(0))
    o_ref[...] = acc[...].astype(BF)
    new_k.wait()
    new_v.wait()


def attend(lengths, q, k_new, v_new, o_short, k_cache, v_cache):
    rows = k_new.shape[0]
    any_spec = pl.BlockSpec(memory_space=pl.ANY)
    vmem_spec = pl.BlockSpec(memory_space=pltpu.VMEM)
    return pl.pallas_call(
        attend_kernel,
        out_shape=(
            jax.ShapeDtypeStruct((HEADS, LOCAL, HD), BF),
            jax.ShapeDtypeStruct((rows, HD), BF),
            jax.ShapeDtypeStruct((rows, HD), BF),
        ),
        in_specs=[pl.BlockSpec(memory_space=pltpu.SMEM)] + [vmem_spec] * 4 + [any_spec] * 2,
        out_specs=(vmem_spec, any_spec, any_spec),
        scratch_shapes=[
            pltpu.VMEM((SLOTS, 2, MAXLEN, HALFW), BF),
            pltpu.VMEM((SLOTS, 2, MAXLEN, HALFW), BF),
            pltpu.VMEM((HEADS, LOCAL, HD), F32),
            pltpu.VMEM((LOCAL, HD), F32),
            pltpu.VMEM((LOCAL, HD), F32),
            pltpu.VMEM((HEADS, LOCAL, HD), F32),
            pltpu.SMEM((LOCAL + 8,), jnp.int32),
            pltpu.SMEM((LOCAL + 8,), jnp.int32),
            pltpu.SemaphoreType.DMA((SLOTS,)),
            pltpu.SemaphoreType.DMA((SLOTS,)),
            pltpu.SemaphoreType.DMA((2,)),
        ],
        compiler_params=pltpu.CompilerParams(vmem_limit_bytes=24 * MIB),
        cost_estimate=pl.CostEstimate(flops=4 * 10 ** 9, bytes_accessed=10 ** 7, transcendentals=10 ** 6),
        name="attend",
    )(lengths, q, k_new, v_new, o_short, k_cache, v_cache)


HALF = HEADS // 2
X, Y, D, S = 2, 4, 6, 1
MSGS = 11


def output_kernel(o_ref, wo_hbm, wx_ref, wy_ref, wd_ref, x_hbm, y_ref, og, wc, xc, load_sem, wss, wrs, os, orr, ys, yr):
    me, _, _, _ = coords()
    chip = me // 2
    load_x = pltpu.make_async_copy(x_hbm.at[:, span(chip, 2 * HD)], xc, load_sem.at[0])
    load_x.start()
    w_loads, w_copies, w_recvs = [], [], []
    for i, (rel, ref) in enumerate(((0, wo_hbm.at[:, span(chip, 2 * HD)]), (D, wd_ref), (X, wx_ref), (Y, wy_ref))):
        w_loads.append(pltpu.make_async_copy(ref, wc.at[peer(rel)], load_sem.at[1 + i]))
        w_loads[-1].start()
        w_copies.append(remote(ref, wc.at[peer(rel)], wss.at[i], wrs.at[i], S))
        w_recvs.append(remote(ref, wc.at[peer(rel + S)], wss.at[i], wrs.at[i], S))
    entry_barrier((X, Y, S))
    started = []

    def go(copy):
        copy.start()
        started.append(copy)

    def o_copy(owner_rel, half, to, index):
        part = pl.ds(half * HALF, HALF)
        dst = og.at[peer(owner_rel) // 2, part]
        return remote(o_ref.at[part] if owner_rel == 0 else dst, dst, os.at[index], orr.at[index], to)

    def y_copy(col_rel, row_rel, half, to, index):
        if half is None:
            rows = span(peer(row_rel), LOCAL)
        else:
            rows = span(peer(row_rel) * 2 + half, LOCAL // 2)
        ref = y_ref.at[rows, span(peer(col_rel) // 2, 2 * HD)]
        return remote(ref, ref, ys.at[index], yr.at[index], to)

    def compute(step, rel):
        total = jnp.zeros((LOCAL, 2 * HD), F32)
        for h in range(HEADS):
            total = total + jnp.dot(og[peer(rel) // 2, h], wc[h], preferred_element_type=F32)
        rows = span(peer(rel), LOCAL)
        y_ref[rows, span(chip, 2 * HD)] = (xc[rows, :].astype(F32) + total).astype(BF)
        b = step * MSGS
        go(y_copy(0, rel, 0, X, b + 0))
        go(y_copy(0, rel, 1, Y, b + 1))
        go(y_copy(0, rel, 1, X, b + 2))
        go(y_copy(0, rel, 0, Y, b + 3))
        go(y_copy(0, rel, None, S, b + 4))

    go(o_copy(0, 0, X, 0))
    go(o_copy(0, 1, Y, 1))
    go(o_copy(0, 1, X, 2))
    go(o_copy(0, 0, Y, 3))
    for c in w_copies:
        go(c)
    og[chip] = o_ref[...]
    load_x.wait()
    for load in w_loads:
        load.wait()
    for c in w_recvs:
        c.wait_recv()
    compute(0, 0)
    o_copy(X, 0, X, 0).wait_recv()
    go(o_copy(X, 0, Y, 4))
    o_copy(Y, 1, Y, 1).wait_recv()
    go(o_copy(Y, 1, X, 5))
    o_copy(X, 1, X, 2).wait_recv()
    compute(1, X)
    o_copy(Y, 0, Y, 3).wait_recv()
    compute(2, Y)
    o_copy(D, 0, Y, 4).wait_recv()
    o_copy(D, 1, X, 5).wait_recv()
    compute(3, D)

    def xor(a, b):
        return ((a // 4 + b // 4) % 2) * 4 + ((a // 2 + b // 2) % 2) * 2 + (a + b) % 2

    order = (0, X, Y, D)
    for step, rel in enumerate(order):
        b = step * MSGS
        at_x, at_y = xor(rel, X), xor(rel, Y)
        y_copy(X, at_x, 0, X, b + 0).wait_recv()
        go(y_copy(X, at_x, 0, Y, b + 5))
        y_copy(Y, at_y, 1, Y, b + 1).wait_recv()
        go(y_copy(Y, at_y, 1, X, b + 6))
        y_copy(X, at_x, 1, X, b + 2).wait_recv()
        go(y_copy(X, at_x, None, S, b + 7))
        y_copy(Y, at_y, 0, Y, b + 3).wait_recv()
        go(y_copy(Y, at_y, None, S, b + 8))
    for step, rel in enumerate(order):
        b = step * MSGS
        at_d = xor(rel, D)
        y_copy(D, at_d, 0, Y, b + 5).wait_recv()
        go(y_copy(D, at_d, 0, S, b + 9))
        y_copy(D, at_d, 1, X, b + 6).wait_recv()
        go(y_copy(D, at_d, 1, S, b + 10))
    for step, rel in enumerate(order):
        b = step * MSGS
        y_copy(S, rel + S, None, S, b + 4).wait_recv()
        y_copy(X + S, xor(rel, X) + S, None, S, b + 7).wait_recv()
        y_copy(Y + S, xor(rel, Y) + S, None, S, b + 8).wait_recv()
        y_copy(D + S, xor(rel, D) + S, 0, S, b + 9).wait_recv()
        y_copy(D + S, xor(rel, D) + S, 1, S, b + 10).wait_recv()
    for copy in started:
        copy.wait_send()


def output(o, wo, wx, wy, wd, x):
    rows, width = x.shape
    hbm_spec = pl.BlockSpec(memory_space=pltpu.HBM)
    vmem_spec = pl.BlockSpec(memory_space=pltpu.VMEM)
    return pl.pallas_call(
        output_kernel,
        out_shape=jax.ShapeDtypeStruct((rows, width), BF),
        in_specs=[vmem_spec, hbm_spec, vmem_spec, vmem_spec, hbm_spec, hbm_spec],
        out_specs=vmem_spec,
        scratch_shapes=[
            pltpu.VMEM((4, HEADS, LOCAL, HD), BF),
            pltpu.VMEM((HEADS, HD, 2 * HD), BF),
            pltpu.VMEM((rows, 2 * HD), BF),
            pltpu.SemaphoreType.DMA((5,)),
            pltpu.SemaphoreType.DMA((4,)),
            pltpu.SemaphoreType.DMA((4,)),
            pltpu.SemaphoreType.DMA((6,)),
            pltpu.SemaphoreType.DMA((6,)),
            pltpu.SemaphoreType.DMA((4 * MSGS,)),
            pltpu.SemaphoreType.DMA((4 * MSGS,)),
        ],
        compiler_params=pltpu.CompilerParams(collective_id=1, has_side_effects=True, vmem_limit_bytes=24 * MIB),
        name="output",
    )(o, wo, wx, wy, wd, x)


def solution(mesh):
    def local_step(x, w_query, w_key, w_value, w_out, k_cache, v_cache, lengths):
        x, w_query, w_key, w_value, w_out = (
            pltpu.with_memory_space_constraint(a, pltpu.HBM) for a in (x, w_query, w_key, w_value, w_out))
        pinned = pltpu.with_memory_space_constraint(lengths, pltpu.HBM)
        q, k_new, v_new, wx, wy, o_short, wd = project(pinned, x, w_query, w_key, w_value, w_out, k_cache, v_cache)
        wd = lax.ppermute(wd, "model", [(d, d ^ D) for d in range(8)])
        o, k_new, v_new = attend(lengths, q, k_new, v_new, o_short, k_cache, v_cache)
        y = output(o, w_out, wx, wy, wd, x)
        return y, k_new[:, None, :], v_new[:, None, :]

    rows_spec = P("replica")
    return jax.shard_map(
        local_step,
        mesh=mesh,
        in_specs=(P("replica", None), P(None, "model"), P(), P(), P("model", None), rows_spec, rows_spec, rows_spec),
        out_specs=(rows_spec, rows_spec, rows_spec),
        check_vma=False,
    )
```
